8 devices in a mesh: z: 2 (over z, y), y: 2 (over x), x: 2 (over core).
Axes of the slice: x: 2, y: 2, z: 1, core: 2. Of those that a mesh axis runs over, the one named last changes fastest.
Arguments:
- atom_pos: float32 [5832, 3], P(('z', 'y', 'x'))
- atom_vel: float32 [5832, 3], P(('z', 'y', 'x'))
- atom_frc: float32 [5832, 3], P(('z', 'y', 'x'))
- atom_id: int32 [5832], P(('z', 'y', 'x'))
- atom_ok: int32 [5832], P(('z', 'y', 'x'))
- brick_side: float32 [], replicated
Outputs:
- output 1: float32 [5832, 3], P(('z', 'y', 'x'))
- output 2: float32 [5832, 3], P(('z', 'y', 'x'))
- output 3: float32 [5832, 3], P(('z', 'y', 'x'))
- output 4: int32 [5832], P(('z', 'y', 'x'))
- output 5: int32 [5832], P(('z', 'y', 'x'))
- output 6: float32 [], replicated
All inputs are finite; a program needn't handle non-finite values.
Results may differ from the reference program's by a relative error of at most 0.001.
Values sent between devices are 32-bit elements.
A program may use at most 1 GiB of HBM per device.

```python
import jax
import jax.numpy as jnp
from jax import lax

NZ = 2
NY = 2
NX = 2
GRID = 8
RHO_E4 = 6500
CAP = 729

DEVICES = NZ * NY * NX
SITES = DEVICES * GRID * GRID * GRID
MOVE_MAX = max(1, CAP // 100)
PLANE = (GRID - 1) * (GRID - 1)
SITE_SHAPE = (NZ, NY, NX, GRID, GRID, GRID)
VEC_SHAPE = (NZ, NY, NX, GRID, GRID, GRID, 3)
DT = 0.005
RC = 2.5
UCUT = 4.0 * (RC ** -12 - RC ** -6)
UPC = -48.0 * RC ** -13 + 24.0 * RC ** -7


def place_atoms(base_key, spacing, jitter, free_disp, prev_force):
    sub_keys = jax.random.split(base_key, 8)
    brick_vec = jnp.stack([lax.broadcasted_iota(jnp.int32, SITE_SHAPE, 2), lax.broadcasted_iota(jnp.int32, SITE_SHAPE, 1), lax.broadcasted_iota(jnp.int32, SITE_SHAPE, 0)], axis=-1)
    site_vec = jnp.stack([lax.broadcasted_iota(jnp.int32, SITE_SHAPE, 5), lax.broadcasted_iota(jnp.int32, SITE_SHAPE, 4), lax.broadcasted_iota(jnp.int32, SITE_SHAPE, 3)], axis=-1)
    dims_int = jnp.array([NX, NY, NZ], jnp.int32)
    on_face = site_vec == 0
    face_count = jnp.sum(on_face.astype(jnp.int32), axis=-1, keepdims=True)
    side_sign = 2 * jax.random.randint(sub_keys[0], VEC_SHAPE, 0, 2) - 1
    plane_perm = jax.random.permutation(sub_keys[1], jnp.broadcast_to(jnp.arange(PLANE), (NZ, NY, NX, 3, PLANE)), axis=-1, independent=True)
    inner_k = jnp.maximum(site_vec - 1, 0)
    plane_idx = jnp.stack([inner_k[..., (axis_d + 1) % 3] * (GRID - 1) + inner_k[..., (axis_d + 2) % 3] for axis_d in range(3)], axis=-1)
    plane_rank = jnp.take_along_axis(jnp.broadcast_to(plane_perm[:, :, :, None, None, None, :, :], VEC_SHAPE + (PLANE,)), plane_idx[..., None], axis=-1)[..., 0]
    down_count = jax.random.randint(sub_keys[2], (NZ, NY, NX, 3), 0, MOVE_MAX + 1)[:, :, :, None, None, None, :]
    up_count = jax.random.randint(sub_keys[3], (NZ, NY, NX, 3), 0, MOVE_MAX + 1).at[0, 0, 0, 0].set(MOVE_MAX)[:, :, :, None, None, None, :]
    plane_site = on_face & (face_count == 1)
    go_down = plane_site & (plane_rank < down_count)
    go_up = plane_site & (plane_rank >= down_count) & (plane_rank < down_count + up_count)
    edge_flag = (face_count == 2) & jnp.logical_not(on_face[..., 2:3]) & (site_vec[..., 2:3] == 1)
    corner_flag = face_count == 3
    crossing = go_down | go_up | (on_face & (edge_flag | corner_flag))
    side_sign = jnp.where(go_down, -1, jnp.where(go_up, 1, side_sign))
    pre_side = jnp.where(crossing, -side_sign, side_sign)
    pre_brick = jnp.mod(brick_vec + jnp.where(on_face & (pre_side < 0), -1, 0), dims_int)
    pre_dev = (pre_brick[..., 2] * NY + pre_brick[..., 1]) * NX + pre_brick[..., 0]
    fill_pct = jax.random.randint(sub_keys[4], (NZ, NY, NX, 1, 1, 1), 50, 101)
    occupied = (jax.random.randint(sub_keys[5], SITE_SHAPE, 0, 100) < fill_pct) | jnp.any(crossing, axis=-1)
    atom_ids = jax.random.permutation(sub_keys[6], SITES).astype(jnp.int32).reshape(SITE_SHAPE)
    near_gaps = jax.random.uniform(sub_keys[7], VEC_SHAPE + (2,), jnp.float32, 0.002, 0.006)
    face_gap = near_gaps[..., 0]
    cross_gap = near_gaps[..., 1]
    sign_f = side_sign.astype(jnp.float32)
    lattice = (brick_vec * GRID + site_vec).astype(jnp.float32) * spacing
    post_pos = lattice + jnp.where(on_face, sign_f * face_gap, jitter * spacing)
    displace = jnp.where(on_face, jnp.where(crossing, sign_f * (face_gap + cross_gap), 0.5 * sign_f * face_gap), free_disp)
    box_len = spacing * GRID * dims_int.astype(jnp.float32)
    start_pos = jnp.mod(post_pos - displace, box_len)
    start_vel = displace / DT - (0.5 * DT) * prev_force
    flat_ok = occupied.reshape(SITES)
    flat_dev = pre_dev.reshape(SITES)
    sort_key = jnp.where(flat_ok, flat_dev * SITES + atom_ids.reshape(SITES), DEVICES * SITES)
    sort_order = jnp.argsort(sort_key)
    counts = jax.ops.segment_sum(flat_ok.astype(jnp.int32), flat_dev, num_segments=DEVICES)
    first_row = jnp.cumsum(counts) - counts
    sorted_dev = flat_dev[sort_order]
    dest_row = jnp.where(flat_ok[sort_order], sorted_dev * CAP + jnp.arange(SITES) - first_row[sorted_dev], DEVICES * CAP)

    def spread(values):
        tail_dims = values.shape[6:]
        flat_vals = values.reshape((SITES,) + tail_dims)[sort_order]
        return jnp.zeros((DEVICES * CAP,) + tail_dims, values.dtype).at[dest_row].set(flat_vals, mode="drop")

    return {"atom_pos": spread(start_pos), "atom_vel": spread(start_vel), "atom_frc": spread(prev_force), "atom_id": spread(atom_ids), "atom_ok": spread(occupied.astype(jnp.int32)), "brick_side": spacing * GRID}


def setup_inputs(seed: int = 0) -> dict:
    value_keys = jax.random.split(jax.random.key(seed + 1), 4)
    spacing = (RHO_E4 / 10000.0) ** (-1.0 / 3.0) * (1.0 + 0.01 * jax.random.uniform(value_keys[0], (), jnp.float32, -1.0, 1.0))
    jitter = jax.random.uniform(value_keys[1], VEC_SHAPE, jnp.float32, -0.05, 0.05)
    free_disp = jax.random.uniform(value_keys[2], VEC_SHAPE, jnp.float32, -0.01, 0.01)
    prev_force = 40.0 * jax.random.normal(value_keys[3], VEC_SHAPE, jnp.float32)
    return place_atoms(jax.random.key(seed), spacing, jitter, free_disp, prev_force)


def pair_terms(own_pos, own_ok, other_pos, other_ok, box_len):
    delta_r = own_pos[..., :, None, :] - other_pos[..., None, :, :]
    delta_r = delta_r - box_len * jnp.floor(delta_r / box_len + 0.5)
    dist_sq = jnp.sum(delta_r * delta_r, axis=-1)
    in_range = own_ok[..., :, None] & other_ok[..., None, :] & (dist_sq < RC * RC) & (dist_sq > 0.01)
    safe_sq = jnp.where(in_range, dist_sq, 1.0)
    inv_r2 = 1.0 / safe_sq
    inv_r6 = inv_r2 * inv_r2 * inv_r2
    radius = jnp.sqrt(safe_sq)
    f_scale = jnp.where(in_range, (48.0 * inv_r6 * inv_r6 - 24.0 * inv_r6) * inv_r2 + UPC / radius, 0.0)
    pair_energy = jnp.where(in_range, 4.0 * (inv_r6 * inv_r6 - inv_r6) - UCUT - (radius - RC) * UPC, 0.0)
    force_sum = jnp.sum(f_scale[..., None] * delta_r, axis=-2)
    return force_sum, jnp.sum(pair_energy)


def brick_forces(own_pos, own_ok, other_pos, other_ok, box_len):
    force_sum = jnp.zeros_like(own_pos)
    energy_sum = jnp.zeros((), own_pos.dtype)
    for neighbor in range(other_pos.shape[0]):
        force_part, energy_part = pair_terms(own_pos, own_ok, other_pos[neighbor], other_ok[neighbor], box_len)
        force_sum = force_sum + force_part
        energy_sum = energy_sum + energy_part
    return force_sum, energy_sum


def reference(atom_pos, atom_vel, atom_frc, atom_id, atom_ok, brick_side):
    dims_int = jnp.array([NX, NY, NZ], jnp.int32)
    box_len = brick_side * dims_int.astype(jnp.float32)
    owned = atom_ok > 0
    half_v = atom_vel + (0.5 * DT) * atom_frc
    moved = jnp.mod(atom_pos + DT * half_v, box_len)
    new_cell = jnp.clip(jnp.floor(moved / brick_side).astype(jnp.int32), 0, dims_int - 1)
    dest_dev = (new_cell[:, 2] * NY + new_cell[:, 1]) * NX + new_cell[:, 0]
    sort_key = jnp.where(owned, dest_dev * SITES + atom_id, DEVICES * SITES)
    sort_order = jnp.argsort(sort_key)
    counts = jax.ops.segment_sum(owned.astype(jnp.int32), dest_dev, num_segments=DEVICES)
    first_row = jnp.cumsum(counts) - counts
    sorted_dev = dest_dev[sort_order]
    dest_row = jnp.where(owned[sort_order], sorted_dev * CAP + jnp.arange(DEVICES * CAP) - first_row[sorted_dev], DEVICES * CAP)

    def spread(values):
        return jnp.zeros_like(values).at[dest_row].set(values[sort_order], mode="drop")

    new_pos = spread(moved)
    new_half = spread(half_v)
    new_id = spread(atom_id)
    new_ok = spread(atom_ok)
    grid_pos = new_pos.reshape(NZ, NY, NX, CAP, 3)
    grid_ok = (new_ok > 0).reshape(NZ, NY, NX, CAP)
    steps_z = range(-1, 2) if NZ > 2 else range(0, 2)
    steps_y = range(-1, 2) if NY > 2 else range(0, 2)
    steps_x = range(-1, 2) if NX > 2 else range(0, 2)
    shell_list = [(shift_z, shift_y, shift_x) for shift_z in steps_z for shift_y in steps_y for shift_x in steps_x]
    other_pos = jnp.stack([jnp.roll(grid_pos, (-shift_zyx[0], -shift_zyx[1], -shift_zyx[2]), axis=(0, 1, 2)) for shift_zyx in shell_list], axis=3)
    other_ok = jnp.stack([jnp.roll(grid_ok, (-shift_zyx[0], -shift_zyx[1], -shift_zyx[2]), axis=(0, 1, 2)) for shift_zyx in shell_list], axis=3)
    n_shell = len(shell_list)
    force_grid, energy_grid = lax.map(lambda packed: brick_forces(packed[0], packed[1], packed[2], packed[3], box_len), (grid_pos.reshape(DEVICES, CAP, 3), grid_ok.reshape(DEVICES, CAP), other_pos.reshape(DEVICES, n_shell, CAP, 3), other_ok.reshape(DEVICES, n_shell, CAP)))
    new_force = force_grid.reshape(DEVICES * CAP, 3)
    ok_f = (new_ok > 0).astype(new_pos.dtype)[:, None]
    new_vel = (new_half + (0.5 * DT) * new_force) * ok_f
    energy = 0.5 * jnp.sum(energy_grid)
    return new_pos, new_vel, new_force, new_id, new_ok, energy
```

```python
import functools

import jax
import jax.numpy as jnp
from jax import lax
from jax.experimental import pallas as pl
from jax.experimental.pallas import tpu as pltpu
from jax.sharding import PartitionSpec as P

DT = 0.005
RC = 2.5
FAR_AWAY = 1.0e6
UCUT = 4.0 * (RC ** -12 - RC ** -6)
UPC = -48.0 * RC ** -13 + 24.0 * RC ** -7
MESH_AXES = ("z", "y", "x")
CAP = 729
PAD = 768
MIG = 256
FULL = PAD + MIG
SEG = {1: (0, 16), 2: (16, 16), 4: (32, 16), 3: (64, 32), 5: (96, 32), 6: (128, 32), 7: (192, 64)}
IC = 32
MESH_ID = pl.DeviceIdType.MESH


def pieces_of(rows):
    first = rows.astype(jnp.bfloat16).astype(jnp.float32)
    rest = rows - first
    second = rest.astype(jnp.bfloat16).astype(jnp.float32)
    third = rest - second
    return jnp.concatenate([first, second, third], axis=0).astype(jnp.bfloat16)


def select_rows(rows, onehot):
    out = lax.dot_general(pieces_of(rows), onehot, (((1,), (1,)), ((), ())), preferred_element_type=jnp.float32)
    return out[0:8] + out[8:16] + out[16:24]


def partner(relation):
    mine = (lax.axis_index("z"), lax.axis_index("y"), lax.axis_index("x"))
    bits = (relation // 4 % 2, relation // 2 % 2, relation % 2)
    return tuple((axis + bit) % 2 for axis, bit in zip(mine, bits))


def greet():
    barrier = pltpu.get_barrier_semaphore()
    for relation in range(1, 8):
        pl.semaphore_signal(barrier, inc=1, device_id=partner(relation), device_id_type=MESH_ID)
    return barrier


def axis_column(values, rows):
    idx = lax.broadcasted_iota(jnp.int32, (rows, 1), 0)
    out = jnp.full((rows, 1), values[-1], jnp.float32)
    for k in range(len(values) - 1):
        out = jnp.where(idx == k, values[k], out)
    return out


def brick_coords():
    return [lax.axis_index(name).astype(jnp.float32) for name in ("x", "y", "z")]


def exchange_kernel(pos_ref, vel_ref, frc_ref, id_ref, ok_ref, side_ref, own_ref, all_ref, mig_ref, pad_ref, send_sem, recv_sem):
    barrier = greet()
    side = side_ref[0, 0]
    box = side * 2.0
    pad_ref[...] = jnp.zeros_like(pad_ref)
    half_v = vel_ref[...] + (0.5 * DT) * frc_ref[...]
    pad_ref[0:3, 0:CAP] = pos_ref[...] + DT * half_v
    pad_ref[3:6, 0:CAP] = half_v
    pad_ref[6:7, 0:CAP] = (id_ref[...] >> 16).astype(jnp.float32) + 1.0
    pad_ref[7:8, 0:CAP] = (id_ref[...] & 65535).astype(jnp.float32)
    pad_ref[8:9, 0:CAP] = ok_ref[...].astype(jnp.float32)
    unwrapped = pad_ref[0:3, :]
    owned = pad_ref[8:9, :] > 0.5
    moved = jnp.where(unwrapped < 0.0, unwrapped + box, jnp.where(unwrapped >= box, unwrapped - box, unwrapped))
    low = axis_column([coord * side for coord in brick_coords()], 3)
    outside = (unwrapped < low) | (unwrapped >= low + side)
    bits = jnp.where(outside, axis_column([1.0, 2.0, 4.0], 3), 0.0)
    code = jnp.sum(bits, axis=0, keepdims=True)
    code = jnp.where(owned, code, -1.0)
    all_ref[0, 0:3, :] = jnp.where(owned, moved, FAR_AWAY)
    all_ref[0, 3:4, :] = jnp.zeros((1, PAD), jnp.float32)

    relation_col = lax.broadcasted_iota(jnp.int32, (8, PAD), 0).astype(jnp.float32)
    member = (code == relation_col).astype(jnp.float32)
    stacked = jnp.concatenate([member[:, 128 * b:128 * (b + 1)] for b in range(PAD // 128)], axis=0).astype(jnp.bfloat16)
    row = lax.broadcasted_iota(jnp.int32, (128, 256), 0)
    col = lax.broadcasted_iota(jnp.int32, (128, 256), 1)
    ladder = ((row < col) | (col >= 128)).astype(jnp.float32).astype(jnp.bfloat16)
    counts = jnp.dot(stacked, ladder, preferred_element_type=jnp.float32)
    before = jnp.zeros((8, 128), jnp.float32)
    ranks = []
    for b in range(PAD // 128):
        ranks.append(counts[8 * b:8 * b + 8, 0:128] + before)
        before = before + counts[8 * b:8 * b + 8, 128:256]
    rank = jnp.concatenate(ranks, axis=1)
    offset = axis_column([0.0] + [float(SEG[m][0]) for m in range(1, 8)], 8)
    moving = (code > 0.5)
    slot = jnp.sum(jnp.where(member > 0.5, rank + offset, 0.0), axis=0, keepdims=True)
    slot = jnp.where(moving, slot, -1.0)
    rows = jnp.concatenate([moved, pad_ref[3:8, :]], axis=0)
    slots = lax.broadcasted_iota(jnp.int32, (MIG, PAD), 0).astype(jnp.float32)
    onehot = (slots == slot).astype(jnp.float32).astype(jnp.bfloat16)
    mig_ref[0] = select_rows(rows, onehot)

    staying = code == 0.0
    own_ref[0:8, :] = rows
    own_ref[8:9, :] = jnp.where(staying, rank[0:1, :], -1.0)

    pl.semaphore_wait(barrier, 7)
    copies = []
    for relation in range(1, 8):
        for which, ref in enumerate((all_ref, mig_ref)):
            copy = pltpu.make_async_remote_copy(src_ref=ref.at[0], dst_ref=ref.at[relation], send_sem=send_sem.at[which, relation], recv_sem=recv_sem.at[which, relation], device_id=partner(relation), device_id_type=MESH_ID)
            copy.start()
            copies.append(copy)
    for copy in copies:
        copy.wait()


def pair_terms(own, other, span):
    delta = []
    for mine, theirs in zip(own, other):
        diff = mine - theirs
        if span is not None:
            diff = diff - jnp.where(diff > 0.5 * span, span, jnp.where(diff < -0.5 * span, -span, 0.0))
        delta.append(diff)
    dist_sq = delta[0] * delta[0] + delta[1] * delta[1] + delta[2] * delta[2]
    in_range = (dist_sq < RC * RC) & (dist_sq > 0.01)
    inv_r = jnp.where(in_range, lax.rsqrt(dist_sq), 0.0)
    inv_r2 = inv_r * inv_r
    inv_r6 = inv_r2 * inv_r2 * inv_r2
    scale = (48.0 * inv_r6 - 24.0) * inv_r6 * inv_r2 + UPC * inv_r
    energy = 4.0 * inv_r6 * (inv_r6 - 1.0) - UPC * (dist_sq * inv_r) - jnp.where(in_range, UCUT - RC * UPC, 0.0)
    return [scale * d for d in delta], energy


def force_kernel(own_ref, all_ref, mig_ref, side_ref, pos_ref, vel_ref, frc_ref, id_ref, ok_ref, en_ref, cand_ref, near_ref, mine_ref, acc_ref):
    side = side_ref[0, 0]
    box = side * 2.0
    lane = lax.broadcasted_iota(jnp.int32, (1, MIG), 1)
    arrivals = jnp.zeros((8, MIG), jnp.float32)
    for relation, (start, size) in SEG.items():
        arrivals = jnp.where((lane >= start) & (lane < start + size), mig_ref[relation], arrivals)
    cand_ref[:, 0:PAD] = own_ref[0:8, :]
    cand_ref[:, PAD:FULL] = arrivals
    stay_rank = own_ref[8:9, :]
    cand = cand_ref[...]
    valid = jnp.concatenate([stay_rank >= 0.0, arrivals[6:7, :] > 0.5], axis=1)
    number = (cand[6:7, :].astype(jnp.int32) - 1) * 65536 + cand[7:8, :].astype(jnp.int32)
    key = jnp.where(valid, number, 2147483647)
    key_col = jnp.transpose(jnp.broadcast_to(key, (8, FULL)))[:, 0:1]
    in_front = jnp.sum((key_col[PAD:FULL] < key).astype(jnp.float32), axis=0, keepdims=True)
    behind = jnp.sum((key_col[0:PAD] < key[:, PAD:FULL]).astype(jnp.float32), axis=0, keepdims=True)
    rank = in_front + jnp.concatenate([stay_rank, behind], axis=1)
    rank = jnp.where(valid, rank, -1.0)
    slots = lax.broadcasted_iota(jnp.int32, (PAD, FULL), 0).astype(jnp.float32)
    onehot = (slots == rank).astype(jnp.float32).astype(jnp.bfloat16)
    rows = select_rows(cand, onehot)
    filled = rows[6:7, :] > 0.5
    total = jnp.sum(filled.astype(jnp.int32))

    centre = [(coord + 0.5) * side for coord in brick_coords()]
    local = rows[0:3, :] - axis_column(centre, 3)
    local = jnp.where(filled, local, -FAR_AWAY)
    columns = jnp.transpose(jnp.concatenate([local, jnp.zeros((5, PAD), jnp.float32)], axis=0))
    for axis in range(3):
        mine_ref[axis] = jnp.broadcast_to(columns[:, axis:axis + 1], (PAD, 128))
    start = 0
    centre4 = axis_column(centre + [0.0], 4)
    for relation in range(8):
        theirs = all_ref[relation] - centre4
        near = jnp.where(theirs > side, theirs - box, jnp.where(theirs < -side, theirs + box, theirs))
        near_ref[:, pl.ds(pl.multiple_of(start, 128), PAD)] = near
        held = jnp.sum((near[0:1, :] < 0.5 * FAR_AWAY).astype(jnp.int32))
        start = start + (held + 127) // 128 * 128
    near_ref[:, pl.ds(pl.multiple_of(start, 128), 128)] = jnp.full((4, 128), FAR_AWAY, jnp.float32)
    n_other = (start + 255) // 256
    n_own = (total + IC - 1) // IC
    acc_ref[...] = jnp.zeros_like(acc_ref)
    en_ref[...] = jnp.zeros_like(en_ref)

    def sweep(span):
        def own_step(i, carry):
            first = pl.multiple_of(i * IC, IC)
            own = [mine_ref[axis, pl.ds(first, IC), :] for axis in range(3)]

            def other_step(j, sums):
                lanes = pl.multiple_of(j * 256, 256)
                for half in range(2):
                    other = [near_ref[axis:axis + 1, pl.ds(lanes + 128 * half, 128)] for axis in range(3)]
                    force, energy = pair_terms(own, other, span)
                    sums = tuple(s + t for s, t in zip(sums, force + [energy]))
                return sums

            zero = jnp.zeros((IC, 128), jnp.float32)
            sums = lax.fori_loop(0, n_other, other_step, (zero,) * 4)
            for axis in range(3):
                acc_ref[axis, pl.ds(first, IC), :] = sums[axis]
            energy = sums[3]
            en_ref[...] += energy[0:8] + energy[8:16] + energy[16:24] + energy[24:32]
            return carry

        lax.fori_loop(0, n_own, own_step, 0)

    @pl.when(side >= 2.0 * RC)
    def _():
        sweep(None)

    @pl.when(side < 2.0 * RC)
    def _():
        sweep(box)

    out_rows = []
    for axis in range(3):
        parts = []
        for b in range(PAD // 128):
            parts.append(jnp.sum(jnp.transpose(acc_ref[axis, 128 * b:128 * b + 128, :]), axis=0, keepdims=True))
        out_rows.append(jnp.concatenate(parts, axis=1))
    force = jnp.where(filled, jnp.concatenate(out_rows, axis=0), 0.0)
    frc_ref[...] = force[:, 0:CAP]
    pos_ref[...] = rows[0:3, 0:CAP]
    vel_ref[...] = (rows[3:6, :] + (0.5 * DT) * force)[:, 0:CAP]
    new_id = (rows[6:7, :].astype(jnp.int32) - 1) * 65536 + rows[7:8, :].astype(jnp.int32)
    id_ref[...] = jnp.where(filled, new_id, 0)[:, 0:CAP]
    ok_ref[...] = filled.astype(jnp.int32)[:, 0:CAP]


def energy_kernel(en_ref, out_ref, parts_ref, send_sem, recv_sem):
    barrier = greet()
    pl.semaphore_wait(barrier, 7)
    copies = []
    for relation in range(1, 8):
        copy = pltpu.make_async_remote_copy(src_ref=en_ref, dst_ref=parts_ref.at[relation], send_sem=send_sem.at[relation], recv_sem=recv_sem.at[relation], device_id=partner(relation), device_id_type=MESH_ID)
        copy.start()
        copies.append(copy)
    for copy in copies:
        copy.wait()
    parts_ref[0] = en_ref[...]
    over_x = [parts_ref[k] + parts_ref[k + 1] for k in (0, 2, 4, 6)]
    total = (over_x[0] + over_x[1]) + (over_x[2] + over_x[3])
    out_ref[...] = jnp.full((1, 1), 0.5 * jnp.sum(total), jnp.float32)


def solution(mesh):
    vmem = pl.BlockSpec(memory_space=pltpu.VMEM)
    smem = pl.BlockSpec(memory_space=pltpu.SMEM)
    f32, i32 = jnp.float32, jnp.int32

    def shape(dims, dtype=f32):
        return jax.ShapeDtypeStruct(dims, dtype)

    exchange = pl.pallas_call(
        exchange_kernel,
        out_shape=(shape((9, PAD)), shape((8, 4, PAD)), shape((8, 8, MIG))),
        in_specs=[vmem] * 5 + [smem],
        out_specs=(vmem, vmem, vmem),
        scratch_shapes=[pltpu.VMEM((9, PAD), f32), pltpu.SemaphoreType.DMA((2, 8)), pltpu.SemaphoreType.DMA((2, 8))],
        compiler_params=pltpu.CompilerParams(collective_id=0, has_side_effects=True),
        name="exchange",
    )
    forces = pl.pallas_call(
        force_kernel,
        out_shape=(shape((3, CAP)), shape((3, CAP)), shape((3, CAP)), shape((1, CAP), i32), shape((1, CAP), i32), shape((8, 128))),
        in_specs=[vmem] * 3 + [smem],
        out_specs=(vmem,) * 6,
        scratch_shapes=[pltpu.VMEM((8, FULL), f32), pltpu.VMEM((4, 9 * PAD), f32), pltpu.VMEM((3, PAD, 128), f32), pltpu.VMEM((3, PAD, 128), f32)],
        name="forces",
    )
    total_energy = pl.pallas_call(
        energy_kernel,
        out_shape=shape((1, 1)),
        in_specs=[vmem],
        out_specs=vmem,
        scratch_shapes=[pltpu.VMEM((8, 8, 128), f32), pltpu.SemaphoreType.DMA((8,)), pltpu.SemaphoreType.DMA((8,))],
        compiler_params=pltpu.CompilerParams(collective_id=1, has_side_effects=True),
        name="energy",
    )

    def local_step(atom_pos, atom_vel, atom_frc, atom_id, atom_ok, brick_side):
        side = brick_side.reshape(1, 1)
        own, everyone, movers = exchange(atom_pos.T, atom_vel.T, atom_frc.T, atom_id.reshape(1, CAP), atom_ok.reshape(1, CAP), side)
        pos, vel, frc, new_id, new_ok, partial = forces(own, everyone, movers, side)
        energy = total_energy(partial)
        return pos.T, vel.T, frc.T, new_id.reshape(CAP), new_ok.reshape(CAP), energy.reshape(())

    row_spec = P(MESH_AXES, None)
    id_spec = P(MESH_AXES)
    return jax.shard_map(local_step, mesh=mesh, in_specs=(row_spec, row_spec, row_spec, id_spec, id_spec, P()), out_specs=(row_spec, row_spec, row_spec, id_spec, id_spec, P()), check_vma=False)
```

```python
import functools

import jax
import jax.numpy as jnp
from jax import lax
from jax.experimental import pallas as pl
from jax.experimental.pallas import tpu as pltpu
from jax.sharding import PartitionSpec as P

DT = 0.005
RC = 2.5
FAR_AWAY = 1.0e6
UCUT = 4.0 * (RC ** -12 - RC ** -6)
UPC = -48.0 * RC ** -13 + 24.0 * RC ** -7
MESH_AXES = ("z", "y", "x")
CAP = 729
PAD = 768
MIG = 256
FULL = PAD + MIG
SEG = {1: (0, 16), 2: (16, 16), 4: (32, 16), 3: (48, 32), 5: (80, 32), 6: (128, 32), 7: (160, 64)}
IC = 32
REACH = RC + 0.01
MESH_ID = pl.DeviceIdType.MESH


def pieces_of(rows):
    first = rows.astype(jnp.bfloat16).astype(jnp.float32)
    rest = rows - first
    second = rest.astype(jnp.bfloat16).astype(jnp.float32)
    third = rest - second
    return jnp.concatenate([first, second, third], axis=0).astype(jnp.bfloat16)


def select_rows(rows, onehot):
    out = lax.dot_general(pieces_of(rows), onehot, (((1,), (1,)), ((), ())), preferred_element_type=jnp.float32)
    return out[0:8] + out[8:16] + out[16:24]


def partner(relation):
    mine = (lax.axis_index("z"), lax.axis_index("y"), lax.axis_index("x"))
    bits = (relation // 4 % 2, relation // 2 % 2, relation % 2)
    return tuple((axis + bit) % 2 for axis, bit in zip(mine, bits))


def greet():
    barrier = pltpu.get_barrier_semaphore()
    for relation in range(1, 8):
        pl.semaphore_signal(barrier, inc=1, device_id=partner(relation), device_id_type=MESH_ID)
    return barrier


def axis_column(values, rows):
    idx = lax.broadcasted_iota(jnp.int32, (rows, 1), 0)
    out = jnp.full((rows, 1), values[-1], jnp.float32)
    for k in range(len(values) - 1):
        out = jnp.where(idx == k, values[k], out)
    return out


def brick_coords():
    return [lax.axis_index(name).astype(jnp.float32) for name in ("x", "y", "z")]


def prefix_counts(member):
    blocks = PAD // 128
    stacked = jnp.concatenate([member[:, 128 * b:128 * (b + 1)] for b in range(blocks)], axis=0).astype(jnp.bfloat16)
    row = lax.broadcasted_iota(jnp.int32, (128, 256), 0)
    col = lax.broadcasted_iota(jnp.int32, (128, 256), 1)
    ladder = ((row < col) | (col >= 128)).astype(jnp.float32).astype(jnp.bfloat16)
    counts = jnp.dot(stacked, ladder, preferred_element_type=jnp.float32)
    before = jnp.zeros((8, 128), jnp.float32)
    ranks = []
    for b in range(blocks):
        ranks.append(counts[8 * b:8 * b + 8, 0:128] + before)
        before = before + counts[8 * b:8 * b + 8, 128:256]
    return jnp.concatenate(ranks, axis=1), before


def exchange_kernel(pos_hbm, vel_hbm, frc_hbm, id_hbm, ok_hbm, side_ref, own_ref, all_ref, mig_ref, pos_ref, vel_ref, frc_ref, id_ref, ok_ref, pad_ref, load_sem, send_sem, recv_sem):
    loads = []
    for k, (src, dst) in enumerate(((pos_hbm, pos_ref), (vel_hbm, vel_ref), (frc_hbm, frc_ref), (id_hbm, id_ref), (ok_hbm, ok_ref))):
        load = pltpu.make_async_copy(src, dst, load_sem.at[k])
        load.start()
        loads.append(load)
    barrier = greet()
    side = side_ref[0, 0]
    box = side * 2.0
    pad_ref[...] = jnp.zeros_like(pad_ref)
    for load in loads:
        load.wait()
    half_v = vel_ref[...] + (0.5 * DT) * frc_ref[...]
    pad_ref[0:3, 0:CAP] = pos_ref[...] + DT * half_v
    pad_ref[3:6, 0:CAP] = half_v
    pad_ref[6:7, 0:CAP] = (id_ref[...].reshape(1, CAP) >> 16).astype(jnp.float32) + 1.0
    pad_ref[7:8, 0:CAP] = (id_ref[...].reshape(1, CAP) & 65535).astype(jnp.float32)
    pad_ref[8:9, 0:CAP] = ok_ref[...].reshape(1, CAP).astype(jnp.float32)
    unwrapped = pad_ref[0:3, :]
    owned = pad_ref[8:9, :] > 0.5
    moved = jnp.where(unwrapped < 0.0, unwrapped + box, jnp.where(unwrapped >= box, unwrapped - box, unwrapped))
    all_ref[0, 0:3, :] = jnp.where(owned, moved, FAR_AWAY)
    all_ref[0, 3:4, :] = jnp.zeros((1, PAD), jnp.float32)

    pl.semaphore_wait(barrier, 7)
    copies = []
    for relation in range(1, 8):
        copy = pltpu.make_async_remote_copy(src_ref=all_ref.at[0], dst_ref=all_ref.at[relation], send_sem=send_sem.at[0, relation], recv_sem=recv_sem.at[0, relation], device_id=partner(relation), device_id_type=MESH_ID)
        copy.start()
        copies.append(copy)

    low = axis_column([coord * side for coord in brick_coords()], 3)
    outside = (unwrapped < low) | (unwrapped >= low + side)
    bits = jnp.where(outside, axis_column([1.0, 2.0, 4.0], 3), 0.0)
    code = jnp.sum(bits, axis=0, keepdims=True)
    code = jnp.where(owned, code, -1.0)
    relation_col = lax.broadcasted_iota(jnp.int32, (8, PAD), 0).astype(jnp.float32)
    member = code == relation_col
    rank, _ = prefix_counts(member.astype(jnp.float32))
    offset = axis_column([0.0] + [float(SEG[m][0]) for m in range(1, 8)], 8)
    slot = jnp.sum(jnp.where(member, rank + offset, 0.0), axis=0, keepdims=True)
    slot = jnp.where(code > 0.5, slot, -1.0)
    rows = jnp.concatenate([moved, pad_ref[3:8, :]], axis=0)
    slots = lax.broadcasted_iota(jnp.int32, (MIG, PAD), 0).astype(jnp.float32)
    onehot = (slots == slot).astype(jnp.float32).astype(jnp.bfloat16)
    mig_ref[0] = select_rows(rows, onehot)
    for relation in range(1, 8):
        block = pl.ds(SEG[relation][0] // 128 * 128, 128)
        copy = pltpu.make_async_remote_copy(src_ref=mig_ref.at[0, :, block], dst_ref=mig_ref.at[relation, :, block], send_sem=send_sem.at[1, relation], recv_sem=recv_sem.at[1, relation], device_id=partner(relation), device_id_type=MESH_ID)
        copy.start()
        copies.append(copy)
    own_ref[0:8, :] = rows
    own_ref[8:9, :] = jnp.where(code == 0.0, rank[0:1, :], -1.0)
    for copy in copies:
        copy.wait()


def pair_terms(own, other, span):
    delta = []
    for mine, theirs in zip(own, other):
        diff = mine - theirs
        if span is not None:
            diff = diff - jnp.where(diff > 0.5 * span, span, jnp.where(diff < -0.5 * span, -span, 0.0))
        delta.append(diff)
    dist_sq = delta[0] * delta[0] + delta[1] * delta[1] + delta[2] * delta[2]
    in_range = (dist_sq < RC * RC) & (dist_sq > 0.01)
    inv_r = jnp.where(in_range, lax.rsqrt(dist_sq), 0.0)
    inv_r2 = inv_r * inv_r
    inv_r6 = inv_r2 * inv_r2 * inv_r2
    scale = (48.0 * inv_r6 - 24.0) * inv_r6 * inv_r2 + UPC * inv_r
    energy = 4.0 * inv_r6 * (inv_r6 - 1.0) - UPC * (dist_sq * inv_r) - jnp.where(in_range, UCUT - RC * UPC, 0.0)
    return [scale * d for d in delta], energy


def force_kernel(own_ref, all_ref, mig_ref, side_ref, pos_ref, vel_ref, frc_ref, id_ref, ok_ref, en_ref, cand_ref, near_ref, mine_ref, acc_ref, plane_ref, list_ref):
    side = side_ref[0, 0]
    box = side * 2.0
    lane = lax.broadcasted_iota(jnp.int32, (1, MIG), 1)
    arrivals = jnp.zeros((8, MIG), jnp.float32)
    for relation, (start, size) in SEG.items():
        arrivals = jnp.where((lane >= start) & (lane < start + size), mig_ref[relation], arrivals)
    cand_ref[:, 0:PAD] = own_ref[0:8, :]
    cand_ref[:, PAD:FULL] = arrivals
    stay_rank = own_ref[8:9, :]
    cand = cand_ref[...]
    valid = jnp.concatenate([stay_rank >= 0.0, arrivals[6:7, :] > 0.5], axis=1)
    number = (cand[6:7, :].astype(jnp.int32) - 1) * 65536 + cand[7:8, :].astype(jnp.int32)
    key = jnp.where(valid, number, 2147483647)
    key_col = jnp.transpose(jnp.broadcast_to(key, (8, FULL)))[:, 0:1]
    in_front = jnp.sum((key_col[PAD:FULL] < key).astype(jnp.float32), axis=0, keepdims=True)
    behind = jnp.sum((key_col[0:PAD] < key[:, PAD:FULL]).astype(jnp.float32), axis=0, keepdims=True)
    rank = in_front + jnp.concatenate([stay_rank, behind], axis=1)
    rank = jnp.where(valid, rank, -1.0)
    slots = lax.broadcasted_iota(jnp.int32, (PAD, FULL), 0).astype(jnp.float32)
    onehot = (slots == rank).astype(jnp.float32).astype(jnp.bfloat16)
    rows = select_rows(cand, onehot)
    filled = rows[6:7, :] > 0.5
    total = jnp.sum(filled.astype(jnp.int32))

    centre = [(coord + 0.5) * side for coord in brick_coords()]
    local = rows[0:3, :] - axis_column(centre, 3)
    local = jnp.where(filled, local, -FAR_AWAY)
    columns = jnp.transpose(jnp.concatenate([local, jnp.zeros((5, PAD), jnp.float32)], axis=0))
    for axis in range(3):
        mine_ref[axis] = jnp.broadcast_to(columns[:, axis:axis + 1], (PAD, 128))
    for relation in range(8):
        for axis in range(3):
            plane_ref[axis, relation:relation + 1, :] = all_ref[relation, axis:axis + 1, :]
    planes = []
    beyond = jnp.zeros((8, PAD), jnp.float32)
    for axis in range(3):
        theirs = plane_ref[axis] - centre[axis]
        theirs = jnp.where(theirs > side, theirs - box, jnp.where(theirs < -side, theirs + box, theirs))
        excess = jnp.maximum(jnp.abs(theirs) - 0.5 * side, 0.0)
        beyond = beyond + excess * excess
        planes.append(theirs)
    keep = beyond < REACH * REACH
    front, held = prefix_counts(keep.astype(jnp.float32))
    lane8 = lax.broadcasted_iota(jnp.int32, (8, PAD), 1)
    hops = jnp.where(keep, lane8 - front.astype(jnp.int32), 0)
    for bit in range(10):
        step = 1 << bit
        coming = pltpu.roll(hops, PAD - step, 1)
        take = (coming & step) != 0
        leave = (hops & step) != 0
        hops = jnp.where(take, coming, jnp.where(leave, 0, hops))
        planes = [jnp.where(take, pltpu.roll(plane, PAD - step, 1), plane) for plane in planes]
    for relation in range(8):
        for axis in range(3):
            list_ref[relation, axis:axis + 1, 0:PAD] = planes[axis][relation:relation + 1, :]
    held = held.astype(jnp.int32)
    lane128 = lax.broadcasted_iota(jnp.int32, (8, 128), 1)
    start = 0
    for relation in range(8):
        into = start % 128
        first = pl.multiple_of(start - into, 128)
        turned = pltpu.roll(list_ref[relation], into, 1)
        near_ref[:, pl.ds(first, 128)] = jnp.where(lane128 < into, near_ref[:, pl.ds(first, 128)], turned[:, 0:128])
        near_ref[:, pl.ds(pl.multiple_of(first + 128, 128), PAD)] = turned[:, 128:PAD + 128]
        start = start + held[relation, 0]
    into = start % 128
    first = pl.multiple_of(start - into, 128)
    near_ref[:, pl.ds(first, 128)] = jnp.where(lane128 < into, near_ref[:, pl.ds(first, 128)], FAR_AWAY)
    near_ref[:, pl.ds(pl.multiple_of(first + 128, 128), 256)] = jnp.full((8, 256), FAR_AWAY, jnp.float32)
    n_other = (start + 255) // 256
    n_own = (total + IC - 1) // IC
    acc_ref[...] = jnp.zeros_like(acc_ref)
    en_ref[...] = jnp.zeros_like(en_ref)

    def sweep(span):
        def own_step(i, carry):
            first = pl.multiple_of(i * IC, IC)
            own = [mine_ref[axis, pl.ds(first, IC), :] for axis in range(3)]

            def other_step(j, sums):
                lanes = pl.multiple_of(j * 256, 256)
                for half in range(2):
                    other = [near_ref[axis:axis + 1, pl.ds(lanes + 128 * half, 128)] for axis in range(3)]
                    force, energy = pair_terms(own, other, span)
                    sums = tuple(s + t for s, t in zip(sums, force + [energy]))
                return sums

            zero = jnp.zeros((IC, 128), jnp.float32)
            sums = lax.fori_loop(0, n_other, other_step, (zero,) * 4)
            for axis in range(3):
                acc_ref[axis, pl.ds(first, IC), :] = sums[axis]
            energy = sums[3]
            en_ref[...] += energy[0:8] + energy[8:16] + energy[16:24] + energy[24:32]
            return carry

        lax.fori_loop(0, n_own, own_step, 0)

    @pl.when(side >= 2.0 * RC)
    def _():
        sweep(None)

    @pl.when(side < 2.0 * RC)
    def _():
        sweep(box)

    out_rows = []
    for axis in range(3):
        parts = []
        for b in range(PAD // 128):
            parts.append(jnp.sum(jnp.transpose(acc_ref[axis, 128 * b:128 * b + 128, :]), axis=0, keepdims=True))
        out_rows.append(jnp.concatenate(parts, axis=1))
    force = jnp.where(filled, jnp.concatenate(out_rows, axis=0), 0.0)
    frc_ref[...] = force[:, 0:CAP]
    pos_ref[...] = rows[0:3, 0:CAP]
    vel_ref[...] = (rows[3:6, :] + (0.5 * DT) * force)[:, 0:CAP]
    new_id = (rows[6:7, :].astype(jnp.int32) - 1) * 65536 + rows[7:8, :].astype(jnp.int32)
    id_ref[...] = jnp.where(filled, new_id, 0)[:, 0:CAP].reshape(CAP)
    ok_ref[...] = filled.astype(jnp.int32)[:, 0:CAP].reshape(CAP)


def energy_kernel(en_ref, out_ref, parts_ref, send_sem, recv_sem):
    barrier = greet()
    pl.semaphore_wait(barrier, 7)
    copies = []
    for relation in range(1, 8):
        copy = pltpu.make_async_remote_copy(src_ref=en_ref, dst_ref=parts_ref.at[relation], send_sem=send_sem.at[relation], recv_sem=recv_sem.at[relation], device_id=partner(relation), device_id_type=MESH_ID)
        copy.start()
        copies.append(copy)
    for copy in copies:
        copy.wait()
    parts_ref[0] = en_ref[...]
    over_x = [parts_ref[k] + parts_ref[k + 1] for k in (0, 2, 4, 6)]
    total = (over_x[0] + over_x[1]) + (over_x[2] + over_x[3])
    out_ref[...] = jnp.full((1, 1), 0.5 * jnp.sum(total), jnp.float32)


def solution(mesh):
    vmem = pl.BlockSpec(memory_space=pltpu.VMEM)
    hbm = pl.BlockSpec(memory_space=pltpu.HBM)
    smem = pl.BlockSpec(memory_space=pltpu.SMEM)
    f32, i32 = jnp.float32, jnp.int32

    def shape(dims, dtype=f32):
        return jax.ShapeDtypeStruct(dims, dtype)

    exchange = pl.pallas_call(
        exchange_kernel,
        out_shape=(shape((9, PAD)), shape((8, 4, PAD)), shape((8, 8, MIG))),
        in_specs=[hbm] * 5 + [smem],
        out_specs=(vmem, vmem, vmem),
        scratch_shapes=[pltpu.VMEM((3, CAP), f32)] * 3 + [pltpu.VMEM((CAP,), i32)] * 2 + [pltpu.VMEM((9, PAD), f32), pltpu.SemaphoreType.DMA((5,)), pltpu.SemaphoreType.DMA((2, 8)), pltpu.SemaphoreType.DMA((2, 8))],
        compiler_params=pltpu.CompilerParams(collective_id=0, has_side_effects=True, vmem_limit_bytes=16 << 20),
        name="exchange",
    )
    forces = pl.pallas_call(
        force_kernel,
        out_shape=(shape((3, CAP)), shape((3, CAP)), shape((3, CAP)), shape((CAP,), i32), shape((CAP,), i32), shape((8, 128))),
        in_specs=[vmem] * 3 + [smem],
        out_specs=(vmem,) * 6,
        scratch_shapes=[pltpu.VMEM((8, FULL), f32), pltpu.VMEM((8, 9 * PAD + 256), f32), pltpu.VMEM((3, PAD, 128), f32), pltpu.VMEM((3, PAD, 128), f32), pltpu.VMEM((3, 8, PAD), f32), pltpu.VMEM((8, 8, PAD + 128), f32)],
        compiler_params=pltpu.CompilerParams(vmem_limit_bytes=16 << 20),
        name="forces",
    )
    total_energy = pl.pallas_call(
        energy_kernel,
        out_shape=shape((1, 1)),
        in_specs=[vmem],
        out_specs=vmem,
        scratch_shapes=[pltpu.VMEM((8, 8, 128), f32), pltpu.SemaphoreType.DMA((8,)), pltpu.SemaphoreType.DMA((8,))],
        compiler_params=pltpu.CompilerParams(collective_id=1, has_side_effects=True, vmem_limit_bytes=16 << 20),
        name="energy",
    )

    def local_step(atom_pos, atom_vel, atom_frc, atom_id, atom_ok, brick_side):
        side = brick_side.reshape(1, 1)
        own, everyone, movers = exchange(atom_pos.T, atom_vel.T, atom_frc.T, atom_id, atom_ok, side)
        pos, vel, frc, new_id, new_ok, partial = forces(own, everyone, movers, side)
        energy = total_energy(partial)
        return pos.T, vel.T, frc.T, new_id, new_ok, energy.reshape(())

    row_spec = P(MESH_AXES, None)
    id_spec = P(MESH_AXES)
    return jax.shard_map(local_step, mesh=mesh, in_specs=(row_spec, row_spec, row_spec, id_spec, id_spec, P()), out_specs=(row_spec, row_spec, row_spec, id_spec, id_spec, P()), check_vma=False)
```

```python
import functools

import jax
import jax.numpy as jnp
from jax import lax
from jax.experimental import pallas as pl
from jax.experimental.pallas import tpu as pltpu
from jax.sharding import PartitionSpec as P

DT = 0.005
RC = 2.5
FAR_AWAY = 1.0e6
UCUT = 4.0 * (RC ** -12 - RC ** -6)
UPC = -48.0 * RC ** -13 + 24.0 * RC ** -7
MESH_AXES = ("z", "y", "x")
CAP = 729
PAD = 768
MIG = 256
FULL = PAD + MIG
SEG = {1: (0, 16), 2: (16, 16), 4: (32, 16), 3: (48, 32), 5: (80, 32), 6: (128, 32), 7: (160, 64)}
IC = 32
REACH = RC + 0.01
MESH_ID = pl.DeviceIdType.MESH


def pieces_of(rows):
    first = rows.astype(jnp.bfloat16).astype(jnp.float32)
    rest = rows - first
    second = rest.astype(jnp.bfloat16).astype(jnp.float32)
    third = rest - second
    return jnp.concatenate([first, second, third], axis=0).astype(jnp.bfloat16)


def select_rows(rows, onehot):
    out = lax.dot_general(pieces_of(rows), onehot, (((1,), (1,)), ((), ())), preferred_element_type=jnp.float32)
    return out[0:8] + out[8:16] + out[16:24]


def partner(relation):
    mine = (lax.axis_index("z"), lax.axis_index("y"), lax.axis_index("x"))
    bits = (relation // 4 % 2, relation // 2 % 2, relation % 2)
    return tuple((axis + bit) % 2 for axis, bit in zip(mine, bits))


def greet():
    barrier = pltpu.get_barrier_semaphore()
    for relation in range(1, 8):
        pl.semaphore_signal(barrier, inc=1, device_id=partner(relation), device_id_type=MESH_ID)
    return barrier


def axis_column(values, rows):
    idx = lax.broadcasted_iota(jnp.int32, (rows, 1), 0)
    out = jnp.full((rows, 1), values[-1], jnp.float32)
    for k in range(len(values) - 1):
        out = jnp.where(idx == k, values[k], out)
    return out


def brick_coords():
    return [lax.axis_index(name).astype(jnp.float32) for name in ("x", "y", "z")]


def prefix_counts(member):
    blocks = PAD // 128
    stacked = jnp.concatenate([member[:, 128 * b:128 * (b + 1)] for b in range(blocks)], axis=0).astype(jnp.bfloat16)
    row = lax.broadcasted_iota(jnp.int32, (128, 256), 0)
    col = lax.broadcasted_iota(jnp.int32, (128, 256), 1)
    ladder = ((row < col) | (col >= 128)).astype(jnp.float32).astype(jnp.bfloat16)
    counts = jnp.dot(stacked, ladder, preferred_element_type=jnp.float32)
    before = jnp.zeros((8, 128), jnp.float32)
    ranks = []
    for b in range(blocks):
        ranks.append(counts[8 * b:8 * b + 8, 0:128] + before)
        before = before + counts[8 * b:8 * b + 8, 128:256]
    return jnp.concatenate(ranks, axis=1), before


def exchange_kernel(pos_hbm, vel_hbm, frc_hbm, id_hbm, ok_hbm, side_ref, own_ref, all_ref, mig_ref, pos_ref, vel_ref, frc_ref, id_ref, ok_ref, pad_ref, load_sem, send_sem, recv_sem):
    loads = []
    for k, (src, dst) in enumerate(((pos_hbm, pos_ref), (vel_hbm, vel_ref), (frc_hbm, frc_ref), (id_hbm, id_ref), (ok_hbm, ok_ref))):
        load = pltpu.make_async_copy(src, dst, load_sem.at[k])
        load.start()
        loads.append(load)
    barrier = greet()
    side = side_ref[0, 0]
    box = side * 2.0
    pad_ref[...] = jnp.zeros_like(pad_ref)
    for load in loads:
        load.wait()
    half_v = vel_ref[...] + (0.5 * DT) * frc_ref[...]
    pad_ref[0:3, 0:CAP] = pos_ref[...] + DT * half_v
    pad_ref[3:6, 0:CAP] = half_v
    pad_ref[6:7, 0:CAP] = (id_ref[...].reshape(1, CAP) >> 16).astype(jnp.float32) + 1.0
    pad_ref[7:8, 0:CAP] = (id_ref[...].reshape(1, CAP) & 65535).astype(jnp.float32)
    pad_ref[8:9, 0:CAP] = ok_ref[...].reshape(1, CAP).astype(jnp.float32)
    unwrapped = pad_ref[0:3, :]
    owned = pad_ref[8:9, :] > 0.5
    moved = jnp.where(unwrapped < 0.0, unwrapped + box, jnp.where(unwrapped >= box, unwrapped - box, unwrapped))
    all_ref[0, 0:3, :] = jnp.where(owned, moved, FAR_AWAY)
    all_ref[0, 3:4, :] = jnp.zeros((1, PAD), jnp.float32)

    pl.semaphore_wait(barrier, 7)
    copies = []
    for relation in range(1, 8):
        copy = pltpu.make_async_remote_copy(src_ref=all_ref.at[0], dst_ref=all_ref.at[relation], send_sem=send_sem.at[0, relation], recv_sem=recv_sem.at[0, relation], device_id=partner(relation), device_id_type=MESH_ID)
        copy.start()
        copies.append(copy)

    low = axis_column([coord * side for coord in brick_coords()], 3)
    outside = (unwrapped < low) | (unwrapped >= low + side)
    bits = jnp.where(outside, axis_column([1.0, 2.0, 4.0], 3), 0.0)
    code = jnp.sum(bits, axis=0, keepdims=True)
    code = jnp.where(owned, code, -1.0)
    relation_col = lax.broadcasted_iota(jnp.int32, (8, PAD), 0).astype(jnp.float32)
    member = code == relation_col
    rank, _ = prefix_counts(member.astype(jnp.float32))
    offset = axis_column([0.0] + [float(SEG[m][0]) for m in range(1, 8)], 8)
    slot = jnp.sum(jnp.where(member, rank + offset, 0.0), axis=0, keepdims=True)
    slot = jnp.where(code > 0.5, slot, -1.0)
    rows = jnp.concatenate([moved, pad_ref[3:8, :]], axis=0)
    slots = lax.broadcasted_iota(jnp.int32, (MIG, PAD), 0).astype(jnp.float32)
    onehot = (slots == slot).astype(jnp.float32).astype(jnp.bfloat16)
    mig_ref[0] = select_rows(rows, onehot)
    for relation in range(1, 8):
        block = pl.ds(SEG[relation][0] // 128 * 128, 128)
        copy = pltpu.make_async_remote_copy(src_ref=mig_ref.at[0, :, block], dst_ref=mig_ref.at[relation, :, block], send_sem=send_sem.at[1, relation], recv_sem=recv_sem.at[1, relation], device_id=partner(relation), device_id_type=MESH_ID)
        copy.start()
        copies.append(copy)
    own_ref[0:8, :] = rows
    own_ref[8:9, :] = jnp.where(code == 0.0, rank[0:1, :], -1.0)
    for copy in copies:
        copy.wait()


def pair_terms(own, other, span):
    delta = []
    for mine, theirs in zip(own, other):
        diff = mine - theirs
        if span is not None:
            diff = diff - jnp.where(diff > 0.5 * span, span, jnp.where(diff < -0.5 * span, -span, 0.0))
        delta.append(diff)
    dist_sq = delta[0] * delta[0] + delta[1] * delta[1] + delta[2] * delta[2]
    in_range = (dist_sq < RC * RC) & (dist_sq > 0.01)
    inv_r = jnp.where(in_range, lax.rsqrt(dist_sq), 0.0)
    inv_r2 = inv_r * inv_r
    inv_r6 = inv_r2 * inv_r2 * inv_r2
    scale = (48.0 * inv_r6 - 24.0) * inv_r6 * inv_r2 + UPC * inv_r
    energy = 4.0 * inv_r6 * (inv_r6 - 1.0) - UPC * (dist_sq * inv_r) - jnp.where(in_range, UCUT - RC * UPC, 0.0)
    return [scale * d for d in delta], energy


def force_kernel(own_ref, all_ref, mig_ref, side_ref, pos_ref, vel_ref, frc_ref, id_ref, ok_ref, en_ref, cand_ref, near_ref, mine_ref, acc_ref, plane_ref, list_ref):
    side = side_ref[0, 0]
    box = side * 2.0
    lane = lax.broadcasted_iota(jnp.int32, (1, MIG), 1)
    arrivals = jnp.zeros((8, MIG), jnp.float32)
    for relation, (start, size) in SEG.items():
        arrivals = jnp.where((lane >= start) & (lane < start + size), mig_ref[relation], arrivals)
    cand_ref[:, 0:PAD] = own_ref[0:8, :]
    cand_ref[:, PAD:FULL] = arrivals
    stay_rank = own_ref[8:9, :]
    cand = cand_ref[...]
    valid = jnp.concatenate([stay_rank >= 0.0, arrivals[6:7, :] > 0.5], axis=1)
    number = (cand[6:7, :].astype(jnp.int32) - 1) * 65536 + cand[7:8, :].astype(jnp.int32)
    key = jnp.where(valid, number, 2147483647)
    key_col = jnp.transpose(jnp.broadcast_to(key, (8, FULL)))[:, 0:1]
    in_front = jnp.sum((key_col[PAD:FULL] < key).astype(jnp.float32), axis=0, keepdims=True)
    behind = jnp.sum((key_col[0:PAD] < key[:, PAD:FULL]).astype(jnp.float32), axis=0, keepdims=True)
    rank = in_front + jnp.concatenate([stay_rank, behind], axis=1)
    rank = jnp.where(valid, rank, -1.0)
    slots = lax.broadcasted_iota(jnp.int32, (PAD, FULL), 0).astype(jnp.float32)
    onehot = (slots == rank).astype(jnp.float32).astype(jnp.bfloat16)
    rows = select_rows(cand, onehot)
    filled = rows[6:7, :] > 0.5
    total = jnp.sum(filled.astype(jnp.int32))

    centre = [(coord + 0.5) * side for coord in brick_coords()]
    local = rows[0:3, :] - axis_column(centre, 3)
    local = jnp.where(filled, local, -FAR_AWAY)
    columns = jnp.transpose(jnp.concatenate([local, jnp.zeros((5, PAD), jnp.float32)], axis=0))
    for axis in range(3):
        mine_ref[axis] = jnp.broadcast_to(columns[:, axis:axis + 1], (PAD, 128))
    for relation in range(8):
        for axis in range(3):
            plane_ref[axis, relation:relation + 1, :] = all_ref[relation, axis:axis + 1, :]
    planes = []
    beyond = jnp.zeros((8, PAD), jnp.float32)
    for axis in range(3):
        theirs = plane_ref[axis] - centre[axis]
        theirs = jnp.where(theirs > side, theirs - box, jnp.where(theirs < -side, theirs + box, theirs))
        excess = jnp.maximum(jnp.abs(theirs) - 0.5 * side, 0.0)
        beyond = beyond + excess * excess
        planes.append(theirs)
    keep = beyond < REACH * REACH
    front, held = prefix_counts(keep.astype(jnp.float32))
    lane8 = lax.broadcasted_iota(jnp.int32, (8, PAD), 1)
    hops = jnp.where(keep, lane8 - front.astype(jnp.int32), 0)
    for bit in range(10):
        step = 1 << bit
        coming = pltpu.roll(hops, PAD - step, 1)
        take = (coming & step) != 0
        leave = (hops & step) != 0
        hops = jnp.where(take, coming, jnp.where(leave, 0, hops))
        planes = [jnp.where(take, pltpu.roll(plane, PAD - step, 1), plane) for plane in planes]
    for relation in range(8):
        for axis in range(3):
            list_ref[relation, axis:axis + 1, 0:PAD] = planes[axis][relation:relation + 1, :]
    held = held.astype(jnp.int32)
    lane128 = lax.broadcasted_iota(jnp.int32, (8, 128), 1)
    start = 0
    for relation in range(8):
        into = start % 128
        first = pl.multiple_of(start - into, 128)
        turned = pltpu.roll(list_ref[relation], into, 1)
        near_ref[:, pl.ds(first, 128)] = jnp.where(lane128 < into, near_ref[:, pl.ds(first, 128)], turned[:, 0:128])
        near_ref[:, pl.ds(pl.multiple_of(first + 128, 128), PAD)] = turned[:, 128:PAD + 128]
        start = start + held[relation, 0]
    into = start % 128
    first = pl.multiple_of(start - into, 128)
    near_ref[:, pl.ds(first, 128)] = jnp.where(lane128 < into, near_ref[:, pl.ds(first, 128)], FAR_AWAY)
    near_ref[:, pl.ds(pl.multiple_of(first + 128, 128), 256)] = jnp.full((8, 256), FAR_AWAY, jnp.float32)
    n_other = (start + 255) // 256
    n_own = (total + IC - 1) // IC
    acc_ref[...] = jnp.zeros_like(acc_ref)
    en_ref[...] = jnp.zeros_like(en_ref)

    def sweep(span):
        def own_step(i, carry):
            first = pl.multiple_of(i * IC, IC)
            own = [mine_ref[axis, pl.ds(first, IC), :] for axis in range(3)]

            def other_step(j, sums):
                lanes = pl.multiple_of(j * 256, 256)
                for half in range(2):
                    other = [near_ref[axis:axis + 1, pl.ds(lanes + 128 * half, 128)] for axis in range(3)]
                    force, energy = pair_terms(own, other, span)
                    sums = tuple(s + t for s, t in zip(sums, force + [energy]))
                return sums

            zero = jnp.zeros((IC, 128), jnp.float32)
            sums = lax.fori_loop(0, n_other, other_step, (zero,) * 4)
            for axis in range(3):
                acc_ref[axis, pl.ds(first, IC), :] = sums[axis]
            energy = sums[3]
            en_ref[...] += energy[0:8] + energy[8:16] + energy[16:24] + energy[24:32]
            return carry

        lax.fori_loop(0, n_own, own_step, 0)

    @pl.when(side >= 2.0 * RC)
    def _():
        sweep(None)

    @pl.when(side < 2.0 * RC)
    def _():
        sweep(box)

    out_rows = []
    for axis in range(3):
        parts = []
        for b in range(PAD // 128):
            parts.append(jnp.sum(jnp.transpose(acc_ref[axis, 128 * b:128 * b + 128, :]), axis=0, keepdims=True))
        out_rows.append(jnp.concatenate(parts, axis=1))
    force = jnp.where(filled, jnp.concatenate(out_rows, axis=0), 0.0)
    frc_ref[...] = force[:, 0:CAP]
    pos_ref[...] = rows[0:3, 0:CAP]
    vel_ref[...] = (rows[3:6, :] + (0.5 * DT) * force)[:, 0:CAP]
    new_id = (rows[6:7, :].astype(jnp.int32) - 1) * 65536 + rows[7:8, :].astype(jnp.int32)
    id_ref[...] = jnp.where(filled, new_id, 0)[:, 0:CAP].reshape(CAP)
    ok_ref[...] = filled.astype(jnp.int32)[:, 0:CAP].reshape(CAP)


def energy_kernel(en_ref, out_ref, parts_ref, send_sem, recv_sem):
    barrier = greet()
    pl.semaphore_wait(barrier, 7)
    copies = []
    for relation in range(1, 8):
        copy = pltpu.make_async_remote_copy(src_ref=en_ref, dst_ref=parts_ref.at[relation], send_sem=send_sem.at[relation], recv_sem=recv_sem.at[relation], device_id=partner(relation), device_id_type=MESH_ID)
        copy.start()
        copies.append(copy)
    for copy in copies:
        copy.wait()
    parts_ref[0] = en_ref[...]
    over_x = [parts_ref[k] + parts_ref[k + 1] for k in (0, 2, 4, 6)]
    total = (over_x[0] + over_x[1]) + (over_x[2] + over_x[3])
    out_ref[...] = jnp.full((1, 1), 0.5 * jnp.sum(total), jnp.float32)


def solution(mesh):
    vmem = pl.BlockSpec(memory_space=pltpu.VMEM)
    hbm = pl.BlockSpec(memory_space=pltpu.HBM)
    smem = pl.BlockSpec(memory_space=pltpu.SMEM)
    f32, i32 = jnp.float32, jnp.int32

    def shape(dims, dtype=f32):
        return jax.ShapeDtypeStruct(dims, dtype)

    exchange = pl.pallas_call(
        exchange_kernel,
        out_shape=(shape((9, PAD)), shape((8, 4, PAD)), shape((8, 8, MIG))),
        in_specs=[hbm] * 5 + [smem],
        out_specs=(vmem, vmem, vmem),
        scratch_shapes=[pltpu.VMEM((3, CAP), f32)] * 3 + [pltpu.VMEM((CAP,), i32)] * 2 + [pltpu.VMEM((9, PAD), f32), pltpu.SemaphoreType.DMA((5,)), pltpu.SemaphoreType.DMA((2, 8)), pltpu.SemaphoreType.DMA((2, 8))],
        compiler_params=pltpu.CompilerParams(collective_id=0, has_side_effects=True, vmem_limit_bytes=16 << 20),
        name="exchange",
    )
    forces = pl.pallas_call(
        force_kernel,
        out_shape=(shape((3, CAP)), shape((3, CAP)), shape((3, CAP)), shape((CAP,), i32), shape((CAP,), i32), shape((8, 128))),
        in_specs=[vmem] * 3 + [smem],
        out_specs=(vmem,) * 6,
        scratch_shapes=[pltpu.VMEM((8, FULL), f32), pltpu.VMEM((8, 9 * PAD + 256), f32), pltpu.VMEM((3, PAD, 128), f32), pltpu.VMEM((3, PAD, 128), f32), pltpu.VMEM((3, 8, PAD), f32), pltpu.VMEM((8, 8, PAD + 128), f32)],
        compiler_params=pltpu.CompilerParams(vmem_limit_bytes=16 << 20),
        name="forces",
    )
    total_energy = pl.pallas_call(
        energy_kernel,
        out_shape=shape((1, 1)),
        in_specs=[vmem],
        out_specs=vmem,
        scratch_shapes=[pltpu.VMEM((8, 8, 128), f32), pltpu.SemaphoreType.DMA((8,)), pltpu.SemaphoreType.DMA((8,))],
        compiler_params=pltpu.CompilerParams(collective_id=1, has_side_effects=True, vmem_limit_bytes=16 << 20),
        name="energy",
    )

    def local_step(atom_pos, atom_vel, atom_frc, atom_id, atom_ok, brick_side):
        side = brick_side.reshape(1, 1)
        own, everyone, movers = exchange(*[pltpu.with_memory_space_constraint(a, pltpu.HBM) for a in (atom_pos.T, atom_vel.T, atom_frc.T, atom_id, atom_ok)], side)
        pos, vel, frc, new_id, new_ok, partial = forces(own, everyone, movers, side)
        energy = total_energy(partial)
        return pos.T, vel.T, frc.T, new_id, new_ok, energy.reshape(())

    row_spec = P(MESH_AXES, None)
    id_spec = P(MESH_AXES)
    return jax.shard_map(local_step, mesh=mesh, in_specs=(row_spec, row_spec, row_spec, id_spec, id_spec, P()), out_specs=(row_spec, row_spec, row_spec, id_spec, id_spec, P()), check_vma=False)
```

```python
import functools

import jax
import jax.numpy as jnp
from jax import lax
from jax.experimental import pallas as pl
from jax.experimental.pallas import tpu as pltpu
from jax.sharding import PartitionSpec as P

DT = 0.005
RC = 2.5
FAR_AWAY = 1.0e6
UCUT = 4.0 * (RC ** -12 - RC ** -6)
UPC = -48.0 * RC ** -13 + 24.0 * RC ** -7
MESH_AXES = ("z", "y", "x")
CAP = 729
PAD = 768
MIG = 256
FULL = PAD + MIG
SEG = {1: (0, 16), 2: (16, 16), 4: (32, 16), 3: (48, 32), 5: (80, 32), 6: (128, 32), 7: (160, 64)}
IC = 32
FAR_FIRST = (6, 7, 4, 2, 5, 3, 1)
REACH = RC + 0.01
MESH_ID = pl.DeviceIdType.MESH


def pieces_of(rows):
    first = rows.astype(jnp.bfloat16).astype(jnp.float32)
    rest = rows - first
    second = rest.astype(jnp.bfloat16).astype(jnp.float32)
    third = rest - second
    return jnp.concatenate([first, second, third], axis=0).astype(jnp.bfloat16)


def select_rows(rows, onehot):
    out = lax.dot_general(pieces_of(rows), onehot, (((1,), (1,)), ((), ())), preferred_element_type=jnp.float32)
    return out[0:8] + out[8:16] + out[16:24]


def partner(relation):
    mine = (lax.axis_index("z"), lax.axis_index("y"), lax.axis_index("x"))
    bits = (relation // 4 % 2, relation // 2 % 2, relation % 2)
    return tuple((axis + bit) % 2 for axis, bit in zip(mine, bits))


def greet():
    barrier = pltpu.get_barrier_semaphore()
    for relation in range(1, 8):
        pl.semaphore_signal(barrier, inc=1, device_id=partner(relation), device_id_type=MESH_ID)
    return barrier


def axis_column(values, rows):
    idx = lax.broadcasted_iota(jnp.int32, (rows, 1), 0)
    out = jnp.full((rows, 1), values[-1], jnp.float32)
    for k in range(len(values) - 1):
        out = jnp.where(idx == k, values[k], out)
    return out


def brick_coords():
    return [lax.axis_index(name).astype(jnp.float32) for name in ("x", "y", "z")]


def prefix_counts(member):
    blocks = PAD // 128
    stacked = jnp.concatenate([member[:, 128 * b:128 * (b + 1)] for b in range(blocks)], axis=0).astype(jnp.bfloat16)
    row = lax.broadcasted_iota(jnp.int32, (128, 256), 0)
    col = lax.broadcasted_iota(jnp.int32, (128, 256), 1)
    ladder = ((row < col) | (col >= 128)).astype(jnp.float32).astype(jnp.bfloat16)
    counts = jnp.dot(stacked, ladder, preferred_element_type=jnp.float32)
    before = jnp.zeros((8, 128), jnp.float32)
    ranks = []
    for b in range(blocks):
        ranks.append(counts[8 * b:8 * b + 8, 0:128] + before)
        before = before + counts[8 * b:8 * b + 8, 128:256]
    return jnp.concatenate(ranks, axis=1), before


def exchange_kernel(pos_hbm, vel_hbm, frc_hbm, id_hbm, ok_hbm, side_ref, own_ref, all_ref, mig_ref, pos_ref, vel_ref, frc_ref, id_ref, ok_ref, pad_ref, load_sem, send_sem, recv_sem):
    loads = []
    for k, (src, dst) in enumerate(((pos_hbm, pos_ref), (vel_hbm, vel_ref), (frc_hbm, frc_ref), (id_hbm, id_ref), (ok_hbm, ok_ref))):
        load = pltpu.make_async_copy(src, dst, load_sem.at[k])
        load.start()
        loads.append(load)
    barrier = greet()
    side = side_ref[0, 0]
    box = side * 2.0
    pad_ref[...] = jnp.zeros_like(pad_ref)
    for load in loads:
        load.wait()
    half_v = vel_ref[...] + (0.5 * DT) * frc_ref[...]
    pad_ref[0:3, 0:CAP] = pos_ref[...] + DT * half_v
    pad_ref[3:6, 0:CAP] = half_v
    pad_ref[6:7, 0:CAP] = (id_ref[...].reshape(1, CAP) >> 16).astype(jnp.float32) + 1.0
    pad_ref[7:8, 0:CAP] = (id_ref[...].reshape(1, CAP) & 65535).astype(jnp.float32)
    pad_ref[8:9, 0:CAP] = ok_ref[...].reshape(1, CAP).astype(jnp.float32)
    unwrapped = pad_ref[0:3, :]
    owned = pad_ref[8:9, :] > 0.5
    moved = jnp.where(unwrapped < 0.0, unwrapped + box, jnp.where(unwrapped >= box, unwrapped - box, unwrapped))
    for axis in range(3):
        all_ref[0, :, PAD * axis:PAD * (axis + 1)] = jnp.where(owned, moved[axis:axis + 1, :], FAR_AWAY)

    low = axis_column([coord * side for coord in brick_coords()], 3)
    outside = (unwrapped < low) | (unwrapped >= low + side)
    bits = jnp.where(outside, axis_column([1.0, 2.0, 4.0], 3), 0.0)
    code = jnp.sum(bits, axis=0, keepdims=True)
    code = jnp.where(owned, code, -1.0)
    relation_col = lax.broadcasted_iota(jnp.int32, (8, PAD), 0).astype(jnp.float32)
    member = code == relation_col
    rank, _ = prefix_counts(member.astype(jnp.float32))
    offset = axis_column([0.0] + [float(SEG[m][0]) for m in range(1, 8)], 8)
    slot = jnp.sum(jnp.where(member, rank + offset, 0.0), axis=0, keepdims=True)
    slot = jnp.where(code > 0.5, slot, -1.0)
    rows = jnp.concatenate([moved, pad_ref[3:8, :]], axis=0)
    slots = lax.broadcasted_iota(jnp.int32, (MIG, PAD), 0).astype(jnp.float32)
    onehot = (slots == slot).astype(jnp.float32).astype(jnp.bfloat16)
    mig_ref[0] = select_rows(rows, onehot)
    own_ref[0:8, :] = rows
    own_ref[8:9, :] = jnp.where(code == 0.0, rank[0:1, :], -1.0)

    pl.semaphore_wait(barrier, 7)
    copies = []
    for relation in FAR_FIRST:
        block = pl.ds(SEG[relation][0] // 128 * 128, 128)
        for which, src, dst in ((0, mig_ref.at[0, :, block], mig_ref.at[relation, :, block]), (1, all_ref.at[0], all_ref.at[relation])):
            copy = pltpu.make_async_remote_copy(src_ref=src, dst_ref=dst, send_sem=send_sem.at[which, relation], recv_sem=recv_sem.at[which, relation], device_id=partner(relation), device_id_type=MESH_ID)
            copy.start()
            copies.append(copy)
    for copy in copies:
        copy.wait()


def pair_terms(own, other, span):
    delta = []
    for mine, theirs in zip(own, other):
        diff = mine - theirs
        if span is not None:
            diff = diff - jnp.where(diff > 0.5 * span, span, jnp.where(diff < -0.5 * span, -span, 0.0))
        delta.append(diff)
    dist_sq = delta[0] * delta[0] + delta[1] * delta[1] + delta[2] * delta[2]
    in_range = (dist_sq < RC * RC) & (dist_sq > 0.01)
    inv_r = jnp.where(in_range, lax.rsqrt(dist_sq), 0.0)
    inv_r2 = inv_r * inv_r
    inv_r6 = inv_r2 * inv_r2 * inv_r2
    inv_r12 = inv_r6 * inv_r6
    well = inv_r12 - inv_r6
    scale = (well + inv_r12) * inv_r2 + (UPC / 24.0) * inv_r
    return [scale * d for d in delta], [well, dist_sq * inv_r, jnp.where(in_range, 1.0, 0.0)]


def force_kernel(own_ref, all_ref, mig_ref, side_ref, pos_ref, vel_ref, frc_ref, id_ref, ok_ref, en_ref, cand_ref, near_ref, mine_ref, acc_ref, plane_ref, list_ref):
    side = side_ref[0, 0]
    box = side * 2.0
    lane = lax.broadcasted_iota(jnp.int32, (1, MIG), 1)
    arrivals = jnp.zeros((8, MIG), jnp.float32)
    for relation, (start, size) in SEG.items():
        arrivals = jnp.where((lane >= start) & (lane < start + size), mig_ref[relation], arrivals)
    cand_ref[:, 0:PAD] = own_ref[0:8, :]
    cand_ref[:, PAD:FULL] = arrivals
    stay_rank = own_ref[8:9, :]
    cand = cand_ref[...]
    valid = jnp.concatenate([stay_rank >= 0.0, arrivals[6:7, :] > 0.5], axis=1)
    number = (cand[6:7, :].astype(jnp.int32) - 1) * 65536 + cand[7:8, :].astype(jnp.int32)
    key = jnp.where(valid, number, 2147483647)
    total = jnp.sum(valid.astype(jnp.int32))
    key_col = jnp.transpose(jnp.broadcast_to(key[:, PAD:FULL], (8, MIG)))[:, 0:1]
    below = (key_col < key).astype(jnp.float32).astype(jnp.bfloat16)
    in_front = jnp.dot(jnp.ones((8, MIG), jnp.bfloat16), below, preferred_element_type=jnp.float32)[0:1, :]
    above = lax.dot_general(jnp.ones((8, PAD), jnp.bfloat16), below[:, 0:PAD], (((1,), (1,)), ((), ())), preferred_element_type=jnp.float32)[0:1, :]
    rank = in_front + jnp.concatenate([stay_rank, float(PAD) - above], axis=1)
    rank = jnp.where(valid, rank, -1.0)
    slots = lax.broadcasted_iota(jnp.int32, (PAD, FULL), 0).astype(jnp.float32)
    onehot = (slots == rank).astype(jnp.float32).astype(jnp.bfloat16)
    rows = select_rows(cand, onehot)
    filled = rows[6:7, :] > 0.5

    centre = [(coord + 0.5) * side for coord in brick_coords()]
    local = rows[0:3, :] - axis_column(centre, 3)
    near_ref[0:3, 0:PAD] = jnp.where(filled, local, FAR_AWAY)
    local = jnp.concatenate([jnp.where(filled, local, -FAR_AWAY), jnp.zeros((5, PAD), jnp.float32)], axis=0)
    piece_row = lax.broadcasted_iota(jnp.int32, (24, 384), 0) % 8
    piece_col = lax.broadcasted_iota(jnp.int32, (24, 384), 1) // 128
    spread = (piece_row == piece_col).astype(jnp.float32).astype(jnp.bfloat16)
    columns = lax.dot_general(pieces_of(local), spread, (((0,), (0,)), ((), ())), preferred_element_type=jnp.float32)
    for axis in range(3):
        mine_ref[axis] = columns[:, 128 * axis:128 * axis + 128]
    for relation in range(8):
        for axis in range(3):
            plane_ref[axis, relation:relation + 1, :] = all_ref[relation, :, PAD * axis:PAD * (axis + 1)]
    planes = []
    beyond = jnp.zeros((8, PAD), jnp.float32)
    for axis in range(3):
        theirs = plane_ref[axis] - centre[axis]
        theirs = jnp.where(theirs > side, theirs - box, jnp.where(theirs < -side, theirs + box, theirs))
        excess = jnp.maximum(jnp.abs(theirs) - 0.5 * side, 0.0)
        beyond = beyond + excess * excess
        planes.append(theirs)
    keep = (beyond < REACH * REACH) & (beyond > 0.0)
    front, held = prefix_counts(keep.astype(jnp.float32))
    lane8 = lax.broadcasted_iota(jnp.int32, (8, PAD), 1)
    hops = jnp.where(keep, lane8 - front.astype(jnp.int32), 0)
    for bit in range(10):
        step = 1 << bit
        coming = pltpu.roll(hops, PAD - step, 1)
        take = (coming & step) != 0
        leave = (hops & step) != 0
        hops = jnp.where(take, coming, jnp.where(leave, 0, hops))
        planes = [jnp.where(take, pltpu.roll(plane, PAD - step, 1), plane) for plane in planes]
    for relation in range(8):
        for axis in range(3):
            list_ref[relation, axis:axis + 1, 0:PAD] = planes[axis][relation:relation + 1, :]
    held = held.astype(jnp.int32)
    lane128 = lax.broadcasted_iota(jnp.int32, (8, 128), 1)
    start = total
    for relation in range(8):
        into = start % 128
        first = pl.multiple_of(start - into, 128)
        turned = pltpu.roll(list_ref[relation], into, 1)
        near_ref[:, pl.ds(first, 128)] = jnp.where(lane128 < into, near_ref[:, pl.ds(first, 128)], turned[:, 0:128])
        near_ref[:, pl.ds(pl.multiple_of(first + 128, 128), PAD)] = turned[:, 128:PAD + 128]
        start = start + held[relation, 0]
    into = start % 128
    first = pl.multiple_of(start - into, 128)
    near_ref[:, pl.ds(first, 128)] = jnp.where(lane128 < into, near_ref[:, pl.ds(first, 128)], FAR_AWAY)
    near_ref[:, pl.ds(pl.multiple_of(first + 128, 128), 256)] = jnp.full((8, 256), FAR_AWAY, jnp.float32)
    n_other = (start + 255) // 256
    n_own = (total + IC - 1) // IC

    def sweep(span):
        def own_step(i, totals):
            first = pl.multiple_of(i * IC, IC)
            own = [mine_ref[axis, pl.ds(first, IC), :] for axis in range(3)]

            def other_step(j, sums):
                forces, totals = sums
                lanes = pl.multiple_of(j * 256, 256)
                for half in range(2):
                    other = [near_ref[axis:axis + 1, pl.ds(lanes + 128 * half, 128)] for axis in range(3)]
                    force, parts = pair_terms(own, other, span)
                    forces = tuple(f + t for f, t in zip(forces, force))
                    totals = tuple(t + ((p[0:8] + p[8:16]) + (p[16:24] + p[24:32])) for t, p in zip(totals, parts))
                return forces, totals

            zero = jnp.zeros((IC, 128), jnp.float32)
            forces, totals = lax.fori_loop(0, n_other, other_step, ((zero,) * 3, totals))
            for axis in range(3):
                acc_ref[axis, pl.ds(first, IC), :] = forces[axis]
            return totals

        zero = jnp.zeros((8, 128), jnp.float32)
        well, distance, pairs = lax.fori_loop(0, n_own, own_step, (zero,) * 3)
        energy = 4.0 * well - UPC * distance - (UCUT - RC * UPC) * pairs
        en_ref[...] = jnp.sum(energy, axis=0, keepdims=True)

    @pl.when(side >= 2.0 * RC)
    def _():
        sweep(None)

    @pl.when(side < 2.0 * RC)
    def _():
        sweep(box)

    out_rows = []
    for axis in range(3):
        parts = []
        for b in range(PAD // 128):
            parts.append(jnp.sum(jnp.transpose(acc_ref[axis, 128 * b:128 * b + 128, :]), axis=0, keepdims=True))
        out_rows.append(jnp.concatenate(parts, axis=1))
    force = jnp.where(filled, 24.0 * jnp.concatenate(out_rows, axis=0), 0.0)
    frc_ref[...] = force[:, 0:CAP]
    pos_ref[...] = rows[0:3, 0:CAP]
    vel_ref[...] = (rows[3:6, :] + (0.5 * DT) * force)[:, 0:CAP]
    new_id = (rows[6:7, :].astype(jnp.int32) - 1) * 65536 + rows[7:8, :].astype(jnp.int32)
    id_ref[...] = jnp.where(filled, new_id, 0)[:, 0:CAP].reshape(CAP)
    ok_ref[...] = filled.astype(jnp.int32)[:, 0:CAP].reshape(CAP)


def energy_kernel(en_ref, out_ref, parts_ref, send_sem, recv_sem):
    barrier = greet()
    pl.semaphore_wait(barrier, 7)
    copies = []
    for relation in FAR_FIRST:
        copy = pltpu.make_async_remote_copy(src_ref=en_ref, dst_ref=parts_ref.at[relation], send_sem=send_sem.at[relation], recv_sem=recv_sem.at[relation], device_id=partner(relation), device_id_type=MESH_ID)
        copy.start()
        copies.append(copy)
    for copy in copies:
        copy.wait()
    parts_ref[0] = en_ref[...]
    over_x = [parts_ref[k] + parts_ref[k + 1] for k in (0, 2, 4, 6)]
    total = (over_x[0] + over_x[1]) + (over_x[2] + over_x[3])
    out_ref[...] = jnp.full((1, 1), 0.5 * jnp.sum(total), jnp.float32)


def solution(mesh):
    vmem = pl.BlockSpec(memory_space=pltpu.VMEM)
    hbm = pl.BlockSpec(memory_space=pltpu.HBM)
    smem = pl.BlockSpec(memory_space=pltpu.SMEM)
    f32, i32 = jnp.float32, jnp.int32

    def shape(dims, dtype=f32):
        return jax.ShapeDtypeStruct(dims, dtype)

    exchange = pl.pallas_call(
        exchange_kernel,
        out_shape=(shape((9, PAD)), shape((8, 1, 3 * PAD)), shape((8, 8, MIG))),
        in_specs=[hbm] * 5 + [smem],
        out_specs=(vmem, vmem, vmem),
        scratch_shapes=[pltpu.VMEM((3, CAP), f32)] * 3 + [pltpu.VMEM((CAP,), i32)] * 2 + [pltpu.VMEM((9, PAD), f32), pltpu.SemaphoreType.DMA((5,)), pltpu.SemaphoreType.DMA((2, 8)), pltpu.SemaphoreType.DMA((2, 8))],
        compiler_params=pltpu.CompilerParams(collective_id=0, has_side_effects=True, vmem_limit_bytes=16 << 20),
        name="exchange",
    )
    forces = pl.pallas_call(
        force_kernel,
        out_shape=(shape((3, CAP)), shape((3, CAP)), shape((3, CAP)), shape((CAP,), i32), shape((CAP,), i32), shape((1, 128))),
        in_specs=[vmem] * 3 + [smem],
        out_specs=(vmem,) * 6,
        scratch_shapes=[pltpu.VMEM((8, FULL), f32), pltpu.VMEM((8, 9 * PAD + 256), f32), pltpu.VMEM((3, PAD, 128), f32), pltpu.VMEM((3, PAD, 128), f32), pltpu.VMEM((3, 8, PAD), f32), pltpu.VMEM((8, 8, PAD + 128), f32)],
        compiler_params=pltpu.CompilerParams(vmem_limit_bytes=16 << 20),
        name="forces",
    )
    total_energy = pl.pallas_call(
        energy_kernel,
        out_shape=shape((1, 1)),
        in_specs=[vmem],
        out_specs=vmem,
        scratch_shapes=[pltpu.VMEM((8, 1, 128), f32), pltpu.SemaphoreType.DMA((8,)), pltpu.SemaphoreType.DMA((8,))],
        compiler_params=pltpu.CompilerParams(collective_id=1, has_side_effects=True, vmem_limit_bytes=16 << 20),
        name="energy",
    )

    def local_step(atom_pos, atom_vel, atom_frc, atom_id, atom_ok, brick_side):
        side = brick_side.reshape(1, 1)
        own, everyone, movers = exchange(*[pltpu.with_memory_space_constraint(a, pltpu.HBM) for a in (atom_pos.T, atom_vel.T, atom_frc.T, atom_id, atom_ok)], side)
        pos, vel, frc, new_id, new_ok, partial = forces(own, everyone, movers, side)
        energy = total_energy(partial)
        return pos.T, vel.T, frc.T, new_id, new_ok, energy.reshape(())

    row_spec = P(MESH_AXES, None)
    id_spec = P(MESH_AXES)
    return jax.shard_map(local_step, mesh=mesh, in_specs=(row_spec, row_spec, row_spec, id_spec, id_spec, P()), out_specs=(row_spec, row_spec, row_spec, id_spec, id_spec, P()), check_vma=False)
```

```python
import functools

import jax
import jax.numpy as jnp
from jax import lax
from jax.experimental import pallas as pl
from jax.experimental.pallas import tpu as pltpu
from jax.sharding import PartitionSpec as P

DT = 0.005
RC = 2.5
FAR_AWAY = 1.0e6
UCUT = 4.0 * (RC ** -12 - RC ** -6)
UPC = -48.0 * RC ** -13 + 24.0 * RC ** -7
MESH_AXES = ("z", "y", "x")
CAP = 729
PAD = 768
MIG = 256
FULL = PAD + MIG
SEG = {1: (0, 16), 2: (16, 16), 4: (32, 16), 3: (48, 32), 5: (80, 32), 6: (128, 32), 7: (160, 64)}
IC = 32
FAR_FIRST = (6, 7, 4, 2, 5, 3, 1)
REACH = RC + 0.01
MESH_ID = pl.DeviceIdType.MESH


def pieces_of(rows):
    first = rows.astype(jnp.bfloat16).astype(jnp.float32)
    rest = rows - first
    second = rest.astype(jnp.bfloat16).astype(jnp.float32)
    third = rest - second
    return jnp.concatenate([first, second, third], axis=0).astype(jnp.bfloat16)


def select_rows(rows, onehot):
    out = lax.dot_general(pieces_of(rows), onehot, (((1,), (1,)), ((), ())), preferred_element_type=jnp.float32)
    return out[0:8] + out[8:16] + out[16:24]


def partner(relation):
    mine = (lax.axis_index("z"), lax.axis_index("y"), lax.axis_index("x"))
    bits = (relation // 4 % 2, relation // 2 % 2, relation % 2)
    return tuple((axis + bit) % 2 for axis, bit in zip(mine, bits))


def greet():
    barrier = pltpu.get_barrier_semaphore()
    for relation in range(1, 8):
        pl.semaphore_signal(barrier, inc=1, device_id=partner(relation), device_id_type=MESH_ID)
    return barrier


def axis_column(values, rows):
    idx = lax.broadcasted_iota(jnp.int32, (rows, 1), 0)
    out = jnp.full((rows, 1), values[-1], jnp.float32)
    for k in range(len(values) - 1):
        out = jnp.where(idx == k, values[k], out)
    return out


def brick_coords():
    return [lax.axis_index(name).astype(jnp.float32) for name in ("x", "y", "z")]


def prefix_counts(member):
    blocks = PAD // 128
    stacked = jnp.concatenate([member[:, 128 * b:128 * (b + 1)] for b in range(blocks)], axis=0).astype(jnp.bfloat16)
    row = lax.broadcasted_iota(jnp.int32, (128, 256), 0)
    col = lax.broadcasted_iota(jnp.int32, (128, 256), 1)
    ladder = ((row < col) | (col >= 128)).astype(jnp.float32).astype(jnp.bfloat16)
    counts = jnp.dot(stacked, ladder, preferred_element_type=jnp.float32)
    before = jnp.zeros((8, 128), jnp.float32)
    ranks = []
    for b in range(blocks):
        ranks.append(counts[8 * b:8 * b + 8, 0:128] + before)
        before = before + counts[8 * b:8 * b + 8, 128:256]
    return jnp.concatenate(ranks, axis=1), before


def exchange_kernel(pos_hbm, vel_hbm, frc_hbm, id_hbm, ok_hbm, side_hbm, own_ref, all_ref, mig_ref, pos_ref, vel_ref, frc_ref, id_ref, ok_ref, side_ref, pad_ref, load_sem, send_sem, recv_sem):
    loads = []
    for k, (src, dst) in enumerate(((pos_hbm, pos_ref), (vel_hbm, vel_ref), (frc_hbm, frc_ref), (id_hbm, id_ref), (ok_hbm, ok_ref), (side_hbm, side_ref))):
        load = pltpu.make_async_copy(src, dst, load_sem.at[k])
        load.start()
        loads.append(load)
    barrier = greet()
    pad_ref[...] = jnp.zeros_like(pad_ref)
    for load in loads:
        load.wait()
    side = side_ref[...]
    box = side * 2.0
    half_v = vel_ref[...] + (0.5 * DT) * frc_ref[...]
    pad_ref[0:3, 0:CAP] = pos_ref[...] + DT * half_v
    pad_ref[3:6, 0:CAP] = half_v
    pad_ref[6:7, 0:CAP] = (id_ref[...].reshape(1, CAP) >> 16).astype(jnp.float32) + 1.0
    pad_ref[7:8, 0:CAP] = (id_ref[...].reshape(1, CAP) & 65535).astype(jnp.float32)
    pad_ref[8:9, 0:CAP] = ok_ref[...].reshape(1, CAP).astype(jnp.float32)
    unwrapped = pad_ref[0:3, :]
    owned = pad_ref[8:9, :] > 0.5
    moved = jnp.where(unwrapped < 0.0, unwrapped + box, jnp.where(unwrapped >= box, unwrapped - box, unwrapped))
    for axis in range(3):
        all_ref[0, :, PAD * axis:PAD * (axis + 1)] = jnp.where(owned, moved[axis:axis + 1, :], FAR_AWAY)

    low = axis_column([coord * side for coord in brick_coords()], 3)
    outside = (unwrapped < low) | (unwrapped >= low + side)
    bits = jnp.where(outside, axis_column([1.0, 2.0, 4.0], 3), 0.0)
    code = jnp.sum(bits, axis=0, keepdims=True)
    code = jnp.where(owned, code, -1.0)
    relation_col = lax.broadcasted_iota(jnp.int32, (8, PAD), 0).astype(jnp.float32)
    member = code == relation_col
    rank, _ = prefix_counts(member.astype(jnp.float32))
    offset = axis_column([0.0] + [float(SEG[m][0]) for m in range(1, 8)], 8)
    slot = jnp.sum(jnp.where(member, rank + offset, 0.0), axis=0, keepdims=True)
    slot = jnp.where(code > 0.5, slot, -1.0)
    rows = jnp.concatenate([moved, pad_ref[3:8, :]], axis=0)
    slots = lax.broadcasted_iota(jnp.int32, (MIG, PAD), 0).astype(jnp.float32)
    onehot = (slots == slot).astype(jnp.float32).astype(jnp.bfloat16)
    mig_ref[0] = select_rows(rows, onehot)
    own_ref[0:8, :] = rows
    own_ref[8:9, :] = jnp.where(code == 0.0, rank[0:1, :], -1.0)
    own_ref[9:10, :] = jnp.broadcast_to(side, (1, PAD))

    pl.semaphore_wait(barrier, 7)
    copies = []
    for relation in FAR_FIRST:
        block = pl.ds(SEG[relation][0] // 128 * 128, 128)
        for which, src, dst in ((0, mig_ref.at[0, :, block], mig_ref.at[relation, :, block]), (1, all_ref.at[0], all_ref.at[relation])):
            copy = pltpu.make_async_remote_copy(src_ref=src, dst_ref=dst, send_sem=send_sem.at[which, relation], recv_sem=recv_sem.at[which, relation], device_id=partner(relation), device_id_type=MESH_ID)
            copy.start()
            copies.append(copy)
    for copy in copies:
        copy.wait()


def pair_terms(own, other, span):
    delta = []
    for mine, theirs in zip(own, other):
        diff = mine - theirs
        if span is not None:
            diff = diff - jnp.where(diff > 0.5 * span, span, jnp.where(diff < -0.5 * span, -span, 0.0))
        delta.append(diff)
    dist_sq = delta[0] * delta[0] + delta[1] * delta[1] + delta[2] * delta[2]
    in_range = (dist_sq < RC * RC) & (dist_sq > 0.01)
    inv_r = jnp.where(in_range, lax.rsqrt(dist_sq), 0.0)
    inv_r2 = inv_r * inv_r
    inv_r6 = inv_r2 * inv_r2 * inv_r2
    inv_r12 = inv_r6 * inv_r6
    well = inv_r12 - inv_r6
    scale = (well + inv_r12) * inv_r2 + (UPC / 24.0) * inv_r
    return [scale * d for d in delta], [well, dist_sq * inv_r, jnp.where(in_range, 1.0, 0.0)]


def force_kernel(own_ref, all_ref, mig_ref, pos_ref, vel_ref, frc_ref, id_ref, ok_ref, en_ref, cand_ref, near_ref, mine_ref, acc_ref, plane_ref, list_ref):
    side = own_ref[9:10, 0:1]
    box = side * 2.0
    lane = lax.broadcasted_iota(jnp.int32, (1, MIG), 1)
    arrivals = jnp.zeros((8, MIG), jnp.float32)
    for relation, (start, size) in SEG.items():
        arrivals = jnp.where((lane >= start) & (lane < start + size), mig_ref[relation], arrivals)
    cand_ref[:, 0:PAD] = own_ref[0:8, :]
    cand_ref[:, PAD:FULL] = arrivals
    stay_rank = own_ref[8:9, :]
    cand = cand_ref[...]
    valid = jnp.concatenate([stay_rank >= 0.0, arrivals[6:7, :] > 0.5], axis=1)
    number = (cand[6:7, :].astype(jnp.int32) - 1) * 65536 + cand[7:8, :].astype(jnp.int32)
    key = jnp.where(valid, number, 2147483647)
    total = jnp.sum(valid.astype(jnp.int32))
    key_col = jnp.transpose(jnp.broadcast_to(key[:, PAD:FULL], (8, MIG)))[:, 0:1]
    below = (key_col < key).astype(jnp.float32).astype(jnp.bfloat16)
    in_front = jnp.dot(jnp.ones((8, MIG), jnp.bfloat16), below, preferred_element_type=jnp.float32)[0:1, :]
    above = lax.dot_general(jnp.ones((8, PAD), jnp.bfloat16), below[:, 0:PAD], (((1,), (1,)), ((), ())), preferred_element_type=jnp.float32)[0:1, :]
    rank = in_front + jnp.concatenate([stay_rank, float(PAD) - above], axis=1)
    rank = jnp.where(valid, rank, -1.0)
    slots = lax.broadcasted_iota(jnp.int32, (PAD, FULL), 0).astype(jnp.float32)
    onehot = (slots == rank).astype(jnp.float32).astype(jnp.bfloat16)
    rows = select_rows(cand, onehot)
    filled = rows[6:7, :] > 0.5

    centre = [(coord + 0.5) * side for coord in brick_coords()]
    local = rows[0:3, :] - axis_column(centre, 3)
    near_ref[0:3, 0:PAD] = jnp.where(filled, local, FAR_AWAY)
    local = jnp.concatenate([jnp.where(filled, local, -FAR_AWAY), jnp.zeros((5, PAD), jnp.float32)], axis=0)
    piece_row = lax.broadcasted_iota(jnp.int32, (24, 384), 0) % 8
    piece_col = lax.broadcasted_iota(jnp.int32, (24, 384), 1) // 128
    spread = (piece_row == piece_col).astype(jnp.float32).astype(jnp.bfloat16)
    columns = lax.dot_general(pieces_of(local), spread, (((0,), (0,)), ((), ())), preferred_element_type=jnp.float32)
    for axis in range(3):
        mine_ref[axis] = columns[:, 128 * axis:128 * axis + 128]
    for relation in range(8):
        for axis in range(3):
            plane_ref[axis, relation:relation + 1, :] = all_ref[relation, :, PAD * axis:PAD * (axis + 1)]
    planes = []
    beyond = jnp.zeros((8, PAD), jnp.float32)
    for axis in range(3):
        theirs = plane_ref[axis] - centre[axis]
        theirs = jnp.where(theirs > side, theirs - box, jnp.where(theirs < -side, theirs + box, theirs))
        excess = jnp.maximum(jnp.abs(theirs) - 0.5 * side, 0.0)
        beyond = beyond + excess * excess
        planes.append(theirs)
    keep = (beyond < REACH * REACH) & (beyond > 0.0)
    front, held = prefix_counts(keep.astype(jnp.float32))
    lane8 = lax.broadcasted_iota(jnp.int32, (8, PAD), 1)
    hops = jnp.where(keep, lane8 - front.astype(jnp.int32), 0)
    for bit in range(10):
        step = 1 << bit
        coming = pltpu.roll(hops, PAD - step, 1)
        take = (coming & step) != 0
        leave = (hops & step) != 0
        hops = jnp.where(take, coming, jnp.where(leave, 0, hops))
        planes = [jnp.where(take, pltpu.roll(plane, PAD - step, 1), plane) for plane in planes]
    for relation in range(8):
        for axis in range(3):
            list_ref[relation, axis:axis + 1, 0:PAD] = planes[axis][relation:relation + 1, :]
    held = held.astype(jnp.int32)
    lane128 = lax.broadcasted_iota(jnp.int32, (8, 128), 1)
    start = total
    for relation in range(8):
        into = start % 128
        first = pl.multiple_of(start - into, 128)
        turned = pltpu.roll(list_ref[relation], into, 1)
        near_ref[:, pl.ds(first, 128)] = jnp.where(lane128 < into, near_ref[:, pl.ds(first, 128)], turned[:, 0:128])
        near_ref[:, pl.ds(pl.multiple_of(first + 128, 128), PAD)] = turned[:, 128:PAD + 128]
        start = start + held[relation, 0]
    into = start % 128
    first = pl.multiple_of(start - into, 128)
    near_ref[:, pl.ds(first, 128)] = jnp.where(lane128 < into, near_ref[:, pl.ds(first, 128)], FAR_AWAY)
    near_ref[:, pl.ds(pl.multiple_of(first + 128, 128), 256)] = jnp.full((8, 256), FAR_AWAY, jnp.float32)
    n_other = (start + 255) // 256
    n_own = (total + IC - 1) // IC

    def sweep(span):
        def own_step(i, totals):
            first = pl.multiple_of(i * IC, IC)
            own = [mine_ref[axis, pl.ds(first, IC), :] for axis in range(3)]

            def other_step(j, sums):
                forces, totals = sums
                lanes = pl.multiple_of(j * 256, 256)
                for half in range(2):
                    other = [near_ref[axis:axis + 1, pl.ds(lanes + 128 * half, 128)] for axis in range(3)]
                    force, parts = pair_terms(own, other, span)
                    forces = tuple(f + t for f, t in zip(forces, force))
                    totals = tuple(t + ((p[0:8] + p[8:16]) + (p[16:24] + p[24:32])) for t, p in zip(totals, parts))
                return forces, totals

            zero = jnp.zeros((IC, 128), jnp.float32)
            forces, totals = lax.fori_loop(0, n_other, other_step, ((zero,) * 3, totals))
            for axis in range(3):
                acc_ref[axis, pl.ds(first, IC), :] = forces[axis]
            return totals

        zero = jnp.zeros((8, 128), jnp.float32)
        well, distance, pairs = lax.fori_loop(0, n_own, own_step, (zero,) * 3)
        energy = 2.0 * well - (0.5 * UPC) * distance - (0.5 * (UCUT - RC * UPC)) * pairs
        en_ref[...] = jnp.sum(energy, axis=0, keepdims=True)

    one_image = side[0, 0] >= 2.0 * RC

    @pl.when(one_image)
    def _():
        sweep(None)

    @pl.when(jnp.logical_not(one_image))
    def _():
        sweep(box)

    out_rows = []
    for axis in range(3):
        parts = []
        for b in range(PAD // 128):
            parts.append(jnp.sum(jnp.transpose(acc_ref[axis, 128 * b:128 * b + 128, :]), axis=0, keepdims=True))
        out_rows.append(jnp.concatenate(parts, axis=1))
    force = jnp.where(filled, 24.0 * jnp.concatenate(out_rows, axis=0), 0.0)
    frc_ref[...] = force[:, 0:CAP]
    pos_ref[...] = rows[0:3, 0:CAP]
    vel_ref[...] = (rows[3:6, :] + (0.5 * DT) * force)[:, 0:CAP]
    new_id = (rows[6:7, :].astype(jnp.int32) - 1) * 65536 + rows[7:8, :].astype(jnp.int32)
    id_ref[...] = jnp.where(filled, new_id, 0)[:, 0:CAP].reshape(CAP)
    ok_ref[...] = filled.astype(jnp.int32)[:, 0:CAP].reshape(CAP)


def energy_kernel(en_ref, out_ref, parts_ref, send_sem, recv_sem):
    barrier = greet()
    pl.semaphore_wait(barrier, 7)
    copies = []
    for relation in FAR_FIRST:
        copy = pltpu.make_async_remote_copy(src_ref=en_ref, dst_ref=parts_ref.at[relation], send_sem=send_sem.at[relation], recv_sem=recv_sem.at[relation], device_id=partner(relation), device_id_type=MESH_ID)
        copy.start()
        copies.append(copy)
    for copy in copies:
        copy.wait()
    parts_ref[0] = en_ref[...]
    over_x = [parts_ref[k] + parts_ref[k + 1] for k in (0, 2, 4, 6)]
    out_ref[...] = (over_x[0] + over_x[1]) + (over_x[2] + over_x[3])


def solution(mesh):
    vmem = pl.BlockSpec(memory_space=pltpu.VMEM)
    hbm = pl.BlockSpec(memory_space=pltpu.HBM)
    f32, i32 = jnp.float32, jnp.int32

    def shape(dims, dtype=f32):
        return jax.ShapeDtypeStruct(dims, dtype)

    exchange = pl.pallas_call(
        exchange_kernel,
        out_shape=(shape((10, PAD)), shape((8, 1, 3 * PAD)), shape((8, 8, MIG))),
        in_specs=[hbm] * 5 + [pl.BlockSpec(memory_space=pl.ANY)],
        out_specs=(vmem, vmem, vmem),
        scratch_shapes=[pltpu.VMEM((3, CAP), f32)] * 3 + [pltpu.VMEM((CAP,), i32)] * 2 + [pltpu.VMEM((1, 1), f32), pltpu.VMEM((9, PAD), f32), pltpu.SemaphoreType.DMA((6,)), pltpu.SemaphoreType.DMA((2, 8)), pltpu.SemaphoreType.DMA((2, 8))],
        compiler_params=pltpu.CompilerParams(collective_id=0, has_side_effects=True, vmem_limit_bytes=16 << 20),
        name="exchange",
    )
    forces = pl.pallas_call(
        force_kernel,
        out_shape=(shape((3, CAP)), shape((3, CAP)), shape((3, CAP)), shape((CAP,), i32), shape((CAP,), i32), shape((1, 128))),
        in_specs=[vmem] * 3,
        out_specs=(vmem,) * 6,
        scratch_shapes=[pltpu.VMEM((8, FULL), f32), pltpu.VMEM((8, 9 * PAD + 256), f32), pltpu.VMEM((3, PAD, 128), f32), pltpu.VMEM((3, PAD, 128), f32), pltpu.VMEM((3, 8, PAD), f32), pltpu.VMEM((8, 8, PAD + 128), f32)],
        compiler_params=pltpu.CompilerParams(vmem_limit_bytes=16 << 20),
        name="forces",
    )
    total_energy = pl.pallas_call(
        energy_kernel,
        out_shape=shape((1, 128)),
        in_specs=[vmem],
        out_specs=vmem,
        scratch_shapes=[pltpu.VMEM((8, 1, 128), f32), pltpu.SemaphoreType.DMA((8,)), pltpu.SemaphoreType.DMA((8,))],
        compiler_params=pltpu.CompilerParams(collective_id=1, has_side_effects=True, vmem_limit_bytes=16 << 20),
        name="energy",
    )

    def local_step(atom_pos, atom_vel, atom_frc, atom_id, atom_ok, brick_side):
        arrays = (atom_pos.T, atom_vel.T, atom_frc.T, atom_id, atom_ok, brick_side.reshape(1, 1))
        own, everyone, movers = exchange(*[pltpu.with_memory_space_constraint(array, pltpu.HBM) for array in arrays[:5]], arrays[5])
        pos, vel, frc, new_id, new_ok, partial = forces(own, everyone, movers)
        energy = jnp.sum(total_energy(partial))
        return pos.T, vel.T, frc.T, new_id, new_ok, energy

    row_spec = P(MESH_AXES, None)
    id_spec = P(MESH_AXES)
    return jax.shard_map(local_step, mesh=mesh, in_specs=(row_spec, row_spec, row_spec, id_spec, id_spec, P()), out_specs=(row_spec, row_spec, row_spec, id_spec, id_spec, P()), check_vma=False)
```

```python
import functools

import jax
import jax.numpy as jnp
from jax import lax
from jax.experimental import pallas as pl
from jax.experimental.pallas import tpu as pltpu
from jax.sharding import PartitionSpec as P

DT = 0.005
RC = 2.5
FAR_AWAY = 1.0e6
UCUT = 4.0 * (RC ** -12 - RC ** -6)
UPC = -48.0 * RC ** -13 + 24.0 * RC ** -7
MESH_AXES = ("z", "y", "x")
CAP = 729
PAD = 768
MIG = 256
FULL = PAD + MIG
SEG = {1: (0, 16), 2: (16, 16), 4: (32, 16), 3: (48, 32), 5: (80, 32), 6: (128, 32), 7: (160, 64)}
IC = 32
NARROW = 512
FAR_FIRST = (6, 7, 4, 2, 5, 3, 1)
REACH = RC + 0.01
MESH_ID = pl.DeviceIdType.MESH


def pieces_of(rows):
    first = rows.astype(jnp.bfloat16).astype(jnp.float32)
    rest = rows - first
    second = rest.astype(jnp.bfloat16).astype(jnp.float32)
    third = rest - second
    return jnp.concatenate([first, second, third], axis=0).astype(jnp.bfloat16)


def select_rows(rows, onehot):
    out = lax.dot_general(pieces_of(rows), onehot, (((1,), (1,)), ((), ())), preferred_element_type=jnp.float32)
    return out[0:8] + out[8:16] + out[16:24]


def partner(relation):
    mine = (lax.axis_index("z"), lax.axis_index("y"), lax.axis_index("x"))
    bits = (relation // 4 % 2, relation // 2 % 2, relation % 2)
    return tuple((axis + bit) % 2 for axis, bit in zip(mine, bits))


def greet():
    barrier = pltpu.get_barrier_semaphore()
    for relation in range(1, 8):
        pl.semaphore_signal(barrier, inc=1, device_id=partner(relation), device_id_type=MESH_ID)
    return barrier


def axis_column(values, rows):
    idx = lax.broadcasted_iota(jnp.int32, (rows, 1), 0)
    out = jnp.full((rows, 1), values[-1], jnp.float32)
    for k in range(len(values) - 1):
        out = jnp.where(idx == k, values[k], out)
    return out


def brick_coords():
    return [lax.axis_index(name).astype(jnp.float32) for name in ("x", "y", "z")]


def prefix_counts(member):
    blocks = member.shape[1] // 128
    stacked = jnp.concatenate([member[:, 128 * b:128 * (b + 1)] for b in range(blocks)], axis=0).astype(jnp.bfloat16)
    row = lax.broadcasted_iota(jnp.int32, (128, 256), 0)
    col = lax.broadcasted_iota(jnp.int32, (128, 256), 1)
    ladder = ((row < col) | (col >= 128)).astype(jnp.float32).astype(jnp.bfloat16)
    counts = jnp.dot(stacked, ladder, preferred_element_type=jnp.float32)
    before = jnp.zeros((8, 128), jnp.float32)
    ranks = []
    for b in range(blocks):
        ranks.append(counts[8 * b:8 * b + 8, 0:128] + before)
        before = before + counts[8 * b:8 * b + 8, 128:256]
    return jnp.concatenate(ranks, axis=1), before


def exchange_kernel(pos_hbm, vel_hbm, frc_hbm, id_hbm, ok_hbm, side_hbm, own_ref, all_ref, mig_ref, pos_ref, vel_ref, frc_ref, id_ref, ok_ref, side_ref, pad_ref, load_sem, send_sem, recv_sem):
    loads = []
    for k, (src, dst) in enumerate(((pos_hbm, pos_ref), (vel_hbm, vel_ref), (frc_hbm, frc_ref), (id_hbm, id_ref), (ok_hbm, ok_ref), (side_hbm, side_ref))):
        load = pltpu.make_async_copy(src, dst, load_sem.at[k])
        load.start()
        loads.append(load)
    barrier = greet()
    pad_ref[...] = jnp.zeros_like(pad_ref)
    for load in loads:
        load.wait()
    side = side_ref[...]
    box = side * 2.0
    half_v = vel_ref[...] + (0.5 * DT) * frc_ref[...]
    pad_ref[0:3, 0:CAP] = pos_ref[...] + DT * half_v
    pad_ref[3:6, 0:CAP] = half_v
    pad_ref[6:7, 0:CAP] = (id_ref[...].reshape(1, CAP) >> 16).astype(jnp.float32) + 1.0
    pad_ref[7:8, 0:CAP] = (id_ref[...].reshape(1, CAP) & 65535).astype(jnp.float32)
    pad_ref[8:9, 0:CAP] = ok_ref[...].reshape(1, CAP).astype(jnp.float32)
    unwrapped = pad_ref[0:3, :]
    owned = pad_ref[8:9, :] > 0.5
    moved = jnp.where(unwrapped < 0.0, unwrapped + box, jnp.where(unwrapped >= box, unwrapped - box, unwrapped))
    for axis in range(3):
        all_ref[0, :, PAD * axis:PAD * (axis + 1)] = jnp.where(owned, moved[axis:axis + 1, :], FAR_AWAY)

    low = axis_column([coord * side for coord in brick_coords()], 3)
    outside = (unwrapped < low) | (unwrapped >= low + side)
    bits = jnp.where(outside, axis_column([1.0, 2.0, 4.0], 3), 0.0)
    code = jnp.sum(bits, axis=0, keepdims=True)
    code = jnp.where(owned, code, -1.0)
    relation_col = lax.broadcasted_iota(jnp.int32, (8, PAD), 0).astype(jnp.float32)
    member = code == relation_col
    rank, _ = prefix_counts(member.astype(jnp.float32))
    offset = axis_column([0.0] + [float(SEG[m][0]) for m in range(1, 8)], 8)
    slot = jnp.sum(jnp.where(member, rank + offset, 0.0), axis=0, keepdims=True)
    slot = jnp.where(code > 0.5, slot, -1.0)
    rows = jnp.concatenate([moved, pad_ref[3:8, :]], axis=0)
    slots = lax.broadcasted_iota(jnp.int32, (MIG, PAD), 0).astype(jnp.float32)
    onehot = (slots == slot).astype(jnp.float32).astype(jnp.bfloat16)
    mig_ref[0] = select_rows(rows, onehot)
    own_ref[0:8, :] = rows
    own_ref[8:9, :] = jnp.where(code == 0.0, rank[0:1, :], -1.0)
    own_ref[9:10, :] = jnp.broadcast_to(side, (1, PAD))

    pl.semaphore_wait(barrier, 7)
    copies = []
    for relation in FAR_FIRST:
        block = pl.ds(SEG[relation][0] // 128 * 128, 128)
        for which, src, dst in ((0, mig_ref.at[0, :, block], mig_ref.at[relation, :, block]), (1, all_ref.at[0], all_ref.at[relation])):
            copy = pltpu.make_async_remote_copy(src_ref=src, dst_ref=dst, send_sem=send_sem.at[which, relation], recv_sem=recv_sem.at[which, relation], device_id=partner(relation), device_id_type=MESH_ID)
            copy.start()
            copies.append(copy)
    for copy in copies:
        copy.wait()


def pair_terms(own, other, span):
    delta = []
    for mine, theirs in zip(own, other):
        diff = mine - theirs
        if span is not None:
            diff = diff - jnp.where(diff > 0.5 * span, span, jnp.where(diff < -0.5 * span, -span, 0.0))
        delta.append(diff)
    dist_sq = delta[0] * delta[0] + delta[1] * delta[1] + delta[2] * delta[2]
    in_range = (dist_sq < RC * RC) & (dist_sq > 0.01)
    inv_r = jnp.where(in_range, lax.rsqrt(dist_sq), 0.0)
    inv_r2 = inv_r * inv_r
    inv_r6 = inv_r2 * inv_r2 * inv_r2
    inv_r12 = inv_r6 * inv_r6
    well = inv_r12 - inv_r6
    scale = (well + inv_r12) * inv_r2 + (UPC / 24.0) * inv_r
    return [scale * d for d in delta], [well, dist_sq * inv_r, jnp.where(in_range, 1.0, 0.0)]


def force_kernel(own_ref, all_ref, mig_ref, pos_ref, vel_ref, frc_ref, id_ref, ok_ref, en_ref, cand_ref, near_ref, mine_ref, acc_ref, plane_ref, list_ref, rows_ref, rank_ref, sum_ref, count_ref):
    side = own_ref[9:10, 0:1]
    box = side * 2.0
    lane = lax.broadcasted_iota(jnp.int32, (1, MIG), 1)
    arrivals = jnp.zeros((8, MIG), jnp.float32)
    for relation, (start, size) in SEG.items():
        arrivals = jnp.where((lane >= start) & (lane < start + size), mig_ref[relation], arrivals)
    cand_ref[:, 0:PAD] = own_ref[0:8, :]
    cand_ref[:, PAD:FULL] = arrivals
    stay_rank = own_ref[8:9, :]
    cand = cand_ref[...]
    valid = jnp.concatenate([stay_rank >= 0.0, arrivals[6:7, :] > 0.5], axis=1)
    total = jnp.sum(valid.astype(jnp.int32))
    tail = all_ref[0, :, NARROW:PAD]
    for relation in range(1, 8):
        tail = jnp.minimum(tail, all_ref[relation, :, NARROW:PAD])
    narrow = (jnp.min(tail) > 0.5 * FAR_AWAY) & (total <= NARROW)
    number = (cand[6:7, :].astype(jnp.int32) - 1) * 65536 + cand[7:8, :].astype(jnp.int32)
    key = jnp.where(valid, number, 2147483647)
    key_col = jnp.transpose(jnp.broadcast_to(key[:, PAD:FULL], (8, MIG)))[:, 0:1]
    below = (key_col < key).astype(jnp.float32).astype(jnp.bfloat16)
    in_front = jnp.dot(jnp.ones((8, MIG), jnp.bfloat16), below, preferred_element_type=jnp.float32)[0:1, :]
    above = lax.dot_general(jnp.ones((8, PAD), jnp.bfloat16), below[:, 0:PAD], (((1,), (1,)), ((), ())), preferred_element_type=jnp.float32)[0:1, :]
    rank = in_front + jnp.concatenate([stay_rank, float(PAD) - above], axis=1)
    rank_ref[...] = jnp.where(valid, rank, -1.0)
    centre = [(coord + 0.5) * side for coord in brick_coords()]

    def prepare(width):
        for relation in range(8):
            for axis in range(3):
                plane_ref[axis, relation:relation + 1, 0:width] = all_ref[relation, :, PAD * axis:PAD * axis + width]
        planes = []
        beyond = jnp.zeros((8, width), jnp.float32)
        for axis in range(3):
            theirs = plane_ref[axis, :, 0:width] - centre[axis]
            theirs = jnp.where(theirs > side, theirs - box, jnp.where(theirs < -side, theirs + box, theirs))
            excess = jnp.maximum(jnp.abs(theirs) - 0.5 * side, 0.0)
            beyond = beyond + excess * excess
            planes.append(theirs)
        keep = (beyond < REACH * REACH) & (beyond > 0.0)
        front, held = prefix_counts(keep.astype(jnp.float32))
        lanes = lax.broadcasted_iota(jnp.int32, (8, width), 1)
        hops = jnp.where(keep, lanes - front.astype(jnp.int32), 0)

        ranks = jnp.concatenate([rank_ref[:, 0:width], rank_ref[:, PAD:FULL]], axis=1)
        pieces = pieces_of(jnp.concatenate([cand_ref[:, 0:width], cand_ref[:, PAD:FULL]], axis=1))
        slots = lax.broadcasted_iota(jnp.int32, (128, width + MIG), 0).astype(jnp.float32)
        blocks = width // 128
        done = 0
        for bit in range(10 if width > 512 else 9):
            step = 1 << bit
            coming = pltpu.roll(hops, width - step, 1)
            take = (coming & step) != 0
            leave = (hops & step) != 0
            hops = jnp.where(take, coming, jnp.where(leave, 0, hops))
            planes = [jnp.where(take, pltpu.roll(plane, width - step, 1), plane) for plane in planes]
            if done < blocks:
                onehot = (slots == ranks - 128.0 * done).astype(jnp.float32).astype(jnp.bfloat16)
                out = lax.dot_general(pieces, onehot, (((1,), (1,)), ((), ())), preferred_element_type=jnp.float32)
                rows_ref[:, 128 * done:128 * done + 128] = out[0:8] + out[8:16] + out[16:24]
                done += 1
        if width < PAD:
            rows_ref[:, width:PAD] = jnp.zeros((8, PAD - width), jnp.float32)

        rows = rows_ref[:, 0:width]
        filled = rows[6:7, :] > 0.5
        local = rows[0:3, :] - axis_column(centre, 3)
        near_ref[0:3, 0:width] = jnp.where(filled, local, FAR_AWAY)
        local = jnp.concatenate([jnp.where(filled, local, -FAR_AWAY), jnp.zeros((5, width), jnp.float32)], axis=0)
        piece_row = lax.broadcasted_iota(jnp.int32, (24, 384), 0) % 8
        piece_col = lax.broadcasted_iota(jnp.int32, (24, 384), 1) // 128
        spread = (piece_row == piece_col).astype(jnp.float32).astype(jnp.bfloat16)
        columns = lax.dot_general(pieces_of(local), spread, (((0,), (0,)), ((), ())), preferred_element_type=jnp.float32)
        for axis in range(3):
            mine_ref[axis, 0:width, :] = columns[:, 128 * axis:128 * axis + 128]

        for relation in range(8):
            for axis in range(3):
                list_ref[relation, axis:axis + 1, 0:width] = planes[axis][relation:relation + 1, :]
        held = held.astype(jnp.int32)
        lane128 = lax.broadcasted_iota(jnp.int32, (8, 128), 1)
        start = total
        for relation in range(8):
            into = start % 128
            first = pl.multiple_of(start - into, 128)
            turned = pltpu.roll(list_ref[relation, :, 0:width + 128], into, 1)
            near_ref[:, pl.ds(first, 128)] = jnp.where(lane128 < into, near_ref[:, pl.ds(first, 128)], turned[:, 0:128])
            near_ref[:, pl.ds(pl.multiple_of(first + 128, 128), width)] = turned[:, 128:width + 128]
            start = start + held[relation, 0]
        into = start % 128
        first = pl.multiple_of(start - into, 128)
        near_ref[:, pl.ds(first, 128)] = jnp.where(lane128 < into, near_ref[:, pl.ds(first, 128)], FAR_AWAY)
        count_ref[0] = (start + 127) // 128

    @pl.when(narrow)
    def _():
        prepare(NARROW)

    @pl.when(jnp.logical_not(narrow))
    def _():
        prepare(PAD)

    n_other = count_ref[0]
    n_own = (total + IC - 1) // IC

    def sweep(span):
        def own_step(i, totals):
            first = pl.multiple_of(i * IC, IC)
            own = [mine_ref[axis, pl.ds(first, IC), :] for axis in range(3)]

            def other_block(first, sums):
                forces, totals = sums
                other = [near_ref[axis:axis + 1, pl.ds(first, 128)] for axis in range(3)]
                force, parts = pair_terms(own, other, span)
                forces = tuple(f + t for f, t in zip(forces, force))
                totals = tuple(t + ((p[0:8] + p[8:16]) + (p[16:24] + p[24:32])) for t, p in zip(totals, parts))
                return forces, totals

            def other_step(j, sums):
                first = pl.multiple_of(j * 256, 256)
                return other_block(first + 128, other_block(first, sums))

            def last_step(j, sums):
                return other_block(pl.multiple_of(n_other * 128 - 128, 128), sums)

            zero = jnp.zeros((IC, 128), jnp.float32)
            sums = lax.fori_loop(0, n_other // 2, other_step, ((zero,) * 3, totals))
            forces, totals = lax.fori_loop(0, n_other % 2, last_step, sums)
            for axis in range(3):
                acc_ref[axis, pl.ds(first, IC), :] = forces[axis]
            return totals

        zero = jnp.zeros((8, 128), jnp.float32)
        well, distance, pairs = lax.fori_loop(0, n_own, own_step, (zero,) * 3)
        energy = 2.0 * well - (0.5 * UPC) * distance - (0.5 * (UCUT - RC * UPC)) * pairs
        en_ref[...] = jnp.sum(energy, axis=0, keepdims=True)

    one_image = side[0, 0] >= 2.0 * RC

    @pl.when(one_image)
    def _():
        sweep(None)

    @pl.when(jnp.logical_not(one_image))
    def _():
        sweep(box)

    def sum_block(b):
        for axis in range(3):
            turned = jnp.transpose(acc_ref[axis, 128 * b:128 * b + 128, :])
            sum_ref[axis:axis + 1, 128 * b:128 * b + 128] = jnp.sum(turned, axis=0, keepdims=True)

    for b in range(NARROW // 128):
        sum_block(b)

    @pl.when(total > NARROW)
    def _():
        for b in range(NARROW // 128, PAD // 128):
            sum_block(b)

    rows = rows_ref[...]
    filled = rows[6:7, :] > 0.5
    force = jnp.where(filled, 24.0 * sum_ref[0:3, :], 0.0)
    frc_ref[...] = force[:, 0:CAP]
    pos_ref[...] = rows[0:3, 0:CAP]
    vel_ref[...] = (rows[3:6, :] + (0.5 * DT) * force)[:, 0:CAP]
    new_id = (rows[6:7, :].astype(jnp.int32) - 1) * 65536 + rows[7:8, :].astype(jnp.int32)
    id_ref[...] = jnp.where(filled, new_id, 0)[:, 0:CAP].reshape(CAP)
    ok_ref[...] = filled.astype(jnp.int32)[:, 0:CAP].reshape(CAP)


def energy_kernel(en_ref, out_ref, parts_ref, send_sem, recv_sem):
    barrier = greet()
    pl.semaphore_wait(barrier, 7)
    copies = []
    for relation in FAR_FIRST:
        copy = pltpu.make_async_remote_copy(src_ref=en_ref, dst_ref=parts_ref.at[relation], send_sem=send_sem.at[relation], recv_sem=recv_sem.at[relation], device_id=partner(relation), device_id_type=MESH_ID)
        copy.start()
        copies.append(copy)
    for copy in copies:
        copy.wait()
    parts_ref[0] = en_ref[...]
    over_x = [parts_ref[k] + parts_ref[k + 1] for k in (0, 2, 4, 6)]
    out_ref[...] = (over_x[0] + over_x[1]) + (over_x[2] + over_x[3])


def solution(mesh):
    vmem = pl.BlockSpec(memory_space=pltpu.VMEM)
    hbm = pl.BlockSpec(memory_space=pltpu.HBM)
    f32, i32 = jnp.float32, jnp.int32

    def shape(dims, dtype=f32):
        return jax.ShapeDtypeStruct(dims, dtype)

    exchange = pl.pallas_call(
        exchange_kernel,
        out_shape=(shape((10, PAD)), shape((8, 1, 3 * PAD)), shape((8, 8, MIG))),
        in_specs=[hbm] * 5 + [pl.BlockSpec(memory_space=pl.ANY)],
        out_specs=(vmem, vmem, vmem),
        scratch_shapes=[pltpu.VMEM((3, CAP), f32)] * 3 + [pltpu.VMEM((CAP,), i32)] * 2 + [pltpu.VMEM((1, 1), f32), pltpu.VMEM((9, PAD), f32), pltpu.SemaphoreType.DMA((6,)), pltpu.SemaphoreType.DMA((2, 8)), pltpu.SemaphoreType.DMA((2, 8))],
        compiler_params=pltpu.CompilerParams(collective_id=0, has_side_effects=True, vmem_limit_bytes=16 << 20),
        name="exchange",
    )
    forces = pl.pallas_call(
        force_kernel,
        out_shape=(shape((3, CAP)), shape((3, CAP)), shape((3, CAP)), shape((CAP,), i32), shape((CAP,), i32), shape((1, 128))),
        in_specs=[vmem] * 3,
        out_specs=(vmem,) * 6,
        scratch_shapes=[pltpu.VMEM((8, FULL), f32), pltpu.VMEM((8, 9 * PAD + 256), f32), pltpu.VMEM((3, PAD, 128), f32), pltpu.VMEM((3, PAD, 128), f32), pltpu.VMEM((3, 8, PAD), f32), pltpu.VMEM((8, 8, PAD + 128), f32), pltpu.VMEM((8, PAD), f32), pltpu.VMEM((1, FULL), f32), pltpu.VMEM((3, PAD), f32), pltpu.SMEM((1,), i32)],
        compiler_params=pltpu.CompilerParams(vmem_limit_bytes=16 << 20),
        name="forces",
    )
    total_energy = pl.pallas_call(
        energy_kernel,
        out_shape=shape((1, 128)),
        in_specs=[vmem],
        out_specs=vmem,
        scratch_shapes=[pltpu.VMEM((8, 1, 128), f32), pltpu.SemaphoreType.DMA((8,)), pltpu.SemaphoreType.DMA((8,))],
        compiler_params=pltpu.CompilerParams(collective_id=1, has_side_effects=True, vmem_limit_bytes=16 << 20),
        name="energy",
    )

    def local_step(atom_pos, atom_vel, atom_frc, atom_id, atom_ok, brick_side):
        arrays = (atom_pos.T, atom_vel.T, atom_frc.T, atom_id, atom_ok, brick_side.reshape(1, 1))
        own, everyone, movers = exchange(*[pltpu.with_memory_space_constraint(array, pltpu.HBM) for array in arrays[:5]], arrays[5])
        pos, vel, frc, new_id, new_ok, partial = forces(own, everyone, movers)
        energy = jnp.sum(total_energy(partial))
        return pos.T, vel.T, frc.T, new_id, new_ok, energy

    row_spec = P(MESH_AXES, None)
    id_spec = P(MESH_AXES)
    return jax.shard_map(local_step, mesh=mesh, in_specs=(row_spec, row_spec, row_spec, id_spec, id_spec, P()), out_specs=(row_spec, row_spec, row_spec, id_spec, id_spec, P()), check_vma=False)
```

```python
import functools

import jax
import jax.numpy as jnp
from jax import lax
from jax.experimental import pallas as pl
from jax.experimental.pallas import tpu as pltpu
from jax.sharding import PartitionSpec as P

DT = 0.005
RC = 2.5
FAR_AWAY = 1.0e6
UCUT = 4.0 * (RC ** -12 - RC ** -6)
UPC = -48.0 * RC ** -13 + 24.0 * RC ** -7
MESH_AXES = ("z", "y", "x")
CAP = 729
PAD = 768
MIG = 256
FULL = PAD + MIG
SEG = {1: (0, 16), 2: (16, 16), 4: (32, 16), 3: (48, 32), 5: (80, 32), 6: (128, 32), 7: (160, 64)}
IC = 32
NARROW = 512
FAR_FIRST = (6, 7, 4, 2, 5, 3, 1)
REACH = RC + 0.01
MESH_ID = pl.DeviceIdType.MESH


def pieces_of(rows):
    first = rows.astype(jnp.bfloat16).astype(jnp.float32)
    rest = rows - first
    second = rest.astype(jnp.bfloat16).astype(jnp.float32)
    third = rest - second
    return jnp.concatenate([first, second, third], axis=0).astype(jnp.bfloat16)


def select_rows(rows, onehot):
    out = lax.dot_general(pieces_of(rows), onehot, (((1,), (1,)), ((), ())), preferred_element_type=jnp.float32)
    return out[0:8] + out[8:16] + out[16:24]


def partner(relation):
    mine = (lax.axis_index("z"), lax.axis_index("y"), lax.axis_index("x"))
    bits = (relation // 4 % 2, relation // 2 % 2, relation % 2)
    return tuple((axis + bit) % 2 for axis, bit in zip(mine, bits))


def greet():
    barrier = pltpu.get_barrier_semaphore()
    for relation in range(1, 8):
        pl.semaphore_signal(barrier, inc=1, device_id=partner(relation), device_id_type=MESH_ID)
    return barrier


def axis_column(values, rows):
    idx = lax.broadcasted_iota(jnp.int32, (rows, 1), 0)
    out = jnp.full((rows, 1), values[-1], jnp.float32)
    for k in range(len(values) - 1):
        out = jnp.where(idx == k, values[k], out)
    return out


def brick_coords():
    return [lax.axis_index(name).astype(jnp.float32) for name in ("x", "y", "z")]


def prefix_counts(member):
    blocks = member.shape[1] // 128
    stacked = jnp.concatenate([member[:, 128 * b:128 * (b + 1)] for b in range(blocks)], axis=0).astype(jnp.bfloat16)
    row = lax.broadcasted_iota(jnp.int32, (128, 256), 0)
    col = lax.broadcasted_iota(jnp.int32, (128, 256), 1)
    ladder = ((row < col) | (col >= 128)).astype(jnp.float32).astype(jnp.bfloat16)
    counts = jnp.dot(stacked, ladder, preferred_element_type=jnp.float32)
    before = jnp.zeros((8, 128), jnp.float32)
    ranks = []
    for b in range(blocks):
        ranks.append(counts[8 * b:8 * b + 8, 0:128] + before)
        before = before + counts[8 * b:8 * b + 8, 128:256]
    return jnp.concatenate(ranks, axis=1), before


def exchange_kernel(pos_hbm, vel_hbm, frc_hbm, id_hbm, ok_hbm, side_hbm, own_ref, all_ref, mig_ref, pos_ref, vel_ref, frc_ref, id_ref, ok_ref, side_ref, pad_ref, load_sem, send_sem, recv_sem):
    loads = []
    for k, (src, dst) in enumerate(((pos_hbm, pos_ref), (vel_hbm, vel_ref), (frc_hbm, frc_ref), (id_hbm, id_ref), (ok_hbm, ok_ref), (side_hbm, side_ref))):
        load = pltpu.make_async_copy(src, dst, load_sem.at[k])
        load.start()
        loads.append(load)
    barrier = greet()
    pad_ref[...] = jnp.zeros_like(pad_ref)
    for load in loads:
        load.wait()
    side = side_ref[...]
    box = side * 2.0
    half_v = vel_ref[...] + (0.5 * DT) * frc_ref[...]
    pad_ref[0:3, 0:CAP] = pos_ref[...] + DT * half_v
    pad_ref[3:6, 0:CAP] = half_v
    pad_ref[6:7, 0:CAP] = (id_ref[...].reshape(1, CAP) >> 16).astype(jnp.float32) + 1.0
    pad_ref[7:8, 0:CAP] = (id_ref[...].reshape(1, CAP) & 65535).astype(jnp.float32)
    pad_ref[8:9, 0:CAP] = ok_ref[...].reshape(1, CAP).astype(jnp.float32)
    unwrapped = pad_ref[0:3, :]
    owned = pad_ref[8:9, :] > 0.5
    moved = jnp.where(unwrapped < 0.0, unwrapped + box, jnp.where(unwrapped >= box, unwrapped - box, unwrapped))
    for axis in range(3):
        all_ref[0, :, PAD * axis:PAD * (axis + 1)] = jnp.where(owned, moved[axis:axis + 1, :], FAR_AWAY)

    low = axis_column([coord * side for coord in brick_coords()], 3)
    outside = (unwrapped < low) | (unwrapped >= low + side)
    bits = jnp.where(outside, axis_column([1.0, 2.0, 4.0], 3), 0.0)
    code = jnp.sum(bits, axis=0, keepdims=True)
    code = jnp.where(owned, code, -1.0)
    relation_col = lax.broadcasted_iota(jnp.int32, (8, PAD), 0).astype(jnp.float32)
    member = code == relation_col
    rank, _ = prefix_counts(member.astype(jnp.float32))
    offset = axis_column([0.0] + [float(SEG[m][0]) for m in range(1, 8)], 8)
    slot = jnp.sum(jnp.where(member, rank + offset, 0.0), axis=0, keepdims=True)
    slot = jnp.where(code > 0.5, slot, -1.0)
    rows = jnp.concatenate([moved, pad_ref[3:8, :]], axis=0)
    slots = lax.broadcasted_iota(jnp.int32, (MIG, PAD), 0).astype(jnp.float32)
    onehot = (slots == slot).astype(jnp.float32).astype(jnp.bfloat16)
    mig_ref[0] = select_rows(rows, onehot)
    own_ref[0:8, :] = rows
    own_ref[8:9, :] = jnp.where(code == 0.0, rank[0:1, :], -1.0)
    own_ref[9:10, :] = jnp.broadcast_to(side, (1, PAD))

    pl.semaphore_wait(barrier, 7)
    copies = []
    for relation in FAR_FIRST:
        block = pl.ds(SEG[relation][0] // 128 * 128, 128)
        for which, src, dst in ((0, mig_ref.at[0, :, block], mig_ref.at[relation, :, block]), (1, all_ref.at[0], all_ref.at[relation])):
            copy = pltpu.make_async_remote_copy(src_ref=src, dst_ref=dst, send_sem=send_sem.at[which, relation], recv_sem=recv_sem.at[which, relation], device_id=partner(relation), device_id_type=MESH_ID)
            copy.start()
            copies.append(copy)
    for copy in copies:
        copy.wait()


def pair_terms(own, other, span):
    delta = []
    for mine, theirs in zip(own, other):
        diff = mine - theirs
        if span is not None:
            diff = diff - jnp.where(diff > 0.5 * span, span, jnp.where(diff < -0.5 * span, -span, 0.0))
        delta.append(diff)
    dist_sq = delta[0] * delta[0] + delta[1] * delta[1] + delta[2] * delta[2]
    in_range = (dist_sq < RC * RC) & (dist_sq > 0.01)
    inv_r = jnp.where(in_range, lax.rsqrt(dist_sq), 0.0)
    inv_r2 = inv_r * inv_r
    inv_r6 = inv_r2 * inv_r2 * inv_r2
    inv_r12 = inv_r6 * inv_r6
    well = inv_r12 - inv_r6
    scale = (well + inv_r12) * inv_r2 + (UPC / 24.0) * inv_r
    return [scale * d for d in delta], [well, dist_sq * inv_r, jnp.where(in_range, 1.0, 0.0)]


def force_kernel(own_ref, all_ref, mig_ref, en_ref, acc_ref, rows_ref, cand_ref, near_ref, mine_ref, plane_ref, list_ref, rank_ref, count_ref):
    side = own_ref[9:10, 0:1]
    box = side * 2.0
    lane = lax.broadcasted_iota(jnp.int32, (1, MIG), 1)
    arrivals = jnp.zeros((8, MIG), jnp.float32)
    for relation, (start, size) in SEG.items():
        arrivals = jnp.where((lane >= start) & (lane < start + size), mig_ref[relation], arrivals)
    cand_ref[:, 0:PAD] = own_ref[0:8, :]
    cand_ref[:, PAD:FULL] = arrivals
    stay_rank = own_ref[8:9, :]
    cand = cand_ref[...]
    valid = jnp.concatenate([stay_rank >= 0.0, arrivals[6:7, :] > 0.5], axis=1)
    total = jnp.sum(valid.astype(jnp.int32))
    tail = all_ref[0, :, NARROW:PAD]
    for relation in range(1, 8):
        tail = jnp.minimum(tail, all_ref[relation, :, NARROW:PAD])
    narrow = (jnp.min(tail) > 0.5 * FAR_AWAY) & (total <= NARROW)
    number = (cand[6:7, :].astype(jnp.int32) - 1) * 65536 + cand[7:8, :].astype(jnp.int32)
    key = jnp.where(valid, number, 2147483647)
    key_col = jnp.transpose(jnp.broadcast_to(key[:, PAD:FULL], (8, MIG)))[:, 0:1]
    below = (key_col < key).astype(jnp.float32).astype(jnp.bfloat16)
    in_front = jnp.dot(jnp.ones((8, MIG), jnp.bfloat16), below, preferred_element_type=jnp.float32)[0:1, :]
    above = lax.dot_general(jnp.ones((8, PAD), jnp.bfloat16), below[:, 0:PAD], (((1,), (1,)), ((), ())), preferred_element_type=jnp.float32)[0:1, :]
    rank = in_front + jnp.concatenate([stay_rank, float(PAD) - above], axis=1)
    rank_ref[...] = jnp.where(valid, rank, -1.0)
    centre = [(coord + 0.5) * side for coord in brick_coords()]

    def prepare(width):
        for relation in range(8):
            for axis in range(3):
                plane_ref[axis, relation:relation + 1, 0:width] = all_ref[relation, :, PAD * axis:PAD * axis + width]
        planes = []
        beyond = jnp.zeros((8, width), jnp.float32)
        for axis in range(3):
            theirs = plane_ref[axis, :, 0:width] - centre[axis]
            theirs = jnp.where(theirs > side, theirs - box, jnp.where(theirs < -side, theirs + box, theirs))
            excess = jnp.maximum(jnp.abs(theirs) - 0.5 * side, 0.0)
            beyond = beyond + excess * excess
            planes.append(theirs)
        keep = (beyond < REACH * REACH) & (beyond > 0.0)
        front, held = prefix_counts(keep.astype(jnp.float32))
        lanes = lax.broadcasted_iota(jnp.int32, (8, width), 1)
        hops = jnp.where(keep, lanes - front.astype(jnp.int32), 0)

        ranks = jnp.concatenate([rank_ref[:, 0:width], rank_ref[:, PAD:FULL]], axis=1)
        pieces = pieces_of(jnp.concatenate([cand_ref[:, 0:width], cand_ref[:, PAD:FULL]], axis=1))
        slots = lax.broadcasted_iota(jnp.int32, (128, width + MIG), 0).astype(jnp.float32)
        blocks = width // 128
        done = 0
        for bit in range(10 if width > 512 else 9):
            step = 1 << bit
            coming = pltpu.roll(hops, width - step, 1)
            take = (coming & step) != 0
            leave = (hops & step) != 0
            hops = jnp.where(take, coming, jnp.where(leave, 0, hops))
            planes = [jnp.where(take, pltpu.roll(plane, width - step, 1), plane) for plane in planes]
            if done < blocks:
                onehot = (slots == ranks - 128.0 * done).astype(jnp.float32).astype(jnp.bfloat16)
                out = lax.dot_general(pieces, onehot, (((1,), (1,)), ((), ())), preferred_element_type=jnp.float32)
                rows_ref[:, 128 * done:128 * done + 128] = out[0:8] + out[8:16] + out[16:24]
                done += 1
        if width < PAD:
            rows_ref[:, width:PAD] = jnp.zeros((8, PAD - width), jnp.float32)

        rows = rows_ref[:, 0:width]
        filled = rows[6:7, :] > 0.5
        local = rows[0:3, :] - axis_column(centre, 3)
        near_ref[0:3, 0:width] = jnp.where(filled, local, FAR_AWAY)
        local = jnp.concatenate([jnp.where(filled, local, -FAR_AWAY), jnp.zeros((5, width), jnp.float32)], axis=0)
        piece_row = lax.broadcasted_iota(jnp.int32, (24, 384), 0) % 8
        piece_col = lax.broadcasted_iota(jnp.int32, (24, 384), 1) // 128
        spread = (piece_row == piece_col).astype(jnp.float32).astype(jnp.bfloat16)
        columns = lax.dot_general(pieces_of(local), spread, (((0,), (0,)), ((), ())), preferred_element_type=jnp.float32)
        for axis in range(3):
            mine_ref[axis, 0:width, :] = columns[:, 128 * axis:128 * axis + 128]

        for relation in range(8):
            for axis in range(3):
                list_ref[relation, axis:axis + 1, 0:width] = planes[axis][relation:relation + 1, :]
        held = held.astype(jnp.int32)
        lane128 = lax.broadcasted_iota(jnp.int32, (8, 128), 1)
        start = total
        for relation in range(8):
            into = start % 128
            first = pl.multiple_of(start - into, 128)
            turned = pltpu.roll(list_ref[relation, :, 0:width + 128], into, 1)
            near_ref[:, pl.ds(first, 128)] = jnp.where(lane128 < into, near_ref[:, pl.ds(first, 128)], turned[:, 0:128])
            near_ref[:, pl.ds(pl.multiple_of(first + 128, 128), width)] = turned[:, 128:width + 128]
            start = start + held[relation, 0]
        into = start % 128
        first = pl.multiple_of(start - into, 128)
        near_ref[:, pl.ds(first, 128)] = jnp.where(lane128 < into, near_ref[:, pl.ds(first, 128)], FAR_AWAY)
        count_ref[0] = (start + 127) // 128

    @pl.when(narrow)
    def _():
        prepare(NARROW)

    @pl.when(jnp.logical_not(narrow))
    def _():
        prepare(PAD)

    n_other = count_ref[0]
    n_own = (total + IC - 1) // IC

    def sweep(span):
        def own_step(i, totals):
            first = pl.multiple_of(i * IC, IC)
            own = [mine_ref[axis, pl.ds(first, IC), :] for axis in range(3)]

            def other_block(first, sums):
                forces, totals = sums
                other = [near_ref[axis:axis + 1, pl.ds(first, 128)] for axis in range(3)]
                force, parts = pair_terms(own, other, span)
                forces = tuple(f + t for f, t in zip(forces, force))
                totals = tuple(t + ((p[0:8] + p[8:16]) + (p[16:24] + p[24:32])) for t, p in zip(totals, parts))
                return forces, totals

            def other_step(j, sums):
                first = pl.multiple_of(j * 256, 256)
                return other_block(first + 128, other_block(first, sums))

            def last_step(j, sums):
                return other_block(pl.multiple_of(n_other * 128 - 128, 128), sums)

            zero = jnp.zeros((IC, 128), jnp.float32)
            sums = lax.fori_loop(0, n_other // 2, other_step, ((zero,) * 3, totals))
            forces, totals = lax.fori_loop(0, n_other % 2, last_step, sums)
            for axis in range(3):
                acc_ref[axis, pl.ds(first, IC), :] = forces[axis]
            return totals

        zero = jnp.zeros((8, 128), jnp.float32)
        well, distance, pairs = lax.fori_loop(0, n_own, own_step, (zero,) * 3)
        energy = 2.0 * well - (0.5 * UPC) * distance - (0.5 * (UCUT - RC * UPC)) * pairs
        en_ref[...] = jnp.sum(energy, axis=0, keepdims=True)

    one_image = side[0, 0] >= 2.0 * RC

    @pl.when(one_image)
    def _():
        sweep(None)

    @pl.when(jnp.logical_not(one_image))
    def _():
        sweep(box)


def energy_kernel(en_ref, acc_ref, rows_ref, sum_ref, pos_ref, vel_ref, frc_ref, id_ref, ok_ref, force_ref, parts_ref, send_sem, recv_sem):
    barrier = greet()
    for axis in range(3):
        for b in range(PAD // 128):
            block = slice(128 * b, 128 * b + 128)
            force_ref[axis:axis + 1, block] = jnp.sum(jnp.transpose(acc_ref[axis, block, :]), axis=0, keepdims=True)
    pl.semaphore_wait(barrier, 7)
    copies = []
    for relation in FAR_FIRST:
        copy = pltpu.make_async_remote_copy(src_ref=en_ref, dst_ref=parts_ref.at[relation], send_sem=send_sem.at[relation], recv_sem=recv_sem.at[relation], device_id=partner(relation), device_id_type=MESH_ID)
        copy.start()
        copies.append(copy)
    rows = rows_ref[...]
    filled = rows[6:7, :] > 0.5
    force = jnp.where(filled, 24.0 * force_ref[...], 0.0)
    frc_ref[...] = force[:, 0:CAP]
    pos_ref[...] = rows[0:3, 0:CAP]
    vel_ref[...] = (rows[3:6, :] + (0.5 * DT) * force)[:, 0:CAP]
    new_id = (rows[6:7, :].astype(jnp.int32) - 1) * 65536 + rows[7:8, :].astype(jnp.int32)
    id_ref[...] = jnp.where(filled, new_id, 0)[:, 0:CAP].reshape(CAP)
    ok_ref[...] = filled.astype(jnp.int32)[:, 0:CAP].reshape(CAP)
    for copy in copies:
        copy.wait()
    parts_ref[0] = en_ref[...]
    over_x = [parts_ref[k] + parts_ref[k + 1] for k in (0, 2, 4, 6)]
    sum_ref[...] = (over_x[0] + over_x[1]) + (over_x[2] + over_x[3])


def store_kernel(sum_ref, *refs):
    sources, targets, total_ref, store_sem = refs[0:5], refs[5:11], refs[11], refs[12]
    stores = [pltpu.make_async_copy(sources[k], targets[k], store_sem.at[k]) for k in range(5)]
    for store in stores:
        store.start()
    total_ref[...] = jnp.sum(sum_ref[...], axis=1, keepdims=True)
    stores.append(pltpu.make_async_copy(total_ref, targets[5], store_sem.at[5]))
    stores[5].start()
    for store in stores:
        store.wait()


def solution(mesh):
    vmem = pl.BlockSpec(memory_space=pltpu.VMEM)
    hbm = pl.BlockSpec(memory_space=pltpu.HBM)
    f32, i32 = jnp.float32, jnp.int32

    def shape(dims, dtype=f32):
        return jax.ShapeDtypeStruct(dims, dtype)

    exchange = pl.pallas_call(
        exchange_kernel,
        out_shape=(shape((10, PAD)), shape((8, 1, 3 * PAD)), shape((8, 8, MIG))),
        in_specs=[hbm] * 5 + [pl.BlockSpec(memory_space=pl.ANY)],
        out_specs=(vmem, vmem, vmem),
        scratch_shapes=[pltpu.VMEM((3, CAP), f32)] * 3 + [pltpu.VMEM((CAP,), i32)] * 2 + [pltpu.VMEM((1, 1), f32), pltpu.VMEM((9, PAD), f32), pltpu.SemaphoreType.DMA((6,)), pltpu.SemaphoreType.DMA((2, 8)), pltpu.SemaphoreType.DMA((2, 8))],
        compiler_params=pltpu.CompilerParams(collective_id=0, has_side_effects=True, vmem_limit_bytes=16 << 20),
        name="exchange",
    )
    forces = pl.pallas_call(
        force_kernel,
        out_shape=(shape((1, 128)), shape((3, PAD, 128)), shape((8, PAD))),
        in_specs=[vmem] * 3,
        out_specs=(vmem,) * 3,
        scratch_shapes=[pltpu.VMEM((8, FULL), f32), pltpu.VMEM((8, 9 * PAD + 256), f32), pltpu.VMEM((3, PAD, 128), f32), pltpu.VMEM((3, 8, PAD), f32), pltpu.VMEM((8, 8, PAD + 128), f32), pltpu.VMEM((1, FULL), f32), pltpu.SMEM((1,), i32)],
        compiler_params=pltpu.CompilerParams(vmem_limit_bytes=16 << 20),
        name="forces",
    )
    results = (shape((3, CAP)), shape((3, CAP)), shape((3, CAP)), shape((CAP,), i32), shape((CAP,), i32))
    total_energy = pl.pallas_call(
        energy_kernel,
        out_shape=(shape((1, 128)),) + results,
        in_specs=[vmem] * 3,
        out_specs=(vmem,) * 6,
        scratch_shapes=[pltpu.VMEM((3, PAD), f32), pltpu.VMEM((8, 1, 128), f32), pltpu.SemaphoreType.DMA((8,)), pltpu.SemaphoreType.DMA((8,))],
        compiler_params=pltpu.CompilerParams(collective_id=1, has_side_effects=True, vmem_limit_bytes=16 << 20),
        name="energy",
    )
    store = pl.pallas_call(
        store_kernel,
        out_shape=results + (shape((1, 1)),),
        in_specs=[vmem] * 6,
        out_specs=(hbm,) * 6,
        scratch_shapes=[pltpu.VMEM((1, 1), f32), pltpu.SemaphoreType.DMA((6,))],
        compiler_params=pltpu.CompilerParams(vmem_limit_bytes=16 << 20),
        name="store",
    )

    def local_step(atom_pos, atom_vel, atom_frc, atom_id, atom_ok, brick_side):
        arrays = (atom_pos.T, atom_vel.T, atom_frc.T, atom_id, atom_ok, brick_side.reshape(1, 1))
        own, everyone, movers = exchange(*[pltpu.with_memory_space_constraint(array, pltpu.HBM) for array in arrays[:5]], arrays[5])
        partial, sums, rows = forces(own, everyone, movers)
        pos, vel, frc, new_id, new_ok, energy = store(*total_energy(partial, sums, rows))
        return pos.T, vel.T, frc.T, new_id, new_ok, energy.reshape(())

    row_spec = P(MESH_AXES, None)
    id_spec = P(MESH_AXES)
    return jax.shard_map(local_step, mesh=mesh, in_specs=(row_spec, row_spec, row_spec, id_spec, id_spec, P()), out_specs=(row_spec, row_spec, row_spec, id_spec, id_spec, P()), check_vma=False)
```

```python
import functools

import jax
import jax.numpy as jnp
from jax import lax
from jax.experimental import pallas as pl
from jax.experimental.pallas import tpu as pltpu
from jax.sharding import PartitionSpec as P

DT = 0.005
RC = 2.5
FAR_AWAY = 1.0e6
UCUT = 4.0 * (RC ** -12 - RC ** -6)
UPC = -48.0 * RC ** -13 + 24.0 * RC ** -7
MESH_AXES = ("z", "y", "x")
CAP = 729
PAD = 768
MIG = 256
SEG = {1: (0, 16), 2: (16, 16), 4: (32, 16), 3: (48, 32), 5: (80, 32), 6: (128, 32), 7: (160, 64)}
IC = 32
NARROW = 512
LANES = 128
ID_SPLIT = 65536
NT = (((1,), (1,)), ((), ()))
OTHERS = tuple(range(1, 8))
FAR_FIRST = (6, 7, 4, 2, 5, 3, 1)
REACH = RC + 0.01
MESH_ID = pl.DeviceIdType.MESH


def pieces_of(rows):
    first = rows.astype(jnp.bfloat16).astype(jnp.float32)
    rest = rows - first
    second = rest.astype(jnp.bfloat16).astype(jnp.float32)
    third = rest - second
    return jnp.concatenate([first, second, third], axis=0).astype(jnp.bfloat16)


def select_rows(rows, onehot):
    out = lax.dot_general(pieces_of(rows), onehot, NT, preferred_element_type=jnp.float32)
    return sum_groups(out, rows.shape[0])


def sum_groups(rows, size):
    total = rows[0:size]
    for k in range(size, rows.shape[0], size):
        total = total + rows[k:k + size]
    return total


def as_bf16(mask):
    return mask.astype(jnp.float32).astype(jnp.bfloat16)


def iota(dims, axis, dtype=jnp.float32):
    return lax.broadcasted_iota(jnp.int32, dims, axis).astype(dtype)


def id_of(rows):
    return (rows[6:7].astype(jnp.int32) - 1) * ID_SPLIT + rows[7:8].astype(jnp.int32)


def partner(relation):
    return tuple((lax.axis_index(name) + relation // bit) % 2 for name, bit in zip(MESH_AXES, (4, 2, 1)))


def greet():
    barrier = pltpu.get_barrier_semaphore()
    for relation in OTHERS:
        pl.semaphore_signal(barrier, inc=1, device_id=partner(relation), device_id_type=MESH_ID)
    return barrier


def send_all(pairs, send_sem, recv_sem):
    copies = []
    for relation in FAR_FIRST:
        for which, (src, dst) in enumerate(pairs(relation)):
            copy = pltpu.make_async_remote_copy(src_ref=src, dst_ref=dst, send_sem=send_sem.at[which, relation], recv_sem=recv_sem.at[which, relation], device_id=partner(relation), device_id_type=MESH_ID)
            copy.start()
            copies.append(copy)
    return copies


def axis_column(values, rows):
    idx = lax.broadcasted_iota(jnp.int32, (rows, 1), 0)
    out = jnp.full((rows, 1), values[-1], jnp.float32)
    for k in range(len(values) - 1):
        out = jnp.where(idx == k, values[k], out)
    return out


def brick_coords():
    return [lax.axis_index(name).astype(jnp.float32) for name in ("x", "y", "z")]


def prefix_counts(member):
    member = member.astype(jnp.float32)
    starts = range(0, member.shape[1], LANES)
    stacked = as_bf16(jnp.concatenate([member[:, k:k + LANES] for k in starts], axis=0) > 0.5)
    col = iota((LANES, 2 * LANES), 1)
    ladder = as_bf16((iota((LANES, 2 * LANES), 0) < col) | (col >= LANES))
    counts = jnp.dot(stacked, ladder, preferred_element_type=jnp.float32)
    before = jnp.zeros((8, LANES), jnp.float32)
    ranks = []
    for k in range(0, counts.shape[0], 8):
        ranks.append(counts[k:k + 8, 0:LANES] + before)
        before = before + counts[k:k + 8, LANES:]
    return jnp.concatenate(ranks, axis=1), before


def exchange_kernel(pos_hbm, vel_hbm, frc_hbm, id_hbm, ok_hbm, side_hbm, own_ref, all_ref, mig_ref, pos_ref, vel_ref, frc_ref, id_ref, ok_ref, side_ref, pad_ref, load_sem, send_sem, recv_sem):
    loads = []
    for k, (src, dst) in enumerate(((pos_hbm, pos_ref), (vel_hbm, vel_ref), (frc_hbm, frc_ref), (id_hbm, id_ref), (ok_hbm, ok_ref), (side_hbm, side_ref))):
        load = pltpu.make_async_copy(src, dst, load_sem.at[k])
        load.start()
        loads.append(load)
    barrier = greet()
    pad_ref[...] = jnp.zeros_like(pad_ref)
    for load in loads:
        load.wait()
    side = side_ref[...]
    box = side * 2.0
    half_v = vel_ref[...] + (0.5 * DT) * frc_ref[...]
    pad_ref[0:3, 0:CAP] = pos_ref[...] + DT * half_v
    pad_ref[3:6, 0:CAP] = half_v
    pad_ref[6:7, 0:CAP] = (id_ref[...].reshape(1, CAP) // ID_SPLIT).astype(jnp.float32) + 1.0
    pad_ref[7:8, 0:CAP] = (id_ref[...].reshape(1, CAP) % ID_SPLIT).astype(jnp.float32)
    pad_ref[8:9, 0:CAP] = ok_ref[...].reshape(1, CAP).astype(jnp.float32)
    unwrapped = pad_ref[0:3, :]
    owned = pad_ref[8:9, :] > 0.5
    moved = jnp.where(unwrapped < 0.0, unwrapped + box, jnp.where(unwrapped >= box, unwrapped - box, unwrapped))
    for axis in range(3):
        all_ref[0, :, PAD * axis:PAD * (axis + 1)] = jnp.where(owned, moved[axis:axis + 1, :], FAR_AWAY)

    low = axis_column([coord * side for coord in brick_coords()], 3)
    outside = (unwrapped < low) | (unwrapped >= low + side)
    bits = jnp.where(outside, axis_column([1.0, 2.0, 4.0], 3), 0.0)
    code = jnp.sum(bits, axis=0, keepdims=True)
    code = jnp.where(owned, code, -1.0)
    member = code == iota((8, PAD), 0)
    rank, _ = prefix_counts(member)
    offset = axis_column([0.0] + [float(SEG[m][0]) for m in OTHERS], 8)
    slot = jnp.sum(jnp.where(member, rank + offset, 0.0), axis=0, keepdims=True)
    rows = jnp.concatenate([moved, pad_ref[3:8, :]], axis=0)
    mig_ref[0] = select_rows(rows, as_bf16(iota((MIG, PAD), 0) == jnp.where(code > 0.5, slot, -1.0)))
    own_ref[8:9, :] = jnp.broadcast_to(side, (1, PAD))

    def pairs(relation):
        block = pl.ds(SEG[relation][0] // LANES * LANES, LANES)
        return (mig_ref.at[0, :, block], mig_ref.at[relation, :, block]), (all_ref.at[0], all_ref.at[relation])

    pl.semaphore_wait(barrier, len(OTHERS))
    copies = send_all(pairs, send_sem, recv_sem)
    pieces = pieces_of(rows)
    slots = iota((LANES, PAD), 0)
    slot = jnp.where(code == 0.0, slot, -1.0)

    def pack(k, carry):
        first = k * LANES
        out = lax.dot_general(pieces, as_bf16(slots == slot - first.astype(jnp.float32)), NT, preferred_element_type=jnp.float32)
        own_ref[0:8, pl.ds(pl.multiple_of(first, LANES), LANES)] = sum_groups(out, 8)
        return carry

    lax.fori_loop(0, PAD // LANES, pack, 0)
    for copy in copies:
        copy.wait()


def pair_terms(own, other, span):
    delta = []
    for mine, theirs in zip(own, other):
        diff = mine - theirs
        if span is not None:
            diff = diff - jnp.where(diff > 0.5 * span, span, jnp.where(diff < -0.5 * span, -span, 0.0))
        delta.append(diff)
    dist_sq = delta[0] * delta[0] + delta[1] * delta[1] + delta[2] * delta[2]
    in_range = (dist_sq < RC * RC) & (dist_sq > 0.01)
    inv_r = jnp.where(in_range, lax.rsqrt(dist_sq), 0.0)
    inv_r2 = inv_r * inv_r
    inv_r6 = inv_r2 * inv_r2 * inv_r2
    inv_r12 = inv_r6 * inv_r6
    well = inv_r12 - inv_r6
    scale = (well + inv_r12) * inv_r2 + (UPC / 24.0) * inv_r
    return [scale * d for d in delta], [well, dist_sq * inv_r, jnp.where(in_range, 1.0, 0.0)]


def force_kernel(own_ref, all_ref, mig_ref, en_ref, acc_ref, rows_ref, near_ref, mine_ref, plane_ref, list_ref, count_ref):
    side = own_ref[8:9, 0:1]
    box = side * 2.0
    lane = iota((1, MIG), 1, jnp.int32)
    arrivals = jnp.zeros((8, MIG), jnp.float32)
    for relation, (start, size) in SEG.items():
        arrivals = jnp.where((lane >= start) & (lane < start + size), mig_ref[relation], arrivals)
    arrived = arrivals[6:7, :] > 0.5
    staying = (own_ref[6:7, :] > 0.5).astype(jnp.float32)
    n_staying = jnp.sum(staying, axis=1, keepdims=True)
    total = jnp.sum((n_staying + jnp.sum(arrived.astype(jnp.float32), axis=1, keepdims=True)).astype(jnp.int32))
    tail = all_ref[0, :, NARROW:PAD]
    for relation in OTHERS:
        tail = jnp.minimum(tail, all_ref[relation, :, NARROW:PAD])
    narrow = (jnp.min(tail) > 0.5 * FAR_AWAY) & (total <= NARROW)
    slot, _ = prefix_counts(jnp.broadcast_to(arrived, (8, MIG)))
    slot = jnp.where(arrived, slot[0:1, :] + n_staying, -1.0)
    pieces = pieces_of(arrivals)
    centre = [(coord + 0.5) * side for coord in brick_coords()]

    def prepare(width):
        for relation in range(8):
            for axis in range(3):
                plane_ref[axis, relation:relation + 1, 0:width] = all_ref[relation, :, PAD * axis:PAD * axis + width]
        planes = []
        beyond = jnp.zeros((8, width), jnp.float32)
        for axis in range(3):
            theirs = plane_ref[axis, :, 0:width] - centre[axis]
            theirs = jnp.where(theirs > side, theirs - box, jnp.where(theirs < -side, theirs + box, theirs))
            excess = jnp.maximum(jnp.abs(theirs) - 0.5 * side, 0.0)
            beyond = beyond + excess * excess
            planes.append(theirs)
        keep = (beyond < REACH * REACH) & (beyond > 0.0)
        front, held = prefix_counts(keep)
        lanes = iota((8, width), 1, jnp.int32)
        hops = jnp.where(keep, lanes - front.astype(jnp.int32), 0)

        slots = iota((LANES, MIG), 0)
        done = 0
        for bit in range(10 if width > 512 else 9):
            step = 1 << bit
            coming = pltpu.roll(hops, width - step, 1)
            take = (coming & step) != 0
            leave = (hops & step) != 0
            hops = jnp.where(take, coming, jnp.where(leave, 0, hops))
            planes = [jnp.where(take, pltpu.roll(plane, width - step, 1), plane) for plane in planes]
            if done < width:
                out = lax.dot_general(pieces, as_bf16(slots == slot - float(done)), NT, preferred_element_type=jnp.float32)
                rows_ref[:, done:done + LANES] = own_ref[0:8, done:done + LANES] + sum_groups(out, 8)
                done += LANES
        if width < PAD:
            rows_ref[:, width:PAD] = jnp.zeros((8, PAD - width), jnp.float32)

        rows = rows_ref[:, 0:width]
        filled = rows[6:7, :] > 0.5
        local = rows[0:3, :] - axis_column(centre, 3)
        near_ref[0:3, 0:width] = jnp.where(filled, local, FAR_AWAY)
        local = jnp.concatenate([jnp.where(filled, local, -FAR_AWAY), jnp.zeros((5, width), jnp.float32)], axis=0)
        spread = as_bf16(iota((24, 3 * LANES), 0, jnp.int32) % 8 == iota((24, 3 * LANES), 1, jnp.int32) // LANES)
        columns = lax.dot_general(pieces_of(local), spread, (((0,), (0,)), ((), ())), preferred_element_type=jnp.float32)
        for axis in range(3):
            mine_ref[axis, 0:width, :] = columns[:, LANES * axis:LANES * (axis + 1)]

        for relation in range(8):
            for axis in range(3):
                list_ref[relation, axis:axis + 1, 0:width] = planes[axis][relation:relation + 1, :]
        held = held.astype(jnp.int32)
        lane128 = iota((8, LANES), 1, jnp.int32)
        start = total
        for relation in range(8):
            into = start % LANES
            first = pl.multiple_of(start - into, LANES)
            turned = pltpu.roll(list_ref[relation, :, 0:width + LANES], into, 1)
            near_ref[:, pl.ds(first, LANES)] = jnp.where(lane128 < into, near_ref[:, pl.ds(first, LANES)], turned[:, 0:LANES])
            near_ref[:, pl.ds(pl.multiple_of(first + LANES, LANES), width)] = turned[:, LANES:]
            start = start + held[relation, 0]
        into = start % LANES
        first = pl.multiple_of(start - into, LANES)
        near_ref[:, pl.ds(first, LANES)] = jnp.where(lane128 < into, near_ref[:, pl.ds(first, LANES)], FAR_AWAY)
        count_ref[0] = (start + LANES - 1) // LANES

    @pl.when(narrow)
    def _():
        prepare(NARROW)

    @pl.when(jnp.logical_not(narrow))
    def _():
        prepare(PAD)

    n_other = count_ref[0]
    n_own = (total + IC - 1) // IC

    def sweep(span):
        def own_step(i, totals):
            first = pl.multiple_of(i * IC, IC)
            own = [mine_ref[axis, pl.ds(first, IC), :] for axis in range(3)]

            def other_block(first, sums):
                forces, totals = sums
                other = [near_ref[axis:axis + 1, pl.ds(first, LANES)] for axis in range(3)]
                force, parts = pair_terms(own, other, span)
                forces = tuple(f + t for f, t in zip(forces, force))
                totals = tuple(t + sum_groups(p, 8) for t, p in zip(totals, parts))
                return forces, totals

            def other_step(j, sums):
                first = pl.multiple_of(j * 2 * LANES, 2 * LANES)
                return other_block(first + LANES, other_block(first, sums))

            def last_step(j, sums):
                return other_block(pl.multiple_of((n_other - 1) * LANES, LANES), sums)

            zero = jnp.zeros((IC, LANES), jnp.float32)
            sums = lax.fori_loop(0, n_other // 2, other_step, ((zero,) * 3, totals))
            forces, totals = lax.fori_loop(0, n_other % 2, last_step, sums)
            for axis in range(3):
                acc_ref[axis, pl.ds(first, IC), :] = forces[axis]
            return totals

        zero = jnp.zeros((8, LANES), jnp.float32)
        well, distance, pairs = lax.fori_loop(0, n_own, own_step, (zero,) * 3)
        energy = 2.0 * well - (0.5 * UPC) * distance - (0.5 * (UCUT - RC * UPC)) * pairs
        en_ref[...] = jnp.sum(energy, axis=0, keepdims=True)

    one_image = side[0, 0] >= 2.0 * RC

    @pl.when(one_image)
    def _():
        sweep(None)

    @pl.when(jnp.logical_not(one_image))
    def _():
        sweep(box)


def energy_kernel(en_ref, acc_ref, rows_ref, sum_ref, pos_ref, vel_ref, frc_ref, id_ref, ok_ref, force_ref, parts_ref, send_sem, recv_sem):
    barrier = greet()
    pl.semaphore_wait(barrier, len(OTHERS))
    copies = send_all(lambda relation: ((en_ref, parts_ref.at[relation]),), send_sem, recv_sem)
    def turn(k, carry):
        block = pl.ds(pl.multiple_of(k * LANES, LANES), LANES)
        for axis in range(3):
            force_ref[axis:axis + 1, block] = jnp.sum(jnp.transpose(acc_ref[axis, block, :]), axis=0, keepdims=True)
        return carry

    lax.fori_loop(0, PAD // LANES, turn, 0)
    rows = rows_ref[...]
    filled = rows[6:7, :] > 0.5
    key = jnp.where(filled, id_of(rows), 2147483647)
    key_col = jnp.transpose(jnp.broadcast_to(key, (8, PAD)))[:, 0:1]
    slot = jnp.dot(jnp.ones((8, PAD), jnp.bfloat16), as_bf16(key_col < key), preferred_element_type=jnp.float32)[0:1, :]
    onehot = as_bf16(iota((PAD, PAD), 0) == jnp.where(filled, slot, -1.0))
    force_ref[0:3, :] = jnp.where(filled, (24.0 * force_ref[0:3, :]), 0.0)
    force_ref[3:8, :] = jnp.zeros((5, PAD), jnp.float32)
    out = select_rows(jnp.concatenate([rows, force_ref[...]], axis=0), onehot)[:, 0:CAP]
    force = out[8:11]
    filled = out[6:7] > 0.5
    frc_ref[...] = force
    pos_ref[...] = out[0:3]
    vel_ref[...] = out[3:6] + (0.5 * DT) * force
    id_ref[...] = jnp.where(filled, id_of(out), 0).reshape(CAP)
    ok_ref[...] = filled.astype(jnp.int32).reshape(CAP)
    for copy in copies:
        copy.wait()
    parts_ref[0] = en_ref[...]
    level = [parts_ref[relation] for relation in range(8)]
    while len(level) > 1:
        level = [one + two for one, two in zip(level[0::2], level[1::2])]
    sum_ref[...] = level[0]


def store_kernel(sum_ref, *refs):
    sources, targets, total_ref, store_sem = refs[0:5], refs[5:11], refs[11], refs[12]
    stores = [pltpu.make_async_copy(sources[k], targets[k], store_sem.at[k]) for k in range(5)]
    for store in stores:
        store.start()
    total_ref[...] = jnp.sum(sum_ref[...], axis=1, keepdims=True)
    stores.append(pltpu.make_async_copy(total_ref, targets[5], store_sem.at[5]))
    stores[5].start()
    for store in stores:
        store.wait()


def solution(mesh):
    vmem = pl.BlockSpec(memory_space=pltpu.VMEM)
    hbm = pl.BlockSpec(memory_space=pltpu.HBM)
    f32, i32 = jnp.float32, jnp.int32

    def shape(dims, dtype=f32):
        return jax.ShapeDtypeStruct(dims, dtype)

    exchange = pl.pallas_call(
        exchange_kernel,
        out_shape=(shape((9, PAD)), shape((8, 1, 3 * PAD)), shape((8, 8, MIG))),
        in_specs=[hbm] * 5 + [pl.BlockSpec(memory_space=pl.ANY)],
        out_specs=(vmem, vmem, vmem),
        scratch_shapes=[pltpu.VMEM((3, CAP), f32)] * 3 + [pltpu.VMEM((CAP,), i32)] * 2 + [pltpu.VMEM((1, 1), f32), pltpu.VMEM((9, PAD), f32), pltpu.SemaphoreType.DMA((6,)), pltpu.SemaphoreType.DMA((2, 8)), pltpu.SemaphoreType.DMA((2, 8))],
        compiler_params=pltpu.CompilerParams(collective_id=0, has_side_effects=True, vmem_limit_bytes=16 << 20),
        name="exchange",
    )
    forces = pl.pallas_call(
        force_kernel,
        out_shape=(shape((1, 128)), shape((3, PAD, 128)), shape((8, PAD))),
        in_specs=[vmem] * 3,
        out_specs=(vmem,) * 3,
        scratch_shapes=[pltpu.VMEM((8, 9 * PAD + 256), f32), pltpu.VMEM((3, PAD, 128), f32), pltpu.VMEM((3, 8, PAD), f32), pltpu.VMEM((8, 8, PAD + 128), f32), pltpu.SMEM((1,), i32)],
        compiler_params=pltpu.CompilerParams(vmem_limit_bytes=16 << 20),
        name="forces",
    )
    results = (shape((3, CAP)), shape((3, CAP)), shape((3, CAP)), shape((CAP,), i32), shape((CAP,), i32))
    total_energy = pl.pallas_call(
        energy_kernel,
        out_shape=(shape((1, 128)),) + results,
        in_specs=[vmem] * 3,
        out_specs=(vmem,) * 6,
        scratch_shapes=[pltpu.VMEM((8, PAD), f32), pltpu.VMEM((8, 1, LANES), f32), pltpu.SemaphoreType.DMA((1, 8)), pltpu.SemaphoreType.DMA((1, 8))],
        compiler_params=pltpu.CompilerParams(collective_id=1, has_side_effects=True, vmem_limit_bytes=16 << 20),
        name="energy",
    )
    store = pl.pallas_call(
        store_kernel,
        out_shape=results + (shape((1, 1)),),
        in_specs=[vmem] * 6,
        out_specs=(hbm,) * 6,
        scratch_shapes=[pltpu.VMEM((1, 1), f32), pltpu.SemaphoreType.DMA((6,))],
        compiler_params=pltpu.CompilerParams(vmem_limit_bytes=16 << 20),
        name="store",
    )

    def local_step(atom_pos, atom_vel, atom_frc, atom_id, atom_ok, brick_side):
        arrays = (atom_pos.T, atom_vel.T, atom_frc.T, atom_id, atom_ok, brick_side.reshape(1, 1))
        own, everyone, movers = exchange(*[pltpu.with_memory_space_constraint(array, pltpu.HBM) for array in arrays[:5]], arrays[5])
        partial, sums, rows = forces(own, everyone, movers)
        pos, vel, frc, new_id, new_ok, energy = store(*total_energy(partial, sums, rows))
        return pos.T, vel.T, frc.T, new_id, new_ok, energy.reshape(())

    row_spec = P(MESH_AXES, None)
    id_spec = P(MESH_AXES)
    return jax.shard_map(local_step, mesh=mesh, in_specs=(row_spec, row_spec, row_spec, id_spec, id_spec, P()), out_specs=(row_spec, row_spec, row_spec, id_spec, id_spec, P()), check_vma=False)
```

```python
import functools

import jax
import jax.numpy as jnp
from jax import lax
from jax.experimental import pallas as pl
from jax.experimental.pallas import tpu as pltpu
from jax.sharding import PartitionSpec as P

DT = 0.005
RC = 2.5
FAR_AWAY = 1.0e6
UCUT = 4.0 * (RC ** -12 - RC ** -6)
UPC = -48.0 * RC ** -13 + 24.0 * RC ** -7
MESH_AXES = ("z", "y", "x")
CAP = 729
PAD = 768
MIG = 256
SEG = {1: (0, 16), 2: (16, 16), 4: (32, 16), 3: (48, 32), 5: (80, 32), 6: (128, 32), 7: (160, 64)}
IC = 32
NARROW = 512
LANES = 128
ID_SPLIT = 65536
NT = (((1,), (1,)), ((), ()))
OTHERS = tuple(range(1, 8))
FAR_FIRST = (6, 7, 4, 2, 5, 3, 1)
REACH = RC + 0.01
MESH_ID = pl.DeviceIdType.MESH


def pieces_of(rows):
    first = rows.astype(jnp.bfloat16).astype(jnp.float32)
    rest = rows - first
    second = rest.astype(jnp.bfloat16).astype(jnp.float32)
    third = rest - second
    return jnp.concatenate([first, second, third], axis=0).astype(jnp.bfloat16)


def select_rows(rows, onehot):
    out = lax.dot_general(pieces_of(rows), onehot, NT, preferred_element_type=jnp.float32)
    return sum_groups(out, rows.shape[0])


def sum_groups(rows, size):
    total = rows[0:size]
    for k in range(size, rows.shape[0], size):
        total = total + rows[k:k + size]
    return total


def as_bf16(mask):
    return mask.astype(jnp.float32).astype(jnp.bfloat16)


def iota(dims, axis, dtype=jnp.float32):
    return lax.broadcasted_iota(jnp.int32, dims, axis).astype(dtype)


def id_of(rows):
    return (rows[6:7].astype(jnp.int32) - 1) * ID_SPLIT + rows[7:8].astype(jnp.int32)


def partner(relation):
    return tuple((lax.axis_index(name) + relation // bit) % 2 for name, bit in zip(MESH_AXES, (4, 2, 1)))


def greet():
    barrier = pltpu.get_barrier_semaphore()
    for relation in FAR_FIRST:
        pl.semaphore_signal(barrier, inc=1, device_id=partner(relation), device_id_type=MESH_ID)
    return barrier


def send_all(pairs, send_sem, recv_sem):
    copies = []
    for relation in FAR_FIRST:
        for which, (src, dst) in enumerate(pairs(relation)):
            copy = pltpu.make_async_remote_copy(src_ref=src, dst_ref=dst, send_sem=send_sem.at[which, relation], recv_sem=recv_sem.at[which, relation], device_id=partner(relation), device_id_type=MESH_ID)
            copy.start()
            copies.append(copy)
    return copies


def axis_column(values, rows):
    idx = lax.broadcasted_iota(jnp.int32, (rows, 1), 0)
    out = jnp.full((rows, 1), values[-1], jnp.float32)
    for k in range(len(values) - 1):
        out = jnp.where(idx == k, values[k], out)
    return out


def brick_coords():
    return [lax.axis_index(name).astype(jnp.float32) for name in ("x", "y", "z")]


def prefix_counts(member):
    member = member.astype(jnp.float32)
    starts = range(0, member.shape[1], LANES)
    stacked = as_bf16(jnp.concatenate([member[:, k:k + LANES] for k in starts], axis=0) > 0.5)
    col = iota((LANES, 2 * LANES), 1)
    ladder = as_bf16((iota((LANES, 2 * LANES), 0) < col) | (col >= LANES))
    counts = jnp.dot(stacked, ladder, preferred_element_type=jnp.float32)
    before = jnp.zeros((8, LANES), jnp.float32)
    ranks = []
    for k in range(0, counts.shape[0], 8):
        ranks.append(counts[k:k + 8, 0:LANES] + before)
        before = before + counts[k:k + 8, LANES:]
    return jnp.concatenate(ranks, axis=1), before


def exchange_kernel(pos_hbm, vel_hbm, frc_hbm, id_hbm, ok_hbm, side_hbm, own_ref, all_ref, mig_ref, pos_ref, vel_ref, frc_ref, id_ref, ok_ref, side_ref, pad_ref, load_sem, send_sem, recv_sem):
    loads = []
    for k, (src, dst) in enumerate(((pos_hbm, pos_ref), (vel_hbm, vel_ref), (frc_hbm, frc_ref), (id_hbm, id_ref), (ok_hbm, ok_ref), (side_hbm, side_ref))):
        load = pltpu.make_async_copy(src, dst, load_sem.at[k])
        load.start()
        loads.append(load)
    barrier = greet()
    pad_ref[...] = jnp.zeros_like(pad_ref)
    for load in loads:
        load.wait()
    side = side_ref[...]
    box = side * 2.0
    half_v = vel_ref[...] + (0.5 * DT) * frc_ref[...]
    pad_ref[0:3, 0:CAP] = pos_ref[...] + DT * half_v
    pad_ref[3:6, 0:CAP] = half_v
    pad_ref[6:7, 0:CAP] = (id_ref[...].reshape(1, CAP) // ID_SPLIT).astype(jnp.float32) + 1.0
    pad_ref[7:8, 0:CAP] = (id_ref[...].reshape(1, CAP) % ID_SPLIT).astype(jnp.float32)
    pad_ref[8:9, 0:CAP] = ok_ref[...].reshape(1, CAP).astype(jnp.float32)
    unwrapped = pad_ref[0:3, :]
    owned = pad_ref[8:9, :] > 0.5
    moved = jnp.where(unwrapped < 0.0, unwrapped + box, jnp.where(unwrapped >= box, unwrapped - box, unwrapped))
    for axis in range(3):
        all_ref[0, :, PAD * axis:PAD * (axis + 1)] = jnp.where(owned, moved[axis:axis + 1, :], FAR_AWAY)

    low = axis_column([coord * side for coord in brick_coords()], 3)
    outside = (unwrapped < low) | (unwrapped >= low + side)
    bits = jnp.where(outside, axis_column([1.0, 2.0, 4.0], 3), 0.0)
    code = jnp.sum(bits, axis=0, keepdims=True)
    code = jnp.where(owned, code, -1.0)
    member = code == iota((8, PAD), 0)
    rank, _ = prefix_counts(member)
    offset = axis_column([0.0] + [float(SEG[m][0]) for m in OTHERS], 8)
    slot = jnp.sum(jnp.where(member, rank + offset, 0.0), axis=0, keepdims=True)
    rows = jnp.concatenate([moved, pad_ref[3:8, :]], axis=0)
    mig_ref[0] = select_rows(rows, as_bf16(iota((MIG, PAD), 0) == jnp.where(code > 0.5, slot, -1.0)))
    own_ref[8:9, :] = jnp.broadcast_to(side, (1, PAD))

    def pairs(relation):
        block = pl.ds(SEG[relation][0] // LANES * LANES, LANES)
        return (mig_ref.at[0, :, block], mig_ref.at[relation, :, block]), (all_ref.at[0], all_ref.at[relation])

    pl.semaphore_wait(barrier, len(OTHERS))
    copies = send_all(pairs, send_sem, recv_sem)
    pieces = pieces_of(rows)
    slots = iota((LANES, PAD), 0)
    slot = jnp.where(code == 0.0, slot, -1.0)

    def pack(k, carry):
        first = k * LANES
        out = lax.dot_general(pieces, as_bf16(slots == slot - first.astype(jnp.float32)), NT, preferred_element_type=jnp.float32)
        own_ref[0:8, pl.ds(pl.multiple_of(first, LANES), LANES)] = sum_groups(out, 8)
        return carry

    lax.fori_loop(0, PAD // LANES, pack, 0)
    for copy in copies:
        copy.wait()


def pair_terms(own, other, span):
    delta = []
    for mine, theirs in zip(own, other):
        diff = mine - theirs
        if span is not None:
            diff = diff - jnp.where(diff > 0.5 * span, span, jnp.where(diff < -0.5 * span, -span, 0.0))
        delta.append(diff)
    dist_sq = delta[0] * delta[0] + delta[1] * delta[1] + delta[2] * delta[2]
    in_range = (dist_sq < RC * RC) & (dist_sq > 0.01)
    inv_r = jnp.where(in_range, lax.rsqrt(dist_sq), 0.0)
    inv_r2 = inv_r * inv_r
    inv_r6 = inv_r2 * inv_r2 * inv_r2
    inv_r12 = inv_r6 * inv_r6
    well = inv_r12 - inv_r6
    scale = (well + inv_r12) * inv_r2 + (UPC / 24.0) * inv_r
    return [scale * d for d in delta], [well, dist_sq * inv_r, jnp.where(in_range, 1.0, 0.0)]


def force_kernel(own_ref, all_ref, mig_ref, en_ref, acc_ref, rows_ref, near_ref, mine_ref, plane_ref, list_ref, count_ref):
    side = own_ref[8:9, 0:1]
    box = side * 2.0
    lane = iota((1, MIG), 1, jnp.int32)
    arrivals = jnp.zeros((8, MIG), jnp.float32)
    for relation, (start, size) in SEG.items():
        arrivals = jnp.where((lane >= start) & (lane < start + size), mig_ref[relation], arrivals)
    arrived = arrivals[6:7, :] > 0.5
    staying = (own_ref[6:7, :] > 0.5).astype(jnp.float32)
    n_staying = jnp.sum(staying, axis=1, keepdims=True)
    total = jnp.sum((n_staying + jnp.sum(arrived.astype(jnp.float32), axis=1, keepdims=True)).astype(jnp.int32))
    tail = all_ref[0, :, NARROW:PAD]
    for relation in OTHERS:
        tail = jnp.minimum(tail, all_ref[relation, :, NARROW:PAD])
    narrow = (jnp.min(tail) > 0.5 * FAR_AWAY) & (total <= NARROW)
    slot, _ = prefix_counts(jnp.broadcast_to(arrived, (8, MIG)))
    slot = jnp.where(arrived, slot[0:1, :] + n_staying, -1.0)
    pieces = pieces_of(arrivals)
    centre = [(coord + 0.5) * side for coord in brick_coords()]

    def prepare(width):
        for relation in range(8):
            for axis in range(3):
                plane_ref[axis, relation:relation + 1, 0:width] = all_ref[relation, :, PAD * axis:PAD * axis + width]
        planes = []
        beyond = jnp.zeros((8, width), jnp.float32)
        for axis in range(3):
            theirs = plane_ref[axis, :, 0:width] - centre[axis]
            theirs = jnp.where(theirs > side, theirs - box, jnp.where(theirs < -side, theirs + box, theirs))
            excess = jnp.maximum(jnp.abs(theirs) - 0.5 * side, 0.0)
            beyond = beyond + excess * excess
            planes.append(theirs)
        keep = (beyond < REACH * REACH) & (beyond > 0.0)
        front, held = prefix_counts(keep)
        lanes = iota((8, width), 1, jnp.int32)
        hops = jnp.where(keep, lanes - front.astype(jnp.int32), 0)

        slots = iota((LANES, MIG), 0)
        starts = range(0, width, LANES)
        for bit in range(0, 10, 2):
            digit = (hops >> bit) & 3
            step = 1 << bit
            next_hops = jnp.where(digit != 0, 0, hops)
            moved = planes
            for times in range(1, 4):
                back = width - times * step
                if back > 0:
                    coming = pltpu.roll(hops, back, 1)
                    take = ((coming >> bit) & 3) == times
                    next_hops = jnp.where(take, coming, next_hops)
                    moved = [jnp.where(take, pltpu.roll(old, back, 1), new) for old, new in zip(planes, moved)]
            hops, planes = next_hops, moved
            for start in starts[bit // 2::5]:
                out = lax.dot_general(pieces, as_bf16(slots == slot - float(start)), NT, preferred_element_type=jnp.float32)
                rows_ref[:, start:start + LANES] = own_ref[0:8, start:start + LANES] + sum_groups(out, 8)
        if width < PAD:
            rows_ref[:, width:PAD] = jnp.zeros((8, PAD - width), jnp.float32)

        rows = rows_ref[:, 0:width]
        filled = rows[6:7, :] > 0.5
        local = rows[0:3, :] - axis_column(centre, 3)
        near_ref[0:3, 0:width] = jnp.where(filled, local, FAR_AWAY)
        local = jnp.concatenate([jnp.where(filled, local, -FAR_AWAY), jnp.zeros((5, width), jnp.float32)], axis=0)
        spread = as_bf16(iota((24, 3 * LANES), 0, jnp.int32) % 8 == iota((24, 3 * LANES), 1, jnp.int32) // LANES)
        columns = lax.dot_general(pieces_of(local), spread, (((0,), (0,)), ((), ())), preferred_element_type=jnp.float32)
        for axis in range(3):
            mine_ref[axis, 0:width, :] = columns[:, LANES * axis:LANES * (axis + 1)]

        for relation in range(8):
            for axis in range(3):
                list_ref[relation, axis:axis + 1, 0:width] = planes[axis][relation:relation + 1, :]
        held = held.astype(jnp.int32)
        lane128 = iota((8, LANES), 1, jnp.int32)
        start = total
        for relation in range(8):
            into = start % LANES
            first = pl.multiple_of(start - into, LANES)
            turned = pltpu.roll(list_ref[relation, :, 0:width + LANES], into, 1)
            near_ref[:, pl.ds(first, LANES)] = jnp.where(lane128 < into, near_ref[:, pl.ds(first, LANES)], turned[:, 0:LANES])
            near_ref[:, pl.ds(pl.multiple_of(first + LANES, LANES), width)] = turned[:, LANES:]
            start = start + held[relation, 0]
        into = start % LANES
        first = pl.multiple_of(start - into, LANES)
        near_ref[:, pl.ds(first, LANES)] = jnp.where(lane128 < into, near_ref[:, pl.ds(first, LANES)], FAR_AWAY)
        count_ref[0] = (start + LANES - 1) // LANES

    @pl.when(narrow)
    def _():
        prepare(NARROW)

    @pl.when(jnp.logical_not(narrow))
    def _():
        prepare(PAD)

    n_other = count_ref[0]
    n_own = (total + IC - 1) // IC

    def sweep(span):
        def own_step(i, totals):
            first = pl.multiple_of(i * IC, IC)
            own = [mine_ref[axis, pl.ds(first, IC), :] for axis in range(3)]

            def other_block(first, sums):
                forces, totals = sums
                other = [near_ref[axis:axis + 1, pl.ds(first, LANES)] for axis in range(3)]
                force, parts = pair_terms(own, other, span)
                forces = tuple(f + t for f, t in zip(forces, force))
                totals = tuple(t + sum_groups(p, 8) for t, p in zip(totals, parts))
                return forces, totals

            def other_step(j, sums):
                first = pl.multiple_of(j * 2 * LANES, 2 * LANES)
                return other_block(first + LANES, other_block(first, sums))

            def last_step(j, sums):
                return other_block(pl.multiple_of((n_other - 1) * LANES, LANES), sums)

            zero = jnp.zeros((IC, LANES), jnp.float32)
            sums = lax.fori_loop(0, n_other // 2, other_step, ((zero,) * 3, totals))
            forces, totals = lax.fori_loop(0, n_other % 2, last_step, sums)
            for axis in range(3):
                acc_ref[axis, pl.ds(first, IC), :] = forces[axis]
            return totals

        zero = jnp.zeros((8, LANES), jnp.float32)
        well, distance, pairs = lax.fori_loop(0, n_own, own_step, (zero,) * 3)
        energy = 2.0 * well - (0.5 * UPC) * distance - (0.5 * (UCUT - RC * UPC)) * pairs
        en_ref[...] = jnp.sum(energy, axis=0, keepdims=True)

    one_image = side[0, 0] >= 2.0 * RC

    @pl.when(one_image)
    def _():
        sweep(None)

    @pl.when(jnp.logical_not(one_image))
    def _():
        sweep(box)


def energy_kernel(en_ref, acc_ref, rows_ref, sum_ref, pos_ref, vel_ref, frc_ref, id_ref, ok_ref, force_ref, parts_ref, send_sem, recv_sem):
    barrier = greet()
    pl.semaphore_wait(barrier, len(OTHERS))
    copies = send_all(lambda relation: ((en_ref, parts_ref.at[relation]),), send_sem, recv_sem)
    def turn(k, carry):
        block = pl.ds(pl.multiple_of(k * LANES, LANES), LANES)
        for axis in range(3):
            force_ref[axis:axis + 1, block] = jnp.sum(jnp.transpose(acc_ref[axis, block, :]), axis=0, keepdims=True)
        return carry

    lax.fori_loop(0, PAD // LANES, turn, 0)
    rows = rows_ref[...]
    filled = rows[6:7, :] > 0.5
    key = jnp.where(filled, id_of(rows), 2147483647)
    key_col = jnp.transpose(jnp.broadcast_to(key, (8, PAD)))[:, 0:1]
    slot = jnp.dot(jnp.ones((8, PAD), jnp.bfloat16), as_bf16(key_col < key), preferred_element_type=jnp.float32)[0:1, :]
    onehot = as_bf16(iota((PAD, PAD), 0) == jnp.where(filled, slot, -1.0))
    force_ref[0:3, :] = jnp.where(filled, (24.0 * force_ref[0:3, :]), 0.0)
    force_ref[3:8, :] = jnp.zeros((5, PAD), jnp.float32)
    out = select_rows(jnp.concatenate([rows, force_ref[...]], axis=0), onehot)[:, 0:CAP]
    force = out[8:11]
    filled = out[6:7] > 0.5
    frc_ref[...] = force
    pos_ref[...] = out[0:3]
    vel_ref[...] = out[3:6] + (0.5 * DT) * force
    id_ref[...] = jnp.where(filled, id_of(out), 0).reshape(CAP)
    ok_ref[...] = filled.astype(jnp.int32).reshape(CAP)
    for copy in copies:
        copy.wait()
    parts_ref[0] = en_ref[...]
    level = [parts_ref[relation] for relation in range(8)]
    while len(level) > 1:
        level = [one + two for one, two in zip(level[0::2], level[1::2])]
    sum_ref[...] = level[0]


def store_kernel(sum_ref, *refs):
    sources, targets, total_ref, store_sem = refs[0:5], refs[5:11], refs[11], refs[12]
    stores = [pltpu.make_async_copy(sources[k], targets[k], store_sem.at[k]) for k in range(5)]
    for store in stores:
        store.start()
    total_ref[...] = jnp.sum(sum_ref[...], axis=1, keepdims=True)
    stores.append(pltpu.make_async_copy(total_ref, targets[5], store_sem.at[5]))
    stores[5].start()
    for store in stores:
        store.wait()


def solution(mesh):
    vmem = pl.BlockSpec(memory_space=pltpu.VMEM)
    hbm = pl.BlockSpec(memory_space=pltpu.HBM)
    f32, i32 = jnp.float32, jnp.int32

    def shape(dims, dtype=f32):
        return jax.ShapeDtypeStruct(dims, dtype)

    exchange = pl.pallas_call(
        exchange_kernel,
        out_shape=(shape((9, PAD)), shape((8, 1, 3 * PAD)), shape((8, 8, MIG))),
        in_specs=[hbm] * 5 + [pl.BlockSpec(memory_space=pl.ANY)],
        out_specs=(vmem, vmem, vmem),
        scratch_shapes=[pltpu.VMEM((3, CAP), f32)] * 3 + [pltpu.VMEM((CAP,), i32)] * 2 + [pltpu.VMEM((1, 1), f32), pltpu.VMEM((9, PAD), f32), pltpu.SemaphoreType.DMA((6,)), pltpu.SemaphoreType.DMA((2, 8)), pltpu.SemaphoreType.DMA((2, 8))],
        compiler_params=pltpu.CompilerParams(collective_id=0, has_side_effects=True, vmem_limit_bytes=16 << 20),
        name="exchange",
    )
    forces = pl.pallas_call(
        force_kernel,
        out_shape=(shape((1, 128)), shape((3, PAD, 128)), shape((8, PAD))),
        in_specs=[vmem] * 3,
        out_specs=(vmem,) * 3,
        scratch_shapes=[pltpu.VMEM((8, 9 * PAD + 256), f32), pltpu.VMEM((3, PAD, 128), f32), pltpu.VMEM((3, 8, PAD), f32), pltpu.VMEM((8, 8, PAD + 128), f32), pltpu.SMEM((1,), i32)],
        compiler_params=pltpu.CompilerParams(vmem_limit_bytes=16 << 20),
        name="forces",
    )
    results = (shape((3, CAP)), shape((3, CAP)), shape((3, CAP)), shape((CAP,), i32), shape((CAP,), i32))
    total_energy = pl.pallas_call(
        energy_kernel,
        out_shape=(shape((1, 128)),) + results,
        in_specs=[vmem] * 3,
        out_specs=(vmem,) * 6,
        scratch_shapes=[pltpu.VMEM((8, PAD), f32), pltpu.VMEM((8, 1, LANES), f32), pltpu.SemaphoreType.DMA((1, 8)), pltpu.SemaphoreType.DMA((1, 8))],
        compiler_params=pltpu.CompilerParams(collective_id=1, has_side_effects=True, vmem_limit_bytes=16 << 20),
        name="energy",
    )
    store = pl.pallas_call(
        store_kernel,
        out_shape=results + (shape((1, 1)),),
        in_specs=[vmem] * 6,
        out_specs=(hbm,) * 6,
        scratch_shapes=[pltpu.VMEM((1, 1), f32), pltpu.SemaphoreType.DMA((6,))],
        compiler_params=pltpu.CompilerParams(vmem_limit_bytes=16 << 20),
        name="store",
    )

    def local_step(atom_pos, atom_vel, atom_frc, atom_id, atom_ok, brick_side):
        arrays = (atom_pos.T, atom_vel.T, atom_frc.T, atom_id, atom_ok, brick_side.reshape(1, 1))
        own, everyone, movers = exchange(*[pltpu.with_memory_space_constraint(array, pltpu.HBM) for array in arrays[:5]], arrays[5])
        partial, sums, rows = forces(own, everyone, movers)
        pos, vel, frc, new_id, new_ok, energy = store(*total_energy(partial, sums, rows))
        return pos.T, vel.T, frc.T, new_id, new_ok, energy.reshape(())

    row_spec = P(MESH_AXES, None)
    id_spec = P(MESH_AXES)
    return jax.shard_map(local_step, mesh=mesh, in_specs=(row_spec, row_spec, row_spec, id_spec, id_spec, P()), out_specs=(row_spec, row_spec, row_spec, id_spec, id_spec, P()), check_vma=False)
```

```python
import functools

import jax
import jax.numpy as jnp
from jax import lax
from jax.experimental import pallas as pl
from jax.experimental.pallas import tpu as pltpu
from jax.sharding import PartitionSpec as P

DT = 0.005
RC = 2.5
FAR_AWAY = 1.0e6
UCUT = 4.0 * (RC ** -12 - RC ** -6)
UPC = -48.0 * RC ** -13 + 24.0 * RC ** -7
MESH_AXES = ("z", "y", "x")
CAP = 729
PAD = 768
MIG = 256
SEG = {1: (0, 16), 2: (16, 16), 4: (32, 16), 3: (48, 32), 5: (80, 32), 6: (128, 32), 7: (160, 64)}
IC = 32
NARROW = 512
LANES = 128
ID_SPLIT = 65536
NT = (((1,), (1,)), ((), ()))
OTHERS = tuple(range(1, 8))
FAR_FIRST = (6, 7, 4, 2, 5, 3, 1)
REACH = RC + 0.01
MESH_ID = pl.DeviceIdType.MESH


def pieces_of(rows):
    first = rows.astype(jnp.bfloat16).astype(jnp.float32)
    rest = rows - first
    second = rest.astype(jnp.bfloat16).astype(jnp.float32)
    third = rest - second
    return jnp.concatenate([first, second, third], axis=0).astype(jnp.bfloat16)


def select_rows(rows, onehot):
    out = lax.dot_general(pieces_of(rows), onehot, NT, preferred_element_type=jnp.float32)
    return sum_groups(out, rows.shape[0])


def sum_groups(rows, size):
    total = rows[0:size]
    for k in range(size, rows.shape[0], size):
        total = total + rows[k:k + size]
    return total


def as_bf16(mask):
    return mask.astype(jnp.float32).astype(jnp.bfloat16)


def iota(dims, axis, dtype=jnp.float32):
    return lax.broadcasted_iota(jnp.int32, dims, axis).astype(dtype)


def id_of(rows):
    return (rows[6:7].astype(jnp.int32) - 1) * ID_SPLIT + rows[7:8].astype(jnp.int32)


def partner(relation):
    return tuple((lax.axis_index(name) + relation // bit) % 2 for name, bit in zip(MESH_AXES, (4, 2, 1)))


def greet():
    barrier = pltpu.get_barrier_semaphore()
    for relation in FAR_FIRST:
        pl.semaphore_signal(barrier, inc=1, device_id=partner(relation), device_id_type=MESH_ID)
    return barrier


def send_all(pairs, send_sem, recv_sem):
    copies = []
    for relation in FAR_FIRST:
        for which, (src, dst) in enumerate(pairs(relation)):
            copy = pltpu.make_async_remote_copy(src_ref=src, dst_ref=dst, send_sem=send_sem.at[which, relation], recv_sem=recv_sem.at[which, relation], device_id=partner(relation), device_id_type=MESH_ID)
            copy.start()
            copies.append(copy)
    return copies


def axis_column(values, rows):
    idx = lax.broadcasted_iota(jnp.int32, (rows, 1), 0)
    out = jnp.full((rows, 1), values[-1], jnp.float32)
    for k in range(len(values) - 1):
        out = jnp.where(idx == k, values[k], out)
    return out


def brick_coords():
    return [lax.axis_index(name).astype(jnp.float32) for name in ("x", "y", "z")]


def prefix_counts(member):
    member = member.astype(jnp.float32)
    starts = range(0, member.shape[1], LANES)
    stacked = as_bf16(jnp.concatenate([member[:, k:k + LANES] for k in starts], axis=0) > 0.5)
    col = iota((LANES, 2 * LANES), 1)
    ladder = as_bf16((iota((LANES, 2 * LANES), 0) < col) | (col >= LANES))
    counts = jnp.dot(stacked, ladder, preferred_element_type=jnp.float32)
    before = jnp.zeros((8, LANES), jnp.float32)
    ranks = []
    for k in range(0, counts.shape[0], 8):
        ranks.append(counts[k:k + 8, 0:LANES] + before)
        before = before + counts[k:k + 8, LANES:]
    return jnp.concatenate(ranks, axis=1), before


def exchange_kernel(pos_hbm, vel_hbm, frc_hbm, id_hbm, ok_hbm, side_hbm, own_ref, all_ref, mig_ref, pos_ref, vel_ref, frc_ref, id_ref, ok_ref, side_ref, pad_ref, load_sem, send_sem, recv_sem):
    loads = []
    for k, (src, dst) in enumerate(((pos_hbm, pos_ref), (vel_hbm, vel_ref), (frc_hbm, frc_ref), (id_hbm, id_ref), (ok_hbm, ok_ref), (side_hbm, side_ref))):
        load = pltpu.make_async_copy(src, dst, load_sem.at[k])
        load.start()
        loads.append(load)
    barrier = greet()
    pad_ref[...] = jnp.zeros_like(pad_ref)
    for load in loads:
        load.wait()
    side = side_ref[...]
    box = side * 2.0
    half_v = vel_ref[...] + (0.5 * DT) * frc_ref[...]
    pad_ref[0:3, 0:CAP] = pos_ref[...] + DT * half_v
    pad_ref[3:6, 0:CAP] = half_v
    pad_ref[6:7, 0:CAP] = (id_ref[...].reshape(1, CAP) // ID_SPLIT).astype(jnp.float32) + 1.0
    pad_ref[7:8, 0:CAP] = (id_ref[...].reshape(1, CAP) % ID_SPLIT).astype(jnp.float32)
    pad_ref[8:9, 0:CAP] = ok_ref[...].reshape(1, CAP).astype(jnp.float32)
    unwrapped = pad_ref[0:3, :]
    owned = pad_ref[8:9, :] > 0.5
    moved = jnp.where(unwrapped < 0.0, unwrapped + box, jnp.where(unwrapped >= box, unwrapped - box, unwrapped))
    for axis in range(3):
        all_ref[0, :, PAD * axis:PAD * (axis + 1)] = jnp.where(owned, moved[axis:axis + 1, :], FAR_AWAY)

    low = axis_column([coord * side for coord in brick_coords()], 3)
    outside = (unwrapped < low) | (unwrapped >= low + side)
    bits = jnp.where(outside, axis_column([1.0, 2.0, 4.0], 3), 0.0)
    code = jnp.sum(bits, axis=0, keepdims=True)
    code = jnp.where(owned, code, -1.0)
    lower = moved[2:3, :] < low[2:3, :] + 0.5 * side
    member = jnp.where((code == 0.0) & jnp.logical_not(lower), -1.0, code) == iota((8, PAD), 0)
    rank, _ = prefix_counts(member)
    offset = axis_column([0.0] + [float(SEG[m][0]) for m in OTHERS], 8)
    slot = jnp.sum(jnp.where(member, rank + offset, 0.0), axis=0, keepdims=True)
    rows = jnp.concatenate([moved, pad_ref[3:8, :]], axis=0)
    mig_ref[0] = select_rows(rows, as_bf16(iota((MIG, PAD), 0) == jnp.where(code > 0.5, slot, -1.0)))
    own_ref[16:17, :] = jnp.broadcast_to(side, (1, PAD))

    def pairs(relation):
        block = pl.ds(SEG[relation][0] // LANES * LANES, LANES)
        return (mig_ref.at[0, :, block], mig_ref.at[relation, :, block]), (all_ref.at[0], all_ref.at[relation])

    pl.semaphore_wait(barrier, len(OTHERS))
    copies = send_all(pairs, send_sem, recv_sem)
    pieces = pieces_of(rows)
    slots = iota((LANES, PAD), 0)
    upper_slot = iota((1, PAD), 1) - jnp.sum(rank, axis=0, keepdims=True)
    halves = (jnp.where((code == 0.0) & lower, slot, -1.0), jnp.where((code == 0.0) & jnp.logical_not(lower), upper_slot, -1.0))

    def pack(k, carry):
        first = k * LANES
        for half, target in enumerate(halves):
            out = lax.dot_general(pieces, as_bf16(slots == target - first.astype(jnp.float32)), NT, preferred_element_type=jnp.float32)
            own_ref[8 * half:8 * half + 8, pl.ds(pl.multiple_of(first, LANES), LANES)] = sum_groups(out, 8)
        return carry

    lax.fori_loop(0, PAD // LANES, pack, 0)
    for copy in copies:
        copy.wait()


def pair_terms(own, other, span):
    delta = []
    for mine, theirs in zip(own, other):
        diff = mine - theirs
        if span is not None:
            diff = diff - jnp.where(diff > 0.5 * span, span, jnp.where(diff < -0.5 * span, -span, 0.0))
        delta.append(diff)
    dist_sq = delta[0] * delta[0] + delta[1] * delta[1] + delta[2] * delta[2]
    in_range = (dist_sq < RC * RC) & (dist_sq > 0.01)
    inv_r = jnp.where(in_range, lax.rsqrt(dist_sq), 0.0)
    inv_r2 = inv_r * inv_r
    inv_r6 = inv_r2 * inv_r2 * inv_r2
    inv_r12 = inv_r6 * inv_r6
    well = inv_r12 - inv_r6
    scale = (well + inv_r12) * inv_r2 + (UPC / 24.0) * inv_r
    return [scale * d for d in delta], [well, dist_sq * inv_r, jnp.where(in_range, 1.0, 0.0)]


def force_kernel(own_ref, all_ref, mig_ref, en_ref, acc_ref, rows_ref, near_ref, mine_ref, plane_ref, list_ref, dense_ref, count_ref):
    side = own_ref[16:17, 0:1]
    box = side * 2.0
    centre = [(coord + 0.5) * side for coord in brick_coords()]
    lane = iota((1, MIG), 1, jnp.int32)
    arrivals = jnp.zeros((8, MIG), jnp.float32)
    for relation, (start, size) in SEG.items():
        arrivals = jnp.where((lane >= start) & (lane < start + size), mig_ref[relation], arrivals)
    half_of = jnp.where(arrivals[2:3, :] < centre[2], 0.0, 1.0)
    arrived = jnp.where(arrivals[6:7, :] > 0.5, half_of, -1.0) == iota((8, MIG), 0)
    ranks, _ = prefix_counts(arrived)
    targets, sizes = [], []
    for half in range(2):
        staying = jnp.sum((own_ref[8 * half + 6:8 * half + 7, :] > 0.5).astype(jnp.float32), axis=1, keepdims=True)
        here = arrived[half:half + 1, :]
        targets.append(jnp.where(here, ranks[half:half + 1, :] + staying, -1.0))
        sizes.append(jnp.sum((staying + jnp.sum(here.astype(jnp.float32), axis=1, keepdims=True)).astype(jnp.int32)))
    split = (sizes[0] + IC - 1) // IC * IC
    total = split + sizes[1]
    tail = all_ref[0, :, NARROW:PAD]
    for relation in OTHERS:
        tail = jnp.minimum(tail, all_ref[relation, :, NARROW:PAD])
    narrow = (jnp.min(tail) > 0.5 * FAR_AWAY) & (total <= NARROW + LANES) & (jnp.maximum(sizes[0], sizes[1]) <= NARROW - LANES)
    pieces = pieces_of(arrivals)

    def lay(target, rows, start):
        into = start % LANES
        first = pl.multiple_of(start - into, LANES)
        turned = pltpu.roll(rows, into, 1)
        behind = iota((8, LANES), 1, jnp.int32) >= into
        pltpu.store(target.at[:, pl.ds(first, LANES)], turned[:, 0:LANES], mask=behind)
        target[:, pl.ds(pl.multiple_of(first + LANES, LANES), rows.shape[1] - LANES)] = turned[:, LANES:]

    def prepare(width, half_width, slots_width):
        for relation in range(8):
            for axis in range(3):
                plane_ref[axis, relation:relation + 1, 0:width] = all_ref[relation, :, PAD * axis:PAD * axis + width]
        places = []
        across = jnp.zeros((8, width), jnp.float32)
        for axis in range(3):
            theirs = plane_ref[axis, :, 0:width] - centre[axis]
            theirs = jnp.where(theirs > side, theirs - box, jnp.where(theirs < -side, theirs + box, theirs))
            places.append(theirs)
            if axis < 2:
                excess = jnp.maximum(jnp.abs(theirs) - 0.5 * side, 0.0)
                across = across + excess * excess
        height = places[2]
        outside = (across > 0.0) | (jnp.abs(height) > 0.5 * side)
        lanes = iota((8, width), 1, jnp.int32)
        lists = []
        for sign in (1.0, -1.0):
            tilted = sign * height
            excess = jnp.minimum(jnp.maximum(jnp.abs(tilted + 0.25 * side) - 0.25 * side, 0.0), 1.5 * side - tilted)
            keep = outside & (across + excess * excess < REACH * REACH)
            front, held = prefix_counts(keep)
            lists.append((jnp.where(keep, lanes - front.astype(jnp.int32), 0), places, held.astype(jnp.int32)))

        slots = iota((LANES, MIG), 0)
        starts = range(0, half_width, LANES)
        for bit in range(0, 10, 2):
            step = 1 << bit
            for half in range(2):
                hops, planes, held = lists[half]
                next_hops = jnp.where(((hops >> bit) & 3) != 0, 0, hops)
                moved = planes
                for times in range(1, 4):
                    back = width - times * step
                    if back > 0:
                        coming = pltpu.roll(hops, back, 1)
                        take = ((coming >> bit) & 3) == times
                        next_hops = jnp.where(take, coming, next_hops)
                        moved = [jnp.where(take, pltpu.roll(old, back, 1), new) for old, new in zip(planes, moved)]
                lists[half] = (next_hops, moved, held)
                for start in starts[bit // 2::5]:
                    out = lax.dot_general(pieces, as_bf16(slots == targets[half] - float(start)), NT, preferred_element_type=jnp.float32)
                    dense_ref[half, :, start:start + LANES] = own_ref[8 * half:8 * half + 8, start:start + LANES] + sum_groups(out, 8)
        dense_ref[0, :, half_width:PAD + LANES] = jnp.zeros((8, PAD + LANES - half_width), jnp.float32)
        dense_ref[1, :, half_width:half_width + LANES] = jnp.zeros((8, LANES), jnp.float32)
        lay(dense_ref.at[0], dense_ref[1, :, 0:half_width + LANES], split)
        rows_ref[...] = dense_ref[0, :, 0:PAD]

        rows = rows_ref[:, 0:slots_width]
        filled = rows[6:7, :] > 0.5
        local = rows[0:3, :] - axis_column(centre, 3)
        for half in range(2):
            near_ref[half, 0:3, 0:slots_width] = jnp.where(filled, local, FAR_AWAY)
        local = jnp.concatenate([jnp.where(filled, local, -FAR_AWAY), jnp.zeros((5, slots_width), jnp.float32)], axis=0)
        spread = as_bf16(iota((24, 3 * LANES), 0, jnp.int32) % 8 == iota((24, 3 * LANES), 1, jnp.int32) // LANES)
        columns = lax.dot_general(pieces_of(local), spread, (((0,), (0,)), ((), ())), preferred_element_type=jnp.float32)
        for axis in range(3):
            mine_ref[axis, 0:slots_width, :] = columns[:, LANES * axis:LANES * (axis + 1)]

        for half in range(2):
            _, planes, held = lists[half]
            for relation in range(8):
                for axis in range(3):
                    list_ref[half, relation, axis:axis + 1, 0:width] = planes[axis][relation:relation + 1, :]
            start = total
            for relation in range(8):
                lay(near_ref.at[half], list_ref[half, relation, :, 0:width + LANES], start)
                start = start + held[relation, 0]
            lay(near_ref.at[half], jnp.full((8, 2 * LANES), FAR_AWAY, jnp.float32), start)
            count_ref[half] = (start + LANES - 1) // LANES

    @pl.when(narrow)
    def _():
        prepare(NARROW, NARROW - LANES, NARROW + LANES)

    @pl.when(jnp.logical_not(narrow))
    def _():
        prepare(PAD, PAD, PAD)

    n_own = (total + IC - 1) // IC

    def sweep(span):
        def own_step(i, totals):
            first = pl.multiple_of(i * IC, IC)
            half = (first >= split).astype(jnp.int32)
            n_other = count_ref[half]
            own = [mine_ref[axis, pl.ds(first, IC), :] for axis in range(3)]

            def other_block(first, sums):
                forces, totals = sums
                other = [near_ref[half, axis:axis + 1, pl.ds(first, LANES)] for axis in range(3)]
                force, parts = pair_terms(own, other, span)
                forces = tuple(f + t for f, t in zip(forces, force))
                totals = tuple(t + sum_groups(p, 8) for t, p in zip(totals, parts))
                return forces, totals

            def other_step(j, sums):
                first = pl.multiple_of(j * 2 * LANES, 2 * LANES)
                return other_block(first + LANES, other_block(first, sums))

            def last_step(j, sums):
                return other_block(pl.multiple_of((n_other - 1) * LANES, LANES), sums)

            zero = jnp.zeros((IC, LANES), jnp.float32)
            sums = lax.fori_loop(0, n_other // 2, other_step, ((zero,) * 3, totals))
            forces, totals = lax.fori_loop(0, n_other % 2, last_step, sums)
            for axis in range(3):
                acc_ref[axis, pl.ds(first, IC), :] = forces[axis]
            return totals

        zero = jnp.zeros((8, LANES), jnp.float32)
        well, distance, pairs = lax.fori_loop(0, n_own, own_step, (zero,) * 3)
        energy = 2.0 * well - (0.5 * UPC) * distance - (0.5 * (UCUT - RC * UPC)) * pairs
        en_ref[...] = jnp.sum(energy, axis=0, keepdims=True)

    one_image = side[0, 0] >= 2.0 * RC

    @pl.when(one_image)
    def _():
        sweep(None)

    @pl.when(jnp.logical_not(one_image))
    def _():
        sweep(box)


def energy_kernel(en_ref, acc_ref, rows_ref, sum_ref, pos_ref, vel_ref, frc_ref, id_ref, ok_ref, force_ref, parts_ref, send_sem, recv_sem):
    barrier = greet()
    pl.semaphore_wait(barrier, len(OTHERS))
    copies = send_all(lambda relation: ((en_ref, parts_ref.at[relation]),), send_sem, recv_sem)
    def turn(k, carry):
        block = pl.ds(pl.multiple_of(k * LANES, LANES), LANES)
        for axis in range(3):
            force_ref[axis:axis + 1, block] = jnp.sum(jnp.transpose(acc_ref[axis, block, :]), axis=0, keepdims=True)
        return carry

    lax.fori_loop(0, PAD // LANES, turn, 0)
    rows = rows_ref[...]
    filled = rows[6:7, :] > 0.5
    key = jnp.where(filled, id_of(rows), 2147483647)
    key_col = jnp.transpose(jnp.broadcast_to(key, (8, PAD)))[:, 0:1]
    slot = jnp.dot(jnp.ones((8, PAD), jnp.bfloat16), as_bf16(key_col < key), preferred_element_type=jnp.float32)[0:1, :]
    onehot = as_bf16(iota((PAD, PAD), 0) == jnp.where(filled, slot, -1.0))
    force_ref[0:3, :] = jnp.where(filled, (24.0 * force_ref[0:3, :]), 0.0)
    force_ref[3:8, :] = jnp.zeros((5, PAD), jnp.float32)
    out = select_rows(jnp.concatenate([rows, force_ref[...]], axis=0), onehot)[:, 0:CAP]
    force = out[8:11]
    filled = out[6:7] > 0.5
    frc_ref[...] = force
    pos_ref[...] = out[0:3]
    vel_ref[...] = out[3:6] + (0.5 * DT) * force
    id_ref[...] = jnp.where(filled, id_of(out), 0).reshape(CAP)
    ok_ref[...] = filled.astype(jnp.int32).reshape(CAP)
    for copy in copies:
        copy.wait()
    parts_ref[0] = en_ref[...]
    level = [parts_ref[relation] for relation in range(8)]
    while len(level) > 1:
        level = [one + two for one, two in zip(level[0::2], level[1::2])]
    sum_ref[...] = level[0]


def store_kernel(sum_ref, *refs):
    sources, targets, total_ref, store_sem = refs[0:5], refs[5:11], refs[11], refs[12]
    stores = [pltpu.make_async_copy(sources[k], targets[k], store_sem.at[k]) for k in range(5)]
    for store in stores:
        store.start()
    total_ref[...] = jnp.sum(sum_ref[...], axis=1, keepdims=True)
    stores.append(pltpu.make_async_copy(total_ref, targets[5], store_sem.at[5]))
    stores[5].start()
    for store in stores:
        store.wait()


def solution(mesh):
    vmem = pl.BlockSpec(memory_space=pltpu.VMEM)
    hbm = pl.BlockSpec(memory_space=pltpu.HBM)
    f32, i32 = jnp.float32, jnp.int32

    def shape(dims, dtype=f32):
        return jax.ShapeDtypeStruct(dims, dtype)

    exchange = pl.pallas_call(
        exchange_kernel,
        out_shape=(shape((17, PAD)), shape((8, 1, 3 * PAD)), shape((8, 8, MIG))),
        in_specs=[hbm] * 5 + [pl.BlockSpec(memory_space=pl.ANY)],
        out_specs=(vmem, vmem, vmem),
        scratch_shapes=[pltpu.VMEM((3, CAP), f32)] * 3 + [pltpu.VMEM((CAP,), i32)] * 2 + [pltpu.VMEM((1, 1), f32), pltpu.VMEM((9, PAD), f32), pltpu.SemaphoreType.DMA((6,)), pltpu.SemaphoreType.DMA((2, 8)), pltpu.SemaphoreType.DMA((2, 8))],
        compiler_params=pltpu.CompilerParams(collective_id=0, has_side_effects=True, vmem_limit_bytes=16 << 20),
        name="exchange",
    )
    forces = pl.pallas_call(
        force_kernel,
        out_shape=(shape((1, 128)), shape((3, PAD, 128)), shape((8, PAD))),
        in_specs=[vmem] * 3,
        out_specs=(vmem,) * 3,
        scratch_shapes=[pltpu.VMEM((2, 8, 9 * PAD + 256), f32), pltpu.VMEM((3, PAD, 128), f32), pltpu.VMEM((3, 8, PAD), f32), pltpu.VMEM((2, 8, 8, PAD + 128), f32), pltpu.VMEM((2, 8, 2 * PAD + 256), f32), pltpu.SMEM((2,), i32)],
        compiler_params=pltpu.CompilerParams(vmem_limit_bytes=16 << 20),
        name="forces",
    )
    results = (shape((3, CAP)), shape((3, CAP)), shape((3, CAP)), shape((CAP,), i32), shape((CAP,), i32))
    total_energy = pl.pallas_call(
        energy_kernel,
        out_shape=(shape((1, 128)),) + results,
        in_specs=[vmem] * 3,
        out_specs=(vmem,) * 6,
        scratch_shapes=[pltpu.VMEM((8, PAD), f32), pltpu.VMEM((8, 1, LANES), f32), pltpu.SemaphoreType.DMA((1, 8)), pltpu.SemaphoreType.DMA((1, 8))],
        compiler_params=pltpu.CompilerParams(collective_id=1, has_side_effects=True, vmem_limit_bytes=16 << 20),
        name="energy",
    )
    store = pl.pallas_call(
        store_kernel,
        out_shape=results + (shape((1, 1)),),
        in_specs=[vmem] * 6,
        out_specs=(hbm,) * 6,
        scratch_shapes=[pltpu.VMEM((1, 1), f32), pltpu.SemaphoreType.DMA((6,))],
        compiler_params=pltpu.CompilerParams(vmem_limit_bytes=16 << 20),
        name="store",
    )

    def local_step(atom_pos, atom_vel, atom_frc, atom_id, atom_ok, brick_side):
        arrays = (atom_pos.T, atom_vel.T, atom_frc.T, atom_id, atom_ok, brick_side.reshape(1, 1))
        own, everyone, movers = exchange(*[pltpu.with_memory_space_constraint(array, pltpu.HBM) for array in arrays[:5]], arrays[5])
        partial, sums, rows = forces(own, everyone, movers)
        pos, vel, frc, new_id, new_ok, energy = store(*total_energy(partial, sums, rows))
        return pos.T, vel.T, frc.T, new_id, new_ok, energy.reshape(())

    row_spec = P(MESH_AXES, None)
    id_spec = P(MESH_AXES)
    return jax.shard_map(local_step, mesh=mesh, in_specs=(row_spec, row_spec, row_spec, id_spec, id_spec, P()), out_specs=(row_spec, row_spec, row_spec, id_spec, id_spec, P()), check_vma=False)
```

```python
import functools

import jax
import jax.numpy as jnp
from jax import lax
from jax.experimental import pallas as pl
from jax.experimental.pallas import tpu as pltpu
from jax.sharding import PartitionSpec as P

DT = 0.005
RC = 2.5
FAR_AWAY = 1.0e6
UCUT = 4.0 * (RC ** -12 - RC ** -6)
UPC = -48.0 * RC ** -13 + 24.0 * RC ** -7
MESH_AXES = ("z", "y", "x")
CAP = 729
PAD = 768
MIG = 256
SEG = {1: (0, 16), 2: (16, 16), 4: (32, 16), 3: (48, 32), 5: (80, 32), 6: (128, 32), 7: (160, 64)}
IC = 32
NARROW = 512
LANES = 128
ID_SPLIT = 65536
NT = (((1,), (1,)), ((), ()))
OTHERS = tuple(range(1, 8))
FAR_FIRST = (6, 7, 4, 2, 5, 3, 1)
REACH = RC + 0.01
MESH_ID = pl.DeviceIdType.MESH


def pieces_of(rows):
    first = rows.astype(jnp.bfloat16).astype(jnp.float32)
    rest = rows - first
    second = rest.astype(jnp.bfloat16).astype(jnp.float32)
    third = rest - second
    return jnp.concatenate([first, second, third], axis=0).astype(jnp.bfloat16)


def select_rows(rows, onehot):
    out = lax.dot_general(pieces_of(rows), onehot, NT, preferred_element_type=jnp.float32)
    return sum_groups(out, rows.shape[0])


def sum_groups(rows, size):
    total = rows[0:size]
    for k in range(size, rows.shape[0], size):
        total = total + rows[k:k + size]
    return total


def as_bf16(mask):
    return mask.astype(jnp.float32).astype(jnp.bfloat16)


def iota(dims, axis, dtype=jnp.float32):
    return lax.broadcasted_iota(jnp.int32, dims, axis).astype(dtype)


def id_of(rows):
    return (rows[6:7].astype(jnp.int32) - 1) * ID_SPLIT + rows[7:8].astype(jnp.int32)


def partner(relation):
    return tuple((lax.axis_index(name) + relation // bit) % 2 for name, bit in zip(MESH_AXES, (4, 2, 1)))


def greet():
    barrier = pltpu.get_barrier_semaphore()
    for relation in FAR_FIRST:
        pl.semaphore_signal(barrier, inc=1, device_id=partner(relation), device_id_type=MESH_ID)
    return barrier


def send_all(pairs, send_sem, recv_sem):
    copies = []
    for relation in FAR_FIRST:
        for which, (src, dst) in enumerate(pairs(relation)):
            copy = pltpu.make_async_remote_copy(src_ref=src, dst_ref=dst, send_sem=send_sem.at[which, relation], recv_sem=recv_sem.at[which, relation], device_id=partner(relation), device_id_type=MESH_ID)
            copy.start()
            copies.append(copy)
    return copies


def axis_column(values, rows):
    idx = lax.broadcasted_iota(jnp.int32, (rows, 1), 0)
    out = jnp.full((rows, 1), values[-1], jnp.float32)
    for k in range(len(values) - 1):
        out = jnp.where(idx == k, values[k], out)
    return out


def brick_coords():
    return [lax.axis_index(name).astype(jnp.float32) for name in ("x", "y", "z")]


def prefix_counts(member):
    member = member.astype(jnp.float32)
    starts = range(0, member.shape[1], LANES)
    stacked = as_bf16(jnp.concatenate([member[:, k:k + LANES] for k in starts], axis=0) > 0.5)
    col = iota((LANES, 2 * LANES), 1)
    ladder = as_bf16((iota((LANES, 2 * LANES), 0) < col) | (col >= LANES))
    counts = jnp.dot(stacked, ladder, preferred_element_type=jnp.float32)
    before = jnp.zeros((8, LANES), jnp.float32)
    ranks = []
    for k in range(0, counts.shape[0], 8):
        ranks.append(counts[k:k + 8, 0:LANES] + before)
        before = before + counts[k:k + 8, LANES:]
    return jnp.concatenate(ranks, axis=1), before


def exchange_kernel(pos_hbm, vel_hbm, frc_hbm, id_hbm, ok_hbm, side_hbm, own_ref, all_ref, mig_ref, pos_ref, vel_ref, frc_ref, id_ref, ok_ref, side_ref, pad_ref, load_sem, send_sem, recv_sem):
    loads = []
    for k, (src, dst) in enumerate(((pos_hbm, pos_ref), (vel_hbm, vel_ref), (frc_hbm, frc_ref), (id_hbm, id_ref), (ok_hbm, ok_ref), (side_hbm, side_ref))):
        load = pltpu.make_async_copy(src, dst, load_sem.at[k])
        load.start()
        loads.append(load)
    barrier = greet()
    pad_ref[...] = jnp.zeros_like(pad_ref)
    for load in loads:
        load.wait()
    side = side_ref[...]
    box = side * 2.0
    half_v = vel_ref[...] + (0.5 * DT) * frc_ref[...]
    pad_ref[0:3, 0:CAP] = pos_ref[...] + DT * half_v
    pad_ref[3:6, 0:CAP] = half_v
    pad_ref[6:7, 0:CAP] = (id_ref[...].reshape(1, CAP) // ID_SPLIT).astype(jnp.float32) + 1.0
    pad_ref[7:8, 0:CAP] = (id_ref[...].reshape(1, CAP) % ID_SPLIT).astype(jnp.float32)
    pad_ref[8:9, 0:CAP] = ok_ref[...].reshape(1, CAP).astype(jnp.float32)
    unwrapped = pad_ref[0:3, :]
    owned = pad_ref[8:9, :] > 0.5
    moved = jnp.where(unwrapped < 0.0, unwrapped + box, jnp.where(unwrapped >= box, unwrapped - box, unwrapped))
    for axis in range(3):
        all_ref[0, :, PAD * axis:PAD * (axis + 1)] = jnp.where(owned, moved[axis:axis + 1, :], FAR_AWAY)

    low = axis_column([coord * side for coord in brick_coords()], 3)
    outside = (unwrapped < low) | (unwrapped >= low + side)
    bits = jnp.where(outside, axis_column([1.0, 2.0, 4.0], 3), 0.0)
    code = jnp.sum(bits, axis=0, keepdims=True)
    code = jnp.where(owned, code, -1.0)
    lower = moved[2:3, :] < low[2:3, :] + 0.5 * side
    member = jnp.where((code == 0.0) & jnp.logical_not(lower), -1.0, code) == iota((8, PAD), 0)
    rank, _ = prefix_counts(member)
    offset = axis_column([0.0] + [float(SEG[m][0]) for m in OTHERS], 8)
    slot = jnp.sum(jnp.where(member, rank + offset, 0.0), axis=0, keepdims=True)
    rows = jnp.concatenate([moved, pad_ref[3:8, :]], axis=0)
    mig_ref[0] = select_rows(rows, as_bf16(iota((MIG, PAD), 0) == jnp.where(code > 0.5, slot, -1.0)))
    own_ref[16:17, :] = jnp.broadcast_to(side, (1, PAD))

    def pairs(relation):
        block = pl.ds(SEG[relation][0] // LANES * LANES, LANES)
        return (mig_ref.at[0, :, block], mig_ref.at[relation, :, block]), (all_ref.at[0], all_ref.at[relation])

    pl.semaphore_wait(barrier, len(OTHERS))
    copies = send_all(pairs, send_sem, recv_sem)
    pieces = pieces_of(rows)
    slots = iota((LANES, PAD), 0)
    upper_slot = iota((1, PAD), 1) - jnp.sum(rank, axis=0, keepdims=True)
    halves = (jnp.where((code == 0.0) & lower, slot, -1.0), jnp.where((code == 0.0) & jnp.logical_not(lower), upper_slot, -1.0))

    def pack(k, carry):
        first = k * LANES
        for half, target in enumerate(halves):
            out = lax.dot_general(pieces, as_bf16(slots == target - first.astype(jnp.float32)), NT, preferred_element_type=jnp.float32)
            own_ref[8 * half:8 * half + 8, pl.ds(pl.multiple_of(first, LANES), LANES)] = sum_groups(out, 8)
        return carry

    lax.fori_loop(0, PAD // LANES, pack, 0)
    for copy in copies:
        copy.wait()


def pair_terms(own, other, span):
    delta = []
    for mine, theirs in zip(own, other):
        diff = mine - theirs
        if span is not None:
            diff = diff - jnp.where(diff > 0.5 * span, span, jnp.where(diff < -0.5 * span, -span, 0.0))
        delta.append(diff)
    dist_sq = delta[0] * delta[0] + delta[1] * delta[1] + delta[2] * delta[2]
    in_range = (dist_sq < RC * RC) & (dist_sq > 0.01)
    inv_r = jnp.where(in_range, lax.rsqrt(dist_sq), 0.0)
    inv_r2 = inv_r * inv_r
    inv_r6 = inv_r2 * inv_r2 * inv_r2
    inv_r12 = inv_r6 * inv_r6
    well = inv_r12 - inv_r6
    scale = (well + inv_r12) * inv_r2 + (UPC / 24.0) * inv_r
    return [scale * d for d in delta], [well, dist_sq * inv_r, jnp.where(in_range, 1.0, 0.0)]


def force_kernel(own_ref, all_ref, mig_ref, en_ref, acc_ref, rows_ref, near_ref, mine_ref, plane_ref, list_ref, dense_ref, count_ref):
    side = own_ref[16:17, 0:1]
    box = side * 2.0
    centre = [(coord + 0.5) * side for coord in brick_coords()]
    lane = iota((1, MIG), 1, jnp.int32)
    arrivals = jnp.zeros((8, MIG), jnp.float32)
    for relation, (start, size) in SEG.items():
        arrivals = jnp.where((lane >= start) & (lane < start + size), mig_ref[relation], arrivals)
    half_of = jnp.where(arrivals[2:3, :] < centre[2], 0.0, 1.0)
    arrived = jnp.where(arrivals[6:7, :] > 0.5, half_of, -1.0) == iota((8, MIG), 0)
    ranks, _ = prefix_counts(arrived)
    targets, sizes = [], []
    for half in range(2):
        staying = jnp.sum((own_ref[8 * half + 6:8 * half + 7, :] > 0.5).astype(jnp.float32), axis=1, keepdims=True)
        here = arrived[half:half + 1, :]
        targets.append(jnp.where(here, ranks[half:half + 1, :] + staying, -1.0))
        sizes.append(jnp.sum((staying + jnp.sum(here.astype(jnp.float32), axis=1, keepdims=True)).astype(jnp.int32)))
    split = (sizes[0] + IC - 1) // IC * IC
    total = split + sizes[1]
    tail = all_ref[0, :, NARROW:PAD]
    for relation in OTHERS:
        tail = jnp.minimum(tail, all_ref[relation, :, NARROW:PAD])
    narrow = (jnp.min(tail) > 0.5 * FAR_AWAY) & (total <= NARROW + LANES) & (jnp.maximum(sizes[0], sizes[1]) <= NARROW - LANES)
    pieces = pieces_of(arrivals)

    def lay(target, rows, start):
        into = start % LANES
        first = pl.multiple_of(start - into, LANES)
        turned = pltpu.roll(rows, into, 1)
        behind = iota((8, LANES), 1, jnp.int32) >= into
        pltpu.store(target.at[:, pl.ds(first, LANES)], turned[:, 0:LANES], mask=behind)
        target[:, pl.ds(pl.multiple_of(first + LANES, LANES), rows.shape[1] - LANES)] = turned[:, LANES:]

    def classify(width):
        for relation in range(8):
            for axis in range(3):
                plane_ref[axis, relation:relation + 1, 0:width] = all_ref[relation, :, PAD * axis:PAD * axis + width]
        places = []
        across = jnp.zeros((8, width), jnp.float32)
        for axis in range(3):
            theirs = plane_ref[axis, :, 0:width] - centre[axis]
            theirs = jnp.where(theirs > side, theirs - box, jnp.where(theirs < -side, theirs + box, theirs))
            places.append(theirs)
            if axis < 2:
                excess = jnp.maximum(jnp.abs(theirs) - 0.5 * side, 0.0)
                across = across + excess * excess
        height = places[2]
        outside = (across > 0.0) | (jnp.abs(height) > 0.5 * side)
        lanes = iota((8, width), 1, jnp.int32)
        lists = []
        for sign in (1.0, -1.0):
            tilted = sign * height
            excess = jnp.minimum(jnp.maximum(jnp.abs(tilted + 0.25 * side) - 0.25 * side, 0.0), 1.5 * side - tilted)
            keep = outside & (across + excess * excess < REACH * REACH)
            front, held = prefix_counts(keep)
            lists.append((jnp.where(keep, lanes - front.astype(jnp.int32), 0), places, held.astype(jnp.int32)))
        return lists

    def prepare(lists, width, half_width, slots_width):
        slots = iota((LANES, MIG), 0)
        starts = range(0, half_width, LANES)
        for bit in range(0, 10, 2):
            step = 1 << bit
            for half in range(2):
                hops, planes, held = lists[half]
                next_hops = jnp.where(((hops >> bit) & 3) != 0, 0, hops)
                moved = planes
                for times in range(1, 4):
                    back = width - times * step
                    if back > 0:
                        coming = pltpu.roll(hops, back, 1)
                        take = ((coming >> bit) & 3) == times
                        next_hops = jnp.where(take, coming, next_hops)
                        moved = [jnp.where(take, pltpu.roll(old, back, 1), new) for old, new in zip(planes, moved)]
                lists[half] = (next_hops, moved, held)
                for start in starts[bit // 2::5]:
                    out = lax.dot_general(pieces, as_bf16(slots == targets[half] - float(start)), NT, preferred_element_type=jnp.float32)
                    dense_ref[half, :, start:start + LANES] = own_ref[8 * half:8 * half + 8, start:start + LANES] + sum_groups(out, 8)
        dense_ref[0, :, half_width:PAD + LANES] = jnp.zeros((8, PAD + LANES - half_width), jnp.float32)
        dense_ref[1, :, half_width:half_width + LANES] = jnp.zeros((8, LANES), jnp.float32)
        lay(dense_ref.at[0], dense_ref[1, :, 0:half_width + LANES], split)
        rows_ref[...] = dense_ref[0, :, 0:PAD]

        rows = rows_ref[:, 0:slots_width]
        filled = rows[6:7, :] > 0.5
        local = rows[0:3, :] - axis_column(centre, 3)
        for half in range(2):
            near_ref[half, 0:3, 0:slots_width] = jnp.where(filled, local, FAR_AWAY)
        local = jnp.concatenate([jnp.where(filled, local, -FAR_AWAY), jnp.zeros((5, slots_width), jnp.float32)], axis=0)
        spread = as_bf16(iota((24, 3 * LANES), 0, jnp.int32) % 8 == iota((24, 3 * LANES), 1, jnp.int32) // LANES)
        columns = lax.dot_general(pieces_of(local), spread, (((0,), (0,)), ((), ())), preferred_element_type=jnp.float32)
        for axis in range(3):
            mine_ref[axis, 0:slots_width, :] = columns[:, LANES * axis:LANES * (axis + 1)]

        for half in range(2):
            _, planes, held = lists[half]
            for relation in range(8):
                for axis in range(3):
                    list_ref[half, relation, axis:axis + 1, 0:width] = planes[axis][relation:relation + 1, :]
            start = total
            for relation in range(8):
                lay(near_ref.at[half], list_ref[half, relation, :, 0:width + LANES], start)
                start = start + held[relation, 0]
            lay(near_ref.at[half], jnp.full((8, 2 * LANES), FAR_AWAY, jnp.float32), start)
            count_ref[half] = (start + LANES - 1) // LANES

    short_lists = classify(NARROW)

    @pl.when(narrow)
    def _():
        prepare(short_lists, NARROW, NARROW - LANES, NARROW + LANES)

    @pl.when(jnp.logical_not(narrow))
    def _():
        prepare(classify(PAD), PAD, PAD, PAD)

    n_own = (total + IC - 1) // IC

    def sweep(span):
        def own_step(i, totals):
            first = pl.multiple_of(i * IC, IC)
            half = (first >= split).astype(jnp.int32)
            n_other = count_ref[half]
            own = [mine_ref[axis, pl.ds(first, IC), :] for axis in range(3)]

            def other_block(first, sums):
                forces, totals = sums
                other = [near_ref[half, axis:axis + 1, pl.ds(first, LANES)] for axis in range(3)]
                force, parts = pair_terms(own, other, span)
                forces = tuple(f + t for f, t in zip(forces, force))
                totals = tuple(t + sum_groups(p, 8) for t, p in zip(totals, parts))
                return forces, totals

            def other_step(j, sums):
                first = pl.multiple_of(j * 2 * LANES, 2 * LANES)
                return other_block(first + LANES, other_block(first, sums))

            def last_step(j, sums):
                return other_block(pl.multiple_of((n_other - 1) * LANES, LANES), sums)

            zero = jnp.zeros((IC, LANES), jnp.float32)
            sums = lax.fori_loop(0, n_other // 2, other_step, ((zero,) * 3, totals))
            forces, totals = lax.fori_loop(0, n_other % 2, last_step, sums)
            for axis in range(3):
                acc_ref[axis, pl.ds(first, IC), :] = forces[axis]
            return totals

        zero = jnp.zeros((8, LANES), jnp.float32)
        well, distance, pairs = lax.fori_loop(0, n_own, own_step, (zero,) * 3)
        energy = 2.0 * well - (0.5 * UPC) * distance - (0.5 * (UCUT - RC * UPC)) * pairs
        en_ref[...] = jnp.sum(energy, axis=0, keepdims=True)

    one_image = side[0, 0] >= 2.0 * RC

    @pl.when(one_image)
    def _():
        sweep(None)

    @pl.when(jnp.logical_not(one_image))
    def _():
        sweep(box)


def energy_kernel(en_ref, acc_ref, rows_ref, sum_ref, pos_ref, vel_ref, frc_ref, id_ref, ok_ref, force_ref, parts_ref, send_sem, recv_sem):
    barrier = greet()
    pl.semaphore_wait(barrier, len(OTHERS))
    copies = send_all(lambda relation: ((en_ref, parts_ref.at[relation]),), send_sem, recv_sem)
    def turn(k, carry):
        block = pl.ds(pl.multiple_of(k * LANES, LANES), LANES)
        for axis in range(3):
            force_ref[axis:axis + 1, block] = jnp.sum(jnp.transpose(acc_ref[axis, block, :]), axis=0, keepdims=True)
        return carry

    lax.fori_loop(0, PAD // LANES, turn, 0)
    rows = rows_ref[...]
    filled = rows[6:7, :] > 0.5
    key = jnp.where(filled, id_of(rows), 2147483647)
    key_col = jnp.transpose(jnp.broadcast_to(key, (8, PAD)))[:, 0:1]
    slot = jnp.dot(jnp.ones((8, PAD), jnp.bfloat16), as_bf16(key_col < key), preferred_element_type=jnp.float32)[0:1, :]
    onehot = as_bf16(iota((PAD, PAD), 0) == jnp.where(filled, slot, -1.0))
    force_ref[0:3, :] = jnp.where(filled, (24.0 * force_ref[0:3, :]), 0.0)
    force_ref[3:8, :] = jnp.zeros((5, PAD), jnp.float32)
    out = select_rows(jnp.concatenate([rows, force_ref[...]], axis=0), onehot)[:, 0:CAP]
    force = out[8:11]
    filled = out[6:7] > 0.5
    frc_ref[...] = force
    pos_ref[...] = out[0:3]
    vel_ref[...] = out[3:6] + (0.5 * DT) * force
    id_ref[...] = jnp.where(filled, id_of(out), 0).reshape(CAP)
    ok_ref[...] = filled.astype(jnp.int32).reshape(CAP)
    for copy in copies:
        copy.wait()
    parts_ref[0] = en_ref[...]
    level = [parts_ref[relation] for relation in range(8)]
    while len(level) > 1:
        level = [one + two for one, two in zip(level[0::2], level[1::2])]
    sum_ref[...] = level[0]


def store_kernel(sum_ref, *refs):
    sources, targets, total_ref, store_sem = refs[0:5], refs[5:11], refs[11], refs[12]
    stores = [pltpu.make_async_copy(sources[k], targets[k], store_sem.at[k]) for k in range(5)]
    for store in stores:
        store.start()
    total_ref[...] = jnp.sum(sum_ref[...], axis=1, keepdims=True)
    stores.append(pltpu.make_async_copy(total_ref, targets[5], store_sem.at[5]))
    stores[5].start()
    for store in stores:
        store.wait()


def solution(mesh):
    vmem = pl.BlockSpec(memory_space=pltpu.VMEM)
    hbm = pl.BlockSpec(memory_space=pltpu.HBM)
    f32, i32 = jnp.float32, jnp.int32

    def shape(dims, dtype=f32):
        return jax.ShapeDtypeStruct(dims, dtype)

    exchange = pl.pallas_call(
        exchange_kernel,
        out_shape=(shape((17, PAD)), shape((8, 1, 3 * PAD)), shape((8, 8, MIG))),
        in_specs=[hbm] * 5 + [pl.BlockSpec(memory_space=pl.ANY)],
        out_specs=(vmem, vmem, vmem),
        scratch_shapes=[pltpu.VMEM((3, CAP), f32)] * 3 + [pltpu.VMEM((CAP,), i32)] * 2 + [pltpu.VMEM((1, 1), f32), pltpu.VMEM((9, PAD), f32), pltpu.SemaphoreType.DMA((6,)), pltpu.SemaphoreType.DMA((2, 8)), pltpu.SemaphoreType.DMA((2, 8))],
        compiler_params=pltpu.CompilerParams(collective_id=0, has_side_effects=True, vmem_limit_bytes=16 << 20),
        name="exchange",
    )
    forces = pl.pallas_call(
        force_kernel,
        out_shape=(shape((1, 128)), shape((3, PAD, 128)), shape((8, PAD))),
        in_specs=[vmem] * 3,
        out_specs=(vmem,) * 3,
        scratch_shapes=[pltpu.VMEM((2, 8, 9 * PAD + 256), f32), pltpu.VMEM((3, PAD, 128), f32), pltpu.VMEM((3, 8, PAD), f32), pltpu.VMEM((2, 8, 8, PAD + 128), f32), pltpu.VMEM((2, 8, 2 * PAD + 256), f32), pltpu.SMEM((2,), i32)],
        compiler_params=pltpu.CompilerParams(vmem_limit_bytes=16 << 20),
        name="forces",
    )
    results = (shape((3, CAP)), shape((3, CAP)), shape((3, CAP)), shape((CAP,), i32), shape((CAP,), i32))
    total_energy = pl.pallas_call(
        energy_kernel,
        out_shape=(shape((1, 128)),) + results,
        in_specs=[vmem] * 3,
        out_specs=(vmem,) * 6,
        scratch_shapes=[pltpu.VMEM((8, PAD), f32), pltpu.VMEM((8, 1, LANES), f32), pltpu.SemaphoreType.DMA((1, 8)), pltpu.SemaphoreType.DMA((1, 8))],
        compiler_params=pltpu.CompilerParams(collective_id=1, has_side_effects=True, vmem_limit_bytes=16 << 20),
        name="energy",
    )
    store = pl.pallas_call(
        store_kernel,
        out_shape=results + (shape((1, 1)),),
        in_specs=[vmem] * 6,
        out_specs=(hbm,) * 6,
        scratch_shapes=[pltpu.VMEM((1, 1), f32), pltpu.SemaphoreType.DMA((6,))],
        compiler_params=pltpu.CompilerParams(vmem_limit_bytes=16 << 20),
        name="store",
    )

    def local_step(atom_pos, atom_vel, atom_frc, atom_id, atom_ok, brick_side):
        arrays = (atom_pos.T, atom_vel.T, atom_frc.T, atom_id, atom_ok, brick_side.reshape(1, 1))
        own, everyone, movers = exchange(*[pltpu.with_memory_space_constraint(array, pltpu.HBM) for array in arrays[:5]], arrays[5])
        partial, sums, rows = forces(own, everyone, movers)
        pos, vel, frc, new_id, new_ok, energy = store(*total_energy(partial, sums, rows))
        return pos.T, vel.T, frc.T, new_id, new_ok, energy.reshape(())

    row_spec = P(MESH_AXES, None)
    id_spec = P(MESH_AXES)
    return jax.shard_map(local_step, mesh=mesh, in_specs=(row_spec, row_spec, row_spec, id_spec, id_spec, P()), out_specs=(row_spec, row_spec, row_spec, id_spec, id_spec, P()), check_vma=False)
```

```python
import functools

import jax
import jax.numpy as jnp
from jax import lax
from jax.experimental import pallas as pl
from jax.experimental.pallas import tpu as pltpu
from jax.sharding import PartitionSpec as P

DT = 0.005
RC = 2.5
FAR_AWAY = 1.0e6
UCUT = 4.0 * (RC ** -12 - RC ** -6)
UPC = -48.0 * RC ** -13 + 24.0 * RC ** -7
MESH_AXES = ("z", "y", "x")
CAP = 729
PAD = 768
MIG = 256
SEG = {1: (0, 16), 2: (16, 16), 4: (32, 16), 3: (48, 32), 5: (80, 32), 6: (128, 32), 7: (160, 64)}
IC = 32
NARROW = 512
LANES = 128
ID_SPLIT = 65536
NT = (((1,), (1,)), ((), ()))
OTHERS = tuple(range(1, 8))
FAR_FIRST = (6, 7, 4, 2, 5, 3, 1)
REACH = RC + 0.01
MESH_ID = pl.DeviceIdType.MESH


def pieces_of(rows):
    first = rows.astype(jnp.bfloat16).astype(jnp.float32)
    rest = rows - first
    second = rest.astype(jnp.bfloat16).astype(jnp.float32)
    third = rest - second
    return jnp.concatenate([first, second, third], axis=0).astype(jnp.bfloat16)


def select_rows(rows, onehot):
    out = lax.dot_general(pieces_of(rows), onehot, NT, preferred_element_type=jnp.float32)
    return sum_groups(out, rows.shape[0])


def sum_groups(rows, size):
    total = rows[0:size]
    for k in range(size, rows.shape[0], size):
        total = total + rows[k:k + size]
    return total


def as_bf16(mask):
    return mask.astype(jnp.float32).astype(jnp.bfloat16)


def iota(dims, axis, dtype=jnp.float32):
    return lax.broadcasted_iota(jnp.int32, dims, axis).astype(dtype)


def id_of(rows):
    return (rows[6:7].astype(jnp.int32) - 1) * ID_SPLIT + rows[7:8].astype(jnp.int32)


def partner(relation):
    return tuple((lax.axis_index(name) + relation // bit) % 2 for name, bit in zip(MESH_AXES, (4, 2, 1)))


def greet():
    barrier = pltpu.get_barrier_semaphore()
    for relation in FAR_FIRST:
        pl.semaphore_signal(barrier, inc=1, device_id=partner(relation), device_id_type=MESH_ID)
    return barrier


def send_all(pairs, send_sem, recv_sem):
    copies = []
    for relation in FAR_FIRST:
        for which, (src, dst) in enumerate(pairs(relation)):
            copy = pltpu.make_async_remote_copy(src_ref=src, dst_ref=dst, send_sem=send_sem.at[which, relation], recv_sem=recv_sem.at[which, relation], device_id=partner(relation), device_id_type=MESH_ID)
            copy.start()
            copies.append(copy)
    return copies


def axis_column(values, rows):
    idx = lax.broadcasted_iota(jnp.int32, (rows, 1), 0)
    out = jnp.full((rows, 1), values[-1], jnp.float32)
    for k in range(len(values) - 1):
        out = jnp.where(idx == k, values[k], out)
    return out


def brick_coords():
    return [lax.axis_index(name).astype(jnp.float32) for name in ("x", "y", "z")]


def prefix_counts(member):
    member = member.astype(jnp.float32)
    starts = range(0, member.shape[1], LANES)
    stacked = as_bf16(jnp.concatenate([member[:, k:k + LANES] for k in starts], axis=0) > 0.5)
    col = iota((LANES, 2 * LANES), 1)
    ladder = as_bf16((iota((LANES, 2 * LANES), 0) < col) | (col >= LANES))
    counts = jnp.dot(stacked, ladder, preferred_element_type=jnp.float32)
    before = jnp.zeros((8, LANES), jnp.float32)
    ranks = []
    for k in range(0, counts.shape[0], 8):
        ranks.append(counts[k:k + 8, 0:LANES] + before)
        before = before + counts[k:k + 8, LANES:]
    return jnp.concatenate(ranks, axis=1), before


def exchange_kernel(pos_hbm, vel_hbm, frc_hbm, id_hbm, ok_hbm, side_hbm, own_ref, all_ref, mig_ref, pos_ref, vel_ref, frc_ref, id_ref, ok_ref, side_ref, pad_ref, load_sem, send_sem, recv_sem):
    loads = []
    for k, (src, dst) in enumerate(((pos_hbm, pos_ref), (vel_hbm, vel_ref), (frc_hbm, frc_ref), (id_hbm, id_ref), (ok_hbm, ok_ref), (side_hbm, side_ref))):
        load = pltpu.make_async_copy(src, dst, load_sem.at[k])
        load.start()
        loads.append(load)
    barrier = greet()
    pad_ref[...] = jnp.zeros_like(pad_ref)
    for load in loads:
        load.wait()
    side = side_ref[...]
    box = side * 2.0
    half_v = vel_ref[...] + (0.5 * DT) * frc_ref[...]
    pad_ref[0:3, 0:CAP] = pos_ref[...] + DT * half_v
    pad_ref[3:6, 0:CAP] = half_v
    pad_ref[6:7, 0:CAP] = (id_ref[...].reshape(1, CAP) // ID_SPLIT).astype(jnp.float32) + 1.0
    pad_ref[7:8, 0:CAP] = (id_ref[...].reshape(1, CAP) % ID_SPLIT).astype(jnp.float32)
    pad_ref[8:9, 0:CAP] = ok_ref[...].reshape(1, CAP).astype(jnp.float32)
    unwrapped = pad_ref[0:3, :]
    owned = pad_ref[8:9, :] > 0.5
    moved = jnp.where(unwrapped < 0.0, unwrapped + box, jnp.where(unwrapped >= box, unwrapped - box, unwrapped))
    for axis in range(3):
        all_ref[0, :, PAD * axis:PAD * (axis + 1)] = jnp.where(owned, moved[axis:axis + 1, :], FAR_AWAY)

    low = axis_column([coord * side for coord in brick_coords()], 3)
    outside = (unwrapped < low) | (unwrapped >= low + side)
    bits = jnp.where(outside, axis_column([1.0, 2.0, 4.0], 3), 0.0)
    code = jnp.sum(bits, axis=0, keepdims=True)
    code = jnp.where(owned, code, -1.0)
    lower = moved[2:3, :] < low[2:3, :] + 0.5 * side
    member = jnp.where((code == 0.0) & jnp.logical_not(lower), -1.0, code) == iota((8, PAD), 0)
    rank, _ = prefix_counts(member)
    offset = axis_column([0.0] + [float(SEG[m][0]) for m in OTHERS], 8)
    slot = jnp.sum(jnp.where(member, rank + offset, 0.0), axis=0, keepdims=True)
    rows = jnp.concatenate([moved, pad_ref[3:8, :]], axis=0)
    mig_ref[0] = select_rows(rows, as_bf16(iota((MIG, PAD), 0) == jnp.where(code > 0.5, slot, -1.0)))
    own_ref[16:17, :] = jnp.broadcast_to(side, (1, PAD))

    def pairs(relation):
        block = pl.ds(SEG[relation][0] // LANES * LANES, LANES)
        return (mig_ref.at[0, :, block], mig_ref.at[relation, :, block]), (all_ref.at[0], all_ref.at[relation])

    pl.semaphore_wait(barrier, len(OTHERS))
    copies = send_all(pairs, send_sem, recv_sem)
    pieces = pieces_of(rows)
    slots = iota((LANES, PAD), 0)
    upper_slot = iota((1, PAD), 1) - jnp.sum(rank, axis=0, keepdims=True)
    halves = (jnp.where((code == 0.0) & lower, slot, -1.0), jnp.where((code == 0.0) & jnp.logical_not(lower), upper_slot, -1.0))

    def pack(k, carry):
        first = k * LANES
        for half, target in enumerate(halves):
            out = lax.dot_general(pieces, as_bf16(slots == target - first.astype(jnp.float32)), NT, preferred_element_type=jnp.float32)
            own_ref[8 * half:8 * half + 8, pl.ds(pl.multiple_of(first, LANES), LANES)] = sum_groups(out, 8)
        return carry

    lax.fori_loop(0, PAD // LANES, pack, 0)
    for copy in copies:
        copy.wait()


def pair_terms(own, other, span):
    delta = []
    for mine, theirs in zip(own, other):
        diff = mine - theirs
        if span is not None:
            diff = diff - jnp.where(diff > 0.5 * span, span, jnp.where(diff < -0.5 * span, -span, 0.0))
        delta.append(diff)
    dist_sq = delta[0] * delta[0] + delta[1] * delta[1] + delta[2] * delta[2]
    in_range = (dist_sq < RC * RC) & (dist_sq > 0.01)
    inv_r = jnp.where(in_range, lax.rsqrt(dist_sq), 0.0)
    inv_r2 = inv_r * inv_r
    inv_r6 = inv_r2 * inv_r2 * inv_r2
    inv_r12 = inv_r6 * inv_r6
    well = inv_r12 - inv_r6
    scale = (well + inv_r12) * inv_r2 + (UPC / 24.0) * inv_r
    return [scale * d for d in delta], [well, dist_sq * inv_r, jnp.where(in_range, 1.0, 0.0)]


def force_kernel(own_ref, all_ref, mig_ref, en_ref, acc_ref, rows_ref, near_ref, mine_ref, plane_ref, list_ref, dense_ref, count_ref):
    side = own_ref[16:17, 0:1]
    box = side * 2.0
    centre = [(coord + 0.5) * side for coord in brick_coords()]
    lane = iota((1, MIG), 1, jnp.int32)
    arrivals = jnp.zeros((8, MIG), jnp.float32)
    for relation, (start, size) in SEG.items():
        arrivals = jnp.where((lane >= start) & (lane < start + size), mig_ref[relation], arrivals)
    half_of = jnp.where(arrivals[2:3, :] < centre[2], 0.0, 1.0)
    arrived = jnp.where(arrivals[6:7, :] > 0.5, half_of, -1.0) == iota((8, MIG), 0)
    ranks, _ = prefix_counts(arrived)
    targets, sizes = [], []
    for half in range(2):
        staying = jnp.sum((own_ref[8 * half + 6:8 * half + 7, :] > 0.5).astype(jnp.float32), axis=1, keepdims=True)
        here = arrived[half:half + 1, :]
        targets.append(jnp.where(here, ranks[half:half + 1, :] + staying, -1.0))
        sizes.append(jnp.sum((staying + jnp.sum(here.astype(jnp.float32), axis=1, keepdims=True)).astype(jnp.int32)))
    split = (sizes[0] + IC - 1) // IC * IC
    total = split + sizes[1]
    tail = all_ref[0, :, NARROW:PAD]
    for relation in OTHERS:
        tail = jnp.minimum(tail, all_ref[relation, :, NARROW:PAD])
    narrow = (jnp.min(tail) > 0.5 * FAR_AWAY) & (total <= NARROW + LANES) & (jnp.maximum(sizes[0], sizes[1]) <= NARROW - LANES)
    pieces = pieces_of(arrivals)

    def lay(target, rows, start):
        into = start % LANES
        first = pl.multiple_of(start - into, LANES)
        turned = pltpu.roll(rows, into, 1)
        behind = iota((8, LANES), 1, jnp.int32) >= into
        pltpu.store(target.at[:, pl.ds(first, LANES)], turned[:, 0:LANES], mask=behind)
        target[:, pl.ds(pl.multiple_of(first + LANES, LANES), rows.shape[1] - LANES)] = turned[:, LANES:]

    def classify(width):
        for relation in range(8):
            for axis in range(3):
                plane_ref[axis, relation:relation + 1, 0:width] = all_ref[relation, :, PAD * axis:PAD * axis + width]
        places = []
        across = jnp.zeros((8, width), jnp.float32)
        for axis in range(3):
            theirs = plane_ref[axis, :, 0:width] - centre[axis]
            theirs = jnp.where(theirs > side, theirs - box, jnp.where(theirs < -side, theirs + box, theirs))
            places.append(theirs)
            if axis < 2:
                excess = jnp.maximum(jnp.abs(theirs) - 0.5 * side, 0.0)
                across = across + excess * excess
        height = places[2]
        outside = (across > 0.0) | (jnp.abs(height) > 0.5 * side)
        lanes = iota((8, width), 1, jnp.int32)
        lists = []
        for sign in (1.0, -1.0):
            tilted = sign * height
            excess = jnp.minimum(jnp.maximum(jnp.abs(tilted + 0.25 * side) - 0.25 * side, 0.0), 1.5 * side - tilted)
            keep = outside & (across + excess * excess < REACH * REACH)
            front, held = prefix_counts(keep)
            lists.append((jnp.where(keep, lanes - front.astype(jnp.int32), 0), places, held.astype(jnp.int32)))
        return lists

    def prepare(lists, width, half_width, slots_width):
        slots = iota((LANES, MIG), 0)
        starts = range(0, half_width, LANES)
        for bit in range(0, 10, 2):
            step = 1 << bit
            for half in range(2):
                hops, planes, held = lists[half]
                next_hops = jnp.where(((hops >> bit) & 3) != 0, 0, hops)
                moved = planes
                for times in range(1, 4):
                    back = width - times * step
                    if back > 0:
                        coming = pltpu.roll(hops, back, 1)
                        take = ((coming >> bit) & 3) == times
                        next_hops = jnp.where(take, coming, next_hops)
                        moved = [jnp.where(take, pltpu.roll(old, back, 1), new) for old, new in zip(planes, moved)]
                lists[half] = (next_hops, moved, held)
                for start in starts[bit // 2::5]:
                    out = lax.dot_general(pieces, as_bf16(slots == targets[half] - float(start)), NT, preferred_element_type=jnp.float32)
                    dense_ref[half, :, start:start + LANES] = own_ref[8 * half:8 * half + 8, start:start + LANES] + sum_groups(out, 8)
        dense_ref[0, :, half_width:PAD + LANES] = jnp.zeros((8, PAD + LANES - half_width), jnp.float32)
        dense_ref[1, :, half_width:half_width + LANES] = jnp.zeros((8, LANES), jnp.float32)
        lay(dense_ref.at[0], dense_ref[1, :, 0:half_width + LANES], split)
        rows_ref[...] = dense_ref[0, :, 0:PAD]

        rows = rows_ref[:, 0:slots_width]
        filled = rows[6:7, :] > 0.5
        local = rows[0:3, :] - axis_column(centre, 3)
        for half in range(2):
            near_ref[half, 0:3, 0:slots_width] = jnp.where(filled, local, FAR_AWAY)
        local = jnp.concatenate([jnp.where(filled, local, -FAR_AWAY), jnp.zeros((5, slots_width), jnp.float32)], axis=0)
        spread = as_bf16(iota((24, 3 * LANES), 0, jnp.int32) % 8 == iota((24, 3 * LANES), 1, jnp.int32) // LANES)
        columns = lax.dot_general(pieces_of(local), spread, (((0,), (0,)), ((), ())), preferred_element_type=jnp.float32)
        for axis in range(3):
            mine_ref[axis, 0:slots_width, :] = columns[:, LANES * axis:LANES * (axis + 1)]

        for half in range(2):
            _, planes, held = lists[half]
            for relation in range(8):
                for axis in range(3):
                    list_ref[half, relation, axis:axis + 1, 0:width] = planes[axis][relation:relation + 1, :]
            start = total
            for relation in range(8):
                lay(near_ref.at[half], list_ref[half, relation, :, 0:width + LANES], start)
                start = start + held[relation, 0]
            lay(near_ref.at[half], jnp.full((8, 2 * LANES), FAR_AWAY, jnp.float32), start)
            count_ref[half] = (start + 2 * LANES - 1) // (2 * LANES)

    short_lists = classify(NARROW)

    @pl.when(narrow)
    def _():
        prepare(short_lists, NARROW, NARROW - LANES, NARROW + LANES)

    @pl.when(jnp.logical_not(narrow))
    def _():
        prepare(classify(PAD), PAD, PAD, PAD)

    n_own = (total + IC - 1) // IC

    def sweep(span):
        def own_step(i, totals):
            first = pl.multiple_of(i * IC, IC)
            half = (first >= split).astype(jnp.int32)
            n_other = count_ref[half]
            own = [mine_ref[axis, pl.ds(first, IC), :] for axis in range(3)]

            def other_block(first, sums):
                forces, totals = sums
                other = [near_ref[half, axis:axis + 1, pl.ds(first, LANES)] for axis in range(3)]
                force, parts = pair_terms(own, other, span)
                forces = tuple(f + t for f, t in zip(forces, force))
                totals = tuple(t + sum_groups(p, 8) for t, p in zip(totals, parts))
                return forces, totals

            def other_step(j, sums):
                first = pl.multiple_of(j * 2 * LANES, 2 * LANES)
                return other_block(first + LANES, other_block(first, sums))

            zero = jnp.zeros((IC, LANES), jnp.float32)
            forces, totals = lax.fori_loop(0, n_other, other_step, ((zero,) * 3, totals))
            for axis in range(3):
                acc_ref[axis, pl.ds(first, IC), :] = forces[axis]
            return totals

        zero = jnp.zeros((8, LANES), jnp.float32)
        well, distance, pairs = lax.fori_loop(0, n_own, own_step, (zero,) * 3)
        energy = 2.0 * well - (0.5 * UPC) * distance - (0.5 * (UCUT - RC * UPC)) * pairs
        en_ref[...] = jnp.sum(energy, axis=0, keepdims=True)

    one_image = side[0, 0] >= 2.0 * RC

    @pl.when(one_image)
    def _():
        sweep(None)

    @pl.when(jnp.logical_not(one_image))
    def _():
        sweep(box)


def energy_kernel(en_ref, acc_ref, rows_ref, sum_ref, pos_ref, vel_ref, frc_ref, id_ref, ok_ref, force_ref, parts_ref, send_sem, recv_sem):
    barrier = greet()
    pl.semaphore_wait(barrier, len(OTHERS))
    copies = send_all(lambda relation: ((en_ref, parts_ref.at[relation]),), send_sem, recv_sem)
    def turn(k, carry):
        block = pl.ds(pl.multiple_of(k * LANES, LANES), LANES)
        for axis in range(3):
            force_ref[axis:axis + 1, block] = jnp.sum(jnp.transpose(acc_ref[axis, block, :]), axis=0, keepdims=True)
        return carry

    lax.fori_loop(0, PAD // LANES, turn, 0)
    rows = rows_ref[...]
    filled = rows[6:7, :] > 0.5
    key = jnp.where(filled, id_of(rows), 2147483647)
    key_col = jnp.transpose(jnp.broadcast_to(key, (8, PAD)))[:, 0:1]
    slot = jnp.dot(jnp.ones((8, PAD), jnp.bfloat16), as_bf16(key_col < key), preferred_element_type=jnp.float32)[0:1, :]
    onehot = as_bf16(iota((PAD, PAD), 0) == jnp.where(filled, slot, -1.0))
    force_ref[0:3, :] = jnp.where(filled, (24.0 * force_ref[0:3, :]), 0.0)
    force_ref[3:8, :] = jnp.zeros((5, PAD), jnp.float32)
    out = select_rows(jnp.concatenate([rows, force_ref[...]], axis=0), onehot)[:, 0:CAP]
    force = out[8:11]
    filled = out[6:7] > 0.5
    frc_ref[...] = force
    pos_ref[...] = out[0:3]
    vel_ref[...] = out[3:6] + (0.5 * DT) * force
    id_ref[...] = jnp.where(filled, id_of(out), 0).reshape(CAP)
    ok_ref[...] = filled.astype(jnp.int32).reshape(CAP)
    for copy in copies:
        copy.wait()
    parts_ref[0] = en_ref[...]
    level = [parts_ref[relation] for relation in range(8)]
    while len(level) > 1:
        level = [one + two for one, two in zip(level[0::2], level[1::2])]
    sum_ref[...] = level[0]


def store_kernel(sum_ref, *refs):
    sources, targets, total_ref, store_sem = refs[0:5], refs[5:11], refs[11], refs[12]
    stores = [pltpu.make_async_copy(sources[k], targets[k], store_sem.at[k]) for k in range(5)]
    for store in stores:
        store.start()
    total_ref[...] = jnp.sum(sum_ref[...], axis=1, keepdims=True)
    stores.append(pltpu.make_async_copy(total_ref, targets[5], store_sem.at[5]))
    stores[5].start()
    for store in stores:
        store.wait()


def solution(mesh):
    vmem = pl.BlockSpec(memory_space=pltpu.VMEM)
    hbm = pl.BlockSpec(memory_space=pltpu.HBM)
    f32, i32 = jnp.float32, jnp.int32

    def shape(dims, dtype=f32):
        return jax.ShapeDtypeStruct(dims, dtype)

    exchange = pl.pallas_call(
        exchange_kernel,
        out_shape=(shape((17, PAD)), shape((8, 1, 3 * PAD)), shape((8, 8, MIG))),
        in_specs=[hbm] * 5 + [pl.BlockSpec(memory_space=pl.ANY)],
        out_specs=(vmem, vmem, vmem),
        scratch_shapes=[pltpu.VMEM((3, CAP), f32)] * 3 + [pltpu.VMEM((CAP,), i32)] * 2 + [pltpu.VMEM((1, 1), f32), pltpu.VMEM((9, PAD), f32), pltpu.SemaphoreType.DMA((6,)), pltpu.SemaphoreType.DMA((2, 8)), pltpu.SemaphoreType.DMA((2, 8))],
        compiler_params=pltpu.CompilerParams(collective_id=0, has_side_effects=True, vmem_limit_bytes=16 << 20),
        name="exchange",
    )
    forces = pl.pallas_call(
        force_kernel,
        out_shape=(shape((1, 128)), shape((3, PAD, 128)), shape((8, PAD))),
        in_specs=[vmem] * 3,
        out_specs=(vmem,) * 3,
        scratch_shapes=[pltpu.VMEM((2, 8, 9 * PAD + 256), f32), pltpu.VMEM((3, PAD, 128), f32), pltpu.VMEM((3, 8, PAD), f32), pltpu.VMEM((2, 8, 8, PAD + 128), f32), pltpu.VMEM((2, 8, 2 * PAD + 256), f32), pltpu.SMEM((2,), i32)],
        compiler_params=pltpu.CompilerParams(vmem_limit_bytes=16 << 20),
        name="forces",
    )
    results = (shape((3, CAP)), shape((3, CAP)), shape((3, CAP)), shape((CAP,), i32), shape((CAP,), i32))
    total_energy = pl.pallas_call(
        energy_kernel,
        out_shape=(shape((1, 128)),) + results,
        in_specs=[vmem] * 3,
        out_specs=(vmem,) * 6,
        scratch_shapes=[pltpu.VMEM((8, PAD), f32), pltpu.VMEM((8, 1, LANES), f32), pltpu.SemaphoreType.DMA((1, 8)), pltpu.SemaphoreType.DMA((1, 8))],
        compiler_params=pltpu.CompilerParams(collective_id=1, has_side_effects=True, vmem_limit_bytes=16 << 20),
        name="energy",
    )
    store = pl.pallas_call(
        store_kernel,
        out_shape=results + (shape((1, 1)),),
        in_specs=[vmem] * 6,
        out_specs=(hbm,) * 6,
        scratch_shapes=[pltpu.VMEM((1, 1), f32), pltpu.SemaphoreType.DMA((6,))],
        compiler_params=pltpu.CompilerParams(vmem_limit_bytes=16 << 20),
        name="store",
    )

    def local_step(atom_pos, atom_vel, atom_frc, atom_id, atom_ok, brick_side):
        arrays = (atom_pos.T, atom_vel.T, atom_frc.T, atom_id, atom_ok, brick_side.reshape(1, 1))
        own, everyone, movers = exchange(*[pltpu.with_memory_space_constraint(array, pltpu.HBM) for array in arrays[:5]], arrays[5])
        partial, sums, rows = forces(own, everyone, movers)
        pos, vel, frc, new_id, new_ok, energy = store(*total_energy(partial, sums, rows))
        return pos.T, vel.T, frc.T, new_id, new_ok, energy.reshape(())

    row_spec = P(MESH_AXES, None)
    id_spec = P(MESH_AXES)
    return jax.shard_map(local_step, mesh=mesh, in_specs=(row_spec, row_spec, row_spec, id_spec, id_spec, P()), out_specs=(row_spec, row_spec, row_spec, id_spec, id_spec, P()), check_vma=False)
```
